32 devices in a mesh: parts: 2 (over y), row: 4 (over x, core), col: 4 (over z).
Axes of the slice: x: 2, y: 2, z: 4, core: 2. Of those that a mesh axis runs over, the one named last changes fastest.
Arguments:
- alignment_tensor: bfloat16 [256, 256, 256], P(('parts', 'col'), 'row'), parts along dimension 0, may hold values from -6 to 6
- standardizer_scaling: float32 [256], replicated, may hold values from 0.25 to 1.75
- standardizer_offset: float32 [256], replicated, may hold values from -3 to 3
- first_projector: bfloat16 [256, 32], replicated, may hold values from -0.375 to 0.375
- second_projector: bfloat16 [256, 32], replicated, may hold values from -0.375 to 0.375
- final_projector: bfloat16 [1024, 128], replicated, may hold values from -1 to 1
- final_offset: float32 [128], replicated, may hold values from -3 to 3
- amino_strand_label: int32 [512], P('parts'), parts along dimension 0, may hold values from 0 to 7, never falling along the last dimension, each value on 1 to 128 neighbouring positions
- matched_strand_count: int32 [16, 8], P('parts'), parts along dimension 0, may hold values from 32 to 128, as said below
- couple_delta_adjoint: bfloat16 [512, 256, 128], P(('parts', 'row'), 'col'), parts along dimension 0, may hold values from -6 to 6
Outputs:
- pair_update: bfloat16 [512, 256, 128], P(('parts', 'row'), 'col'), parts along dimension 0
- adjoint_first_factor: bfloat16 [256, 8192], P(('parts', 'col'), 'row'), parts along dimension 0
- grad_right: bfloat16 [256, 8192], P(('parts', 'col'), 'row'), parts along dimension 0
- grad_w_out: float32 [2048, 128], P('parts'), parts along dimension 0
The draws below stay inside these ranges and needn't reach their ends.
There are 2 independent parts, one for each index of `parts`. The reference program is written for one: setup_inputs(seed, part) draws one part's arguments, and reference() takes and returns one part's arrays. A program takes and returns all parts, laid end to end along the dimension named above; an argument that names none is the same for every part. Nothing has to cross between parts.
Inputs may be any that keep to these rules, and one draw needn't show every extreme that they name: `amino_strand_label`: chain numbers never fall along the residues; a chain has 1 to 128 residues. `matched_strand_count`: every entry is a multiple of 32.
All inputs are finite; a program needn't handle non-finite values.
Results may differ from the reference program's by a relative error of at most 0.018.
Values may be sent and summed in bfloat16 or wider, within the bound.
A program may use at most 256 MiB of HBM per device.

```python
import math
import jax
import jax.numpy as jnp
import numpy as np
from jax import lax

ALIGNED_HOMOLOGS = 128
ALIGNED_FEATS = 256
PROJECTED_SIZE = 32
CZ = 128
WINDOW_AMINOS = 256
DEPTH_STEP = 32
CHAINS = 8
LEVELS = 4
N_ROW = 4


def draw_matched_strand_count(key, part):
    levels = jax.random.randint(jax.random.fold_in(key, 11), (CHAINS * CHAINS,), 1, LEVELS + 1)
    spots = jax.random.permutation(jax.random.fold_in(key, 12), CHAINS * CHAINS)
    levels = levels.at[spots[0]].set(LEVELS).at[spots[1]].set(1)
    return (levels * DEPTH_STEP).reshape(CHAINS, CHAINS).astype(jnp.int32)


def steps_of(key, shape, shards, smallest, top_value):
    def one(dim, shards_of):
        steps = jax.random.uniform(jax.random.fold_in(jax.random.fold_in(key, 6), dim), (shards_of,), jnp.float32, smallest / len(shards), top_value / len(shards))
        return jnp.repeat(jnp.exp(steps), shape[dim] // shards_of).reshape((-1,) + (1,) * (len(shape) - dim - 1))

    loudness = one(*shards[0])
    for cut in shards[1:]:
        loudness = loudness * one(*cut)
    return loudness


def length_profile(amount, total, reach, lean):
    weights = [(1 << 20) // math.isqrt(grade ** lean) + 1 for grade in range(2, amount + 1)]
    rest, counts = total - reach - (amount - 1), [1] * (amount - 1)
    while rest > 0:
        free = [i for i in range(amount - 1) if counts[i] < reach]
        pool, budget = sum([weights[i] for i in free]), rest
        for i in free:
            more = min(reach - counts[i], max(1, budget * weights[i] // pool), rest)
            counts[i] = counts[i] + more
            rest = rest - more
    return np.array([reach] + counts)


def uneven(stream_key, amount, total, bound, slope):
    if amount == 2:
        one = jax.random.randint(stream_key, (), max(1, total - bound), min(bound, total - 1) + 1)
        return jnp.stack([one, total - one])
    sizes = jnp.asarray(length_profile(amount, total, bound, slope), jnp.int32)
    twos = (amount - 1) // 2
    donor, taker = sizes[1:1 + 2 * twos:2], sizes[2:2 + 2 * twos:2]
    slack = jnp.minimum(donor - 1, bound - taker)
    shifted = jax.random.randint(jax.random.fold_in(stream_key, 1), (twos,), 0, 1 << 20) % (slack + 1)
    sizes = sizes.at[1:1 + 2 * twos:2].set(donor - shifted).at[2:2 + 2 * twos:2].set(taker + shifted)
    return sizes[jax.random.permutation(jax.random.fold_in(stream_key, 2), amount)]


def bell_draw(own_key, shape, scale, limit, cuts=(), held_as=jnp.bfloat16):
    array = scale * jax.random.normal(own_key, shape, jnp.float32)
    if cuts:
        array = array * steps_of(own_key, shape, cuts, -0.22, 0.18)
    return jnp.clip(array, -limit, limit).astype(held_as)


def setup_inputs(seed: int = 0, part: int = 0) -> dict:
    key_of = jax.random.split(jax.random.key(seed), 11)
    part_splits = jax.random.split(jax.random.fold_in(key_of[10], part), 11)
    return {
        "alignment_tensor": bell_draw(part_splits[0], (ALIGNED_HOMOLOGS, WINDOW_AMINOS, ALIGNED_FEATS), 1.0, 6.0, ((0, 4), (1, 4))),
        "standardizer_scaling": jnp.clip(1.0 + 0.15 * jax.random.normal(key_of[1], (ALIGNED_FEATS,), jnp.float32), 0.25, 1.75),
        "standardizer_offset": bell_draw(key_of[2], (ALIGNED_FEATS,), 0.5, 3.0, (), jnp.float32),
        "first_projector": bell_draw(key_of[3], (ALIGNED_FEATS, PROJECTED_SIZE), ALIGNED_FEATS ** -0.5, 0.375),
        "second_projector": bell_draw(key_of[4], (ALIGNED_FEATS, PROJECTED_SIZE), ALIGNED_FEATS ** -0.5, 0.375),
        "final_projector": bell_draw(key_of[5], (PROJECTED_SIZE * PROJECTED_SIZE, CZ), PROJECTED_SIZE ** -0.5, 1.0),
        "final_offset": bell_draw(key_of[6], (CZ,), 0.5, 3.0, (), jnp.float32),
        "amino_strand_label": jnp.searchsorted(jnp.cumsum(uneven(part_splits[7], CHAINS, WINDOW_AMINOS, WINDOW_AMINOS // 2, 1)), jnp.arange(WINDOW_AMINOS), side="right").astype(jnp.int32),
        "matched_strand_count": draw_matched_strand_count(jax.random.fold_in(jax.random.fold_in(key_of[10], part), 71), part),
        "couple_delta_adjoint": bell_draw(part_splits[9], (WINDOW_AMINOS, WINDOW_AMINOS, CZ), 1.0, 6.0, ((0, 4), (1, 4))),
    }


def standardize_entries(alignment_tensor, standard_multiplier, additive_offset):
    incoming_entries = alignment_tensor.astype(jnp.float32)
    center = incoming_entries - lax.optimization_barrier(jnp.mean(incoming_entries, axis=-1, keepdims=True))
    spread = lax.optimization_barrier(jnp.mean(center * center, axis=-1, keepdims=True))
    return (center * lax.rsqrt(spread + 1e-05) * standard_multiplier + additive_offset).astype(jnp.bfloat16)

def reference(alignment_tensor, standardizer_scaling, standardizer_offset, first_projector, second_projector, final_projector, final_offset, amino_strand_label, matched_strand_count, couple_delta_adjoint):
    standardized_entries = standardize_entries(alignment_tensor, standardizer_scaling, standardizer_offset).reshape(-1, ALIGNED_FEATS)
    first_factor = jnp.dot(standardized_entries, first_projector, preferred_element_type=jnp.float32).astype(jnp.bfloat16).reshape(ALIGNED_HOMOLOGS, WINDOW_AMINOS * PROJECTED_SIZE)
    second_factor = jnp.dot(standardized_entries, second_projector, preferred_element_type=jnp.float32).astype(jnp.bfloat16).reshape(ALIGNED_HOMOLOGS, WINDOW_AMINOS * PROJECTED_SIZE)
    chains = jnp.arange(CHAINS, dtype=jnp.int32)
    onehot = (amino_strand_label[:, None] == chains[None, :]).astype(jnp.float32)
    table = matched_strand_count.astype(jnp.float32)
    depth = jnp.dot(jnp.dot(onehot, table, precision=lax.Precision.HIGHEST), onehot.T, precision=lax.Precision.HIGHEST)
    block = WINDOW_AMINOS // N_ROW
    right_wide = second_factor.astype(jnp.float32)

    def row_block(index):
        start = (index * block).astype(jnp.int32)
        left_rows = lax.dynamic_slice_in_dim(first_factor, start * PROJECTED_SIZE, block * PROJECTED_SIZE, 1).astype(jnp.float32)
        depth_rows = lax.dynamic_slice_in_dim(depth, start, block, 0)
        grad_rows = lax.dynamic_slice_in_dim(couple_delta_adjoint, start, block, 0)
        acc = jnp.zeros((block, WINDOW_AMINOS, PROJECTED_SIZE * PROJECTED_SIZE), jnp.float32)
        for level in range(LEVELS):
            low = level * DEPTH_STEP
            prod = jnp.einsum('sa,sb->ab', left_rows[low:low + DEPTH_STEP], right_wide[low:low + DEPTH_STEP])
            prod = prod.reshape(block, PROJECTED_SIZE, WINDOW_AMINOS, PROJECTED_SIZE).transpose(0, 2, 1, 3).reshape(block, WINDOW_AMINOS, PROJECTED_SIZE * PROJECTED_SIZE)
            acc = acc + (depth_rows > low).astype(jnp.float32)[:, :, None] * prod
        outer = (acc / depth_rows[:, :, None]).astype(jnp.bfloat16)
        flat_outer = outer.reshape(-1, PROJECTED_SIZE * PROJECTED_SIZE)
        pair = (jnp.dot(flat_outer, final_projector, preferred_element_type=jnp.float32) + final_offset).astype(jnp.bfloat16)
        flat_grad = grad_rows.reshape(-1, CZ)
        back = jnp.dot(flat_grad, final_projector.T, preferred_element_type=jnp.float32).reshape(block, WINDOW_AMINOS, PROJECTED_SIZE * PROJECTED_SIZE)
        scaled = (back / depth_rows[:, :, None]).astype(jnp.bfloat16)
        weight_part = jnp.dot(flat_outer.T, flat_grad, preferred_element_type=jnp.float32)
        turned = scaled.reshape(block, WINDOW_AMINOS, PROJECTED_SIZE, PROJECTED_SIZE).transpose(0, 2, 1, 3).reshape(block * PROJECTED_SIZE, WINDOW_AMINOS * PROJECTED_SIZE).astype(jnp.float32)
        left_parts = []
        right_parts = []
        for level in range(LEVELS):
            low = level * DEPTH_STEP
            keep = (depth_rows > low).astype(jnp.float32)
            keep_wide = jnp.broadcast_to(keep[:, None, :, None], (block, PROJECTED_SIZE, WINDOW_AMINOS, PROJECTED_SIZE)).reshape(block * PROJECTED_SIZE, WINDOW_AMINOS * PROJECTED_SIZE)
            masked = turned * keep_wide
            left_parts.append(jnp.einsum('sb,ab->sa', right_wide[low:low + DEPTH_STEP], masked))
            right_parts.append(jnp.einsum('sa,ab->sb', left_rows[low:low + DEPTH_STEP], masked))
        return (pair.reshape(block, WINDOW_AMINOS, CZ), jnp.concatenate(left_parts, 0), jnp.concatenate(right_parts, 0), weight_part)
    pairs, first_factor_adjoint, right_grads, weight_parts = lax.map(row_block, jnp.arange(N_ROW, dtype=jnp.int32))
    pair_update = pairs.reshape(WINDOW_AMINOS, WINDOW_AMINOS, CZ)
    adjoint_first_factor = first_factor_adjoint.transpose(1, 0, 2).reshape(ALIGNED_HOMOLOGS, WINDOW_AMINOS * PROJECTED_SIZE).astype(jnp.bfloat16)
    grad_right = lax.optimization_barrier(jnp.sum(right_grads, axis=0)).astype(jnp.bfloat16)
    grad_w_out = lax.optimization_barrier(jnp.sum(weight_parts, axis=0)) / WINDOW_AMINOS
    return (pair_update, adjoint_first_factor, grad_right, grad_w_out)
```

```python
import functools

import jax
import jax.numpy as jnp
from jax import lax
from jax.experimental import pallas as pl
from jax.experimental.pallas import tpu as pltpu
from jax.sharding import PartitionSpec as P

PROJECTED_SIZE = 32
CZ = 128
WINDOW_AMINOS = 256
CHAINS = 8
LANES = 128
MESH = pl.DeviceIdType.MESH


def standardize_entries(alignment_tensor, standard_multiplier, additive_offset):
    incoming_entries = alignment_tensor.astype(jnp.float32)
    center = incoming_entries - jnp.mean(incoming_entries, axis=-1, keepdims=True)
    spread = jnp.mean(center * center, axis=-1, keepdims=True)
    return (center * lax.rsqrt(spread + 1e-05) * standard_multiplier + additive_offset).astype(
        jnp.bfloat16
    )


def to(source, target, send, recv, row, col):
    return pltpu.make_async_remote_copy(
        src_ref=source,
        dst_ref=target,
        send_sem=send,
        recv_sem=recv,
        device_id={"row": row, "col": col},
        device_id_type=MESH,
    )


def arrived(ref, sem):
    pltpu.make_async_copy(ref, ref, sem).wait()


def greet(n_row, n_col, me):
    peers = n_row * n_col
    barrier = pltpu.get_barrier_semaphore()

    def signal(off, carry):
        peer = (me + off) % peers
        pl.semaphore_signal(
            barrier,
            inc=1,
            device_id={"row": peer // n_col, "col": peer % n_col},
            device_id_type=MESH,
        )
        return carry

    lax.fori_loop(1, peers, signal, 0)
    pl.semaphore_wait(barrier, peers - 1)


def gather_kernel(
    n_row, n_col, ratio,
    left_ref, right_ref,
    left_out, right_out,
    left_send, left_recv, right_send, right_recv, hop_send, twin_send, own_sem,
):
    row, col = lax.axis_index("row"), lax.axis_index("col")
    share = left_ref.shape[0]
    greet(n_row, n_col, row * n_col + col)
    block = lambda ref, index: ref.at[pl.ds(pl.multiple_of(index * share, share), share)]
    owner = col // ratio
    twin = row + 1 - 2 * (row % 2)
    chips = n_row // 2

    def right_copy(t):
        return to(
            right_ref.at[t], block(right_out, col), right_send.at[t], right_recv.at[col],
            row, row * ratio + t,
        )

    def left_copy(off):
        peer = (col + off) % n_col
        return to(left_ref, block(left_out, col), left_send.at[off], left_recv.at[col], row, peer)

    def hop_copy(source, index, hop):
        return to(
            source, block(right_out, index), hop_send.at[index, hop], right_recv.at[index],
            (row + 2 * hop) % n_row, col,
        )

    def twin_copy(source, index):
        return to(
            source, block(right_out, index), twin_send.at[index], right_recv.at[index], twin, col
        )

    own_left = pltpu.make_async_copy(left_ref, block(left_out, col), own_sem.at[0])
    own_left.start()
    for t in range(ratio):
        pl.when(row * ratio + t != col)(right_copy(t).start)
    mine = right_ref.at[col % ratio]
    own_right = pltpu.make_async_copy(mine, block(right_out, col), own_sem.at[1])

    @pl.when(row == owner)
    def _():
        own_right.start()
        for hop in range(1, chips):
            hop_copy(mine, col, hop).start()
        twin_copy(mine, col).start()

    for off in range(1, n_col):
        left_copy(off).start()

    @pl.when(row == owner)
    def _():
        own_right.wait()
        for off in range(1, n_col):
            peer = (col + off) % n_col
            source = block(right_out, peer)
            arrived(source, right_recv.at[peer])
            for hop in range(1, chips):
                hop_copy(source, peer, hop).start()
            twin_copy(source, peer).start()

    relays = jnp.logical_and(row != owner, row % 2 == owner % 2)

    @pl.when(relays)
    def _():
        for off in range(n_col):
            peer = (col + off) % n_col
            source = block(right_out, peer)
            arrived(source, right_recv.at[peer])
            twin_copy(source, peer).start()

    @pl.when(row % 2 != owner % 2)
    def _():
        for off in range(n_col):
            peer = (col + off) % n_col
            arrived(block(right_out, peer), right_recv.at[peer])

    own_left.wait()
    for off in range(1, n_col):
        peer = (col + off) % n_col
        arrived(block(left_out, peer), left_recv.at[peer])
    for off in range(1, n_col):
        left_copy(off).wait_send()
    for t in range(ratio):
        pl.when(row * ratio + t != col)(right_copy(t).wait_send)

    @pl.when(row == owner)
    def _():
        for off in range(n_col):
            peer = (col + off) % n_col
            for hop in range(1, chips):
                hop_copy(block(right_out, peer), peer, hop).wait_send()

    @pl.when(row % 2 == owner % 2)
    def _():
        for off in range(n_col):
            peer = (col + off) % n_col
            twin_copy(block(right_out, peer), peer).wait_send()


def pair_kernel(
    tile, cols, seqs,
    labels_ref,
    left_ref, right_ref, table_ref, chain_ref, inverse_ref, grad_ref, weight_ref, weight_t_ref,
    bias_ref,
    pair_ref, left_grad_ref, right_grad_ref, weight_grad_ref,
    kept, kept_t, spread, scaled, outer, acc, left_acc, right_acc, weight_acc, slots,
):
    step = pl.program_id(0)
    size = PROJECTED_SIZE
    inner = LANES // cols
    blocks = size // inner
    width = 2 * LANES if blocks % 2 == 0 else LANES
    f32, bf16 = jnp.float32, jnp.bfloat16
    seq = lax.broadcasted_iota(jnp.int32, (seqs, LANES), 0).astype(f32)

    @pl.when(step == 0)
    def _():
        spread[...] = jnp.zeros_like(spread)
        right_acc[...] = jnp.zeros_like(right_acc)
        weight_acc[...] = jnp.zeros_like(weight_acc)

        def fill(chain, carry):
            keep = jnp.where(seq < table_ref[pl.ds(chain, 1), :], 1.0, 0.0).astype(bf16)
            for b in range(blocks):
                lanes = slice(b * LANES, (b + 1) * LANES)
                piece = right_ref[:, lanes] * keep
                kept[chain, :, lanes] = piece
                kept_t[chain, lanes, :] = piece.T
            return carry

        lax.fori_loop(labels_ref[0], labels_ref[labels_ref.shape[0] - 1] + 2, fill, 0)

    for i in range(tile):
        grad = grad_ref[i * cols : (i + 1) * cols, :]
        for e in range(inner):
            spread[i * LANES + e * cols : i * LANES + (e + 1) * cols, e * CZ : (e + 1) * CZ] = grad
    inverse = [inverse_ref[i : i + 1, :] for i in range(tile)]
    for i in range(0, tile, 2):
        back = lax.dot_general(
            weight_ref[...], spread[i * LANES : (i + 2) * LANES, :], (((1,), (1,)), ((), ())),
            preferred_element_type=f32,
        )
        for k in range(2):
            part = (back[:, k * LANES : (k + 1) * LANES] * inverse[i + k]).astype(bf16)
            for b in range(blocks):
                scaled[(i + k) * size : (i + k + 1) * size, b * LANES : (b + 1) * LANES] = part[
                    b * size : (b + 1) * size
                ]

    low = labels_ref[step * tile]
    high = labels_ref[step * tile + tile - 1]

    def chain_pair(first, chain):
        left = left_ref[...]
        lane = chain_ref[0]
        for k in range(2):
            slots[k * seqs : (k + 1) * seqs, :] = left * jnp.where(
                lane == (chain + k).astype(f32), 1.0, 0.0
            ).astype(bf16)
        both = slots[...]
        both_t = both.T
        keep = [seq < table_ref[pl.ds(chain + k, 1), :] for k in range(2)]
        for start in range(0, blocks * LANES, width):
            lanes = slice(start, start + width)
            right = kept[pl.ds(chain, 2), :, lanes].reshape(2 * seqs, width)
            prod = jnp.dot(both_t, right, preferred_element_type=f32)
            if first:
                acc[:, lanes] = prod
            else:
                acc[:, lanes] += prod
            out = jnp.dot(both, scaled[:, lanes], preferred_element_type=f32)
            for b in range(width // LANES):
                part = slice(b * LANES, (b + 1) * LANES)
                right_acc[:, start + b * LANES : start + (b + 1) * LANES] += jnp.where(
                    keep[0], out[:seqs, part], 0.0
                ) + jnp.where(keep[1], out[seqs:, part], 0.0)
        right_t = jnp.concatenate([kept_t[chain], kept_t[chain + 1]], axis=1)
        out = jnp.dot(scaled[...], right_t, preferred_element_type=f32)
        for i in range(tile):
            label = labels_ref[step * tile + i]
            rows = slice(i * size, (i + 1) * size)
            part = jnp.where(label == chain, out[rows, :seqs], 0.0) + jnp.where(
                label == chain + 1, out[rows, seqs:], 0.0
            )
            if first:
                left_acc[rows, :] = part
            else:
                left_acc[rows, :] += part

    chain_pair(True, low)

    def more(p, carry):
        chain_pair(False, low + 2 * p)
        return carry

    lax.fori_loop(1, (high - low) // 2 + 1, more, 0)
    left_grad_ref[...] = left_acc[...].T.astype(bf16)
    for i in range(tile):
        for b in range(blocks):
            outer[b * size : (b + 1) * size, i * LANES : (i + 1) * LANES] = (
                acc[i * size : (i + 1) * size, b * LANES : (b + 1) * LANES] * inverse[i]
            ).astype(bf16)
    lane = lax.broadcasted_iota(jnp.int32, (CZ, LANES), 1) // cols
    for i in range(0, tile, 2):
        both = jnp.dot(
            weight_t_ref[...], outer[:, i * LANES : (i + 2) * LANES], preferred_element_type=f32
        )
        for k in range(2):
            lanes = slice(k * LANES, (k + 1) * LANES)
            total = both[:CZ, lanes]
            for e in range(1, inner):
                total = jnp.where(lane == e, both[e * CZ : (e + 1) * CZ, lanes], total)
            turned = total.T
            pair = turned[:cols]
            for e in range(1, inner):
                pair = pair + turned[e * cols : (e + 1) * cols]
            pair_ref[(i + k) * cols : (i + k + 1) * cols, :] = (pair + bias_ref[...]).astype(bf16)
    weight_acc[...] += jnp.dot(outer[...], spread[...], preferred_element_type=f32)

    @pl.when(step == pl.num_programs(0) - 1)
    def _():
        right_grad_ref[...] = right_acc[...].astype(bf16)
        rows = blocks * size
        for e in range(inner):
            weight_grad_ref[e * rows : (e + 1) * rows, :] = weight_acc[
                :, e * CZ : (e + 1) * CZ
            ].astype(bf16)


def sum_kernel(
    n_row, n_col, ratio,
    left_ref, right_ref, weight_ref,
    left_out, right_out, weight_out,
    left_in, right_mid, right_sum, right_in, weight_mid, weight_sum, weight_in, weight_part,
    weight_all,
    left_send, left_recv, mid_send, mid_recv, right_send, right_recv,
    w1_send, w1_recv, w2_send, w2_recv, w3_send, w3_recv, w4_send, w4_recv,
):
    f32, bf16 = jnp.float32, jnp.bfloat16
    row, col = lax.axis_index("row"), lax.axis_index("col")
    greet(n_row, n_col, row * n_col + col)
    many = n_col // n_row
    quarter = weight_ref.shape[0] // n_row
    piece = quarter // n_col
    owner, slot = col // ratio, col % ratio
    rows_of = lambda index, extent: pl.ds(pl.multiple_of(index * extent, extent), extent)

    def w1_copy(off):
        peer = (row + off) % n_row
        return to(
            weight_ref.at[rows_of(peer, quarter)], weight_mid.at[row], w1_send.at[off],
            w1_recv.at[row], peer, col,
        )

    def mid_copy(off):
        peer = (row + off) % n_row
        return to(
            right_ref.at[rows_of(peer, many)], right_mid.at[row], mid_send.at[off],
            mid_recv.at[row], peer, col,
        )

    def left_copy(off):
        peer = (col + off) % n_col
        return to(
            left_ref.at[peer], left_in.at[col], left_send.at[off], left_recv.at[col], row, peer
        )

    def right_copy(b):
        return to(
            right_sum.at[b], right_in.at[slot, row], right_send.at[b],
            right_recv.at[slot, row], owner, row * many + b,
        )

    def w2_copy(off):
        peer = (col + off) % n_col
        return to(
            weight_sum.at[rows_of(peer, piece)], weight_in.at[col], w2_send.at[off],
            w2_recv.at[col], row, peer,
        )

    def w3_copy(off):
        peer = (col + off) % n_col
        return to(
            weight_part, weight_all.at[rows_of(row * n_col + col, piece)], w3_send.at[off],
            w3_recv.at[col], row, peer,
        )

    def w4_copy(off):
        peer = (row + off) % n_row
        mine = weight_all.at[rows_of(row, quarter)]
        return to(mine, mine, w4_send.at[off], w4_recv.at[row], peer, col)

    for off in range(1, n_row):
        w1_copy(off).start()
    for off in range(1, n_row):
        mid_copy(off).start()
    late = n_col - 1
    for off in range(1, late):
        left_copy(off).start()

    own = weight_ref[rows_of(row, quarter), :].astype(f32)
    for off in range(1, n_row):
        peer = (row + off) % n_row
        arrived(weight_mid.at[peer], w1_recv.at[peer])
        own = own + weight_mid[peer].astype(f32)
    weight_sum[...] = own.astype(bf16)
    for off in range(1, n_col):
        w2_copy(off).start()
    left_copy(late).start()

    total = right_ref[rows_of(row, many)].astype(f32)
    for off in range(1, n_row):
        peer = (row + off) % n_row
        arrived(right_mid.at[peer], mid_recv.at[peer])
        total = total + right_mid[peer].astype(f32)
    right_sum[...] = total.astype(bf16)
    for b in range(many):
        here = jnp.logical_and(owner == row, row * many + b == col)
        pl.when(jnp.logical_not(here))(right_copy(b).start)
        pl.when(here)(
            pltpu.make_async_copy(
                right_sum.at[b], right_in.at[slot, row], right_recv.at[slot, row]
            ).start
        )

    own = weight_sum[rows_of(col, piece), :].astype(f32)
    for off in range(1, n_col):
        peer = (col + off) % n_col
        arrived(weight_in.at[peer], w2_recv.at[peer])
        own = own + weight_in[peer].astype(f32)
    weight_part[...] = own.astype(bf16)
    weight_all[rows_of(row * n_col + col, piece), :] = own.astype(bf16)
    for off in range(1, n_col):
        w3_copy(off).start()
    for off in range(1, n_col):
        peer = (col + off) % n_col
        arrived(weight_all.at[rows_of(row * n_col + peer, piece)], w3_recv.at[peer])
    for off in range(1, n_row):
        w4_copy(off).start()

    total = left_ref[col].astype(f32)
    for off in range(1, n_col):
        peer = (col + off) % n_col
        arrived(left_in.at[peer], left_recv.at[peer])
        total = total + left_in[peer].astype(f32)
    left_out[...] = total.astype(bf16)
    for t in range(ratio):
        source = col // many
        arrived(right_in.at[t, source], right_recv.at[t, source])
        right_out[t] = right_in[t, source]
    for off in range(1, n_row):
        peer = (row + off) % n_row
        arrived(weight_all.at[rows_of(peer, quarter)], w4_recv.at[peer])
    weight_out[...] = weight_all[...].astype(f32) * (1.0 / WINDOW_AMINOS)

    for off in range(1, n_row):
        w1_copy(off).wait_send()
        mid_copy(off).wait_send()
        w4_copy(off).wait_send()
    for off in range(1, n_col):
        left_copy(off).wait_send()
        w2_copy(off).wait_send()
        w3_copy(off).wait_send()
    for b in range(many):
        here = jnp.logical_and(owner == row, row * many + b == col)
        pl.when(jnp.logical_not(here))(right_copy(b).wait_send)


def shards(
    alignment_tensor,
    standardizer_scaling,
    standardizer_offset,
    first_projector,
    second_projector,
    final_projector,
    final_offset,
    amino_strand_label,
    matched_strand_count,
    couple_delta_adjoint,
):
    f32, bf16 = jnp.float32, jnp.bfloat16
    share, rows, feats = alignment_tensor.shape
    cols = couple_delta_adjoint.shape[1]
    size = PROJECTED_SIZE
    n_row, n_col = lax.axis_size("row"), lax.axis_size("col")
    ratio = rows // cols
    seqs = share * n_col
    inner = LANES // cols
    blocks = size // inner
    wide = size * cols
    vmem = pl.BlockSpec(memory_space=pltpu.VMEM)
    dma = pltpu.SemaphoreType.DMA

    entries = standardize_entries(
        alignment_tensor, standardizer_scaling, standardizer_offset
    ).reshape(-1, feats)
    both = jnp.dot(
        entries,
        jnp.concatenate([first_projector, second_projector], axis=1),
        preferred_element_type=f32,
    ).astype(bf16)
    left_own = both[:, :size].reshape(share, rows * size)
    right_own = (
        both[:, size:]
        .reshape(share, ratio, cols, size)
        .transpose(1, 0, 3, 2)
        .reshape(ratio, share, wide)
    )
    left_panel, right_panel = pl.pallas_call(
        functools.partial(gather_kernel, n_row, n_col, ratio),
        in_specs=[vmem] * 2,
        out_specs=[vmem] * 2,
        out_shape=[
            jax.ShapeDtypeStruct((seqs, rows * size), bf16),
            jax.ShapeDtypeStruct((seqs, wide), bf16),
        ],
        scratch_shapes=[
            dma((n_col,)), dma((n_col,)), dma((ratio,)), dma((n_col,)),
            dma((n_col, n_row // 2)), dma((n_col,)), dma((2,)),
        ],
        compiler_params=pltpu.CompilerParams(collective_id=0, has_side_effects=True),
    )(left_own, right_own)

    row_labels = lax.dynamic_slice_in_dim(
        amino_strand_label, lax.axis_index("row") * rows, rows, 0
    )
    col_labels = lax.dynamic_slice_in_dim(
        amino_strand_label, lax.axis_index("col") * cols, cols, 0
    )
    chains = jnp.arange(CHAINS, dtype=jnp.int32)
    row_hot = (row_labels[:, None] == chains[None, :]).astype(f32)
    col_hot = (col_labels[:, None] == chains[None, :]).astype(f32)
    by_chain = jnp.dot(
        matched_strand_count.astype(f32), col_hot.T, precision=lax.Precision.HIGHEST
    )
    depth = jnp.dot(row_hot, by_chain, precision=lax.Precision.HIGHEST)
    table = jnp.pad(jnp.tile(by_chain, (1, inner)), ((0, CHAINS), (0, 0)))
    inverse = jnp.tile(1.0 / depth, (1, inner))
    tile = 8
    steps = rows // tile
    chain_lanes = jnp.repeat(row_labels.astype(f32), size).reshape(steps, 1, tile * size)
    weight = (
        final_projector.reshape(size, blocks, inner, CZ)
        .transpose(1, 0, 2, 3)
        .reshape(blocks * size, inner * CZ)
    )
    flat_grad = couple_delta_adjoint.reshape(-1, CZ)
    whole = lambda shape: pl.BlockSpec(shape, lambda g, labels: (0,) * len(shape))
    pair, left_grad, right_grad, weight_part = pl.pallas_call(
        functools.partial(pair_kernel, tile, cols, seqs),
        grid_spec=pltpu.PrefetchScalarGridSpec(
            num_scalar_prefetch=1,
            grid=(steps,),
            in_specs=[
                pl.BlockSpec((seqs, tile * size), lambda g, labels: (0, g)),
                whole((seqs, wide)),
                whole((2 * CHAINS, LANES)),
                pl.BlockSpec((1, 1, tile * size), lambda g, labels: (g, 0, 0)),
                pl.BlockSpec((tile, LANES), lambda g, labels: (g, 0)),
                pl.BlockSpec((tile * cols, CZ), lambda g, labels: (g, 0)),
                whole((blocks * size, inner * CZ)),
                whole((inner * CZ, blocks * size)),
                whole((1, CZ)),
            ],
            out_specs=[
                pl.BlockSpec((tile * cols, CZ), lambda g, labels: (g, 0)),
                pl.BlockSpec((seqs, tile * size), lambda g, labels: (0, g)),
                whole((seqs, wide)),
                whole((size * size, CZ)),
            ],
            scratch_shapes=[
                pltpu.VMEM((CHAINS + 1, seqs, wide), bf16),
                pltpu.VMEM((CHAINS + 1, wide, seqs), bf16),
                pltpu.VMEM((tile * LANES, inner * CZ), bf16),
                pltpu.VMEM((tile * size, wide), bf16),
                pltpu.VMEM((blocks * size, tile * LANES), bf16),
                pltpu.VMEM((tile * size, wide), f32),
                pltpu.VMEM((tile * size, seqs), f32),
                pltpu.VMEM((seqs, wide), f32),
                pltpu.VMEM((blocks * size, inner * CZ), f32),
                pltpu.VMEM((2 * seqs, tile * size), bf16),
            ],
        ),
        out_shape=[
            jax.ShapeDtypeStruct((rows * cols, CZ), bf16),
            jax.ShapeDtypeStruct((seqs, rows * size), bf16),
            jax.ShapeDtypeStruct((seqs, wide), bf16),
            jax.ShapeDtypeStruct((size * size, CZ), bf16),
        ],
        compiler_params=pltpu.CompilerParams(
            dimension_semantics=("arbitrary",), vmem_limit_bytes=56 * 1024 * 1024
        ),
    )(
        row_labels,
        left_panel,
        right_panel,
        table,
        chain_lanes,
        inverse,
        flat_grad,
        weight,
        weight.T,
        final_offset[None, :],
    )
    pair_update = pair.reshape(rows, cols, CZ)
    many = n_col // n_row
    quarter = size * size // n_row
    piece = quarter // n_col
    adjoint_first_factor, right_sum, weight_total = pl.pallas_call(
        functools.partial(sum_kernel, n_row, n_col, ratio),
        in_specs=[vmem] * 3,
        out_specs=[vmem] * 3,
        out_shape=[
            jax.ShapeDtypeStruct((share, rows * size), bf16),
            jax.ShapeDtypeStruct((ratio, share, wide), bf16),
            jax.ShapeDtypeStruct((size * size, CZ), f32),
        ],
        scratch_shapes=[
            pltpu.VMEM((n_col, share, rows * size), bf16),
            pltpu.VMEM((n_row, many, share, wide), bf16),
            pltpu.VMEM((many, share, wide), bf16),
            pltpu.VMEM((ratio, n_row, share, wide), bf16),
            pltpu.VMEM((n_row, quarter, CZ), bf16),
            pltpu.VMEM((quarter, CZ), bf16),
            pltpu.VMEM((n_col, piece, CZ), bf16),
            pltpu.VMEM((piece, CZ), bf16),
            pltpu.VMEM((size * size, CZ), bf16),
            dma((n_col,)), dma((n_col,)),
            dma((n_row,)), dma((n_row,)),
            dma((many,)), dma((ratio, n_row)),
            dma((n_row,)), dma((n_row,)),
            dma((n_col,)), dma((n_col,)),
            dma((n_col,)), dma((n_col,)),
            dma((n_row,)), dma((n_row,)),
        ],
        compiler_params=pltpu.CompilerParams(collective_id=1, has_side_effects=True),
    )(
        left_grad.reshape(n_col, share, rows * size),
        right_grad.reshape(n_col, share, wide),
        weight_part,
    )
    grad_right = (
        right_sum.reshape(ratio, share, size, cols)
        .transpose(1, 0, 3, 2)
        .reshape(share, rows * size)
    )
    grad_w_out = (
        weight_total.reshape(inner, blocks, size, CZ).transpose(2, 1, 0, 3).reshape(size * size, CZ)
    )
    return (pair_update, adjoint_first_factor, grad_right, grad_w_out)


def solution(mesh):
    in_specs = (
        P(("parts", "col"), "row", None),
        P(),
        P(),
        P(),
        P(),
        P(),
        P(),
        P("parts"),
        P("parts", None),
        P(("parts", "row"), "col", None),
    )
    out_specs = (
        P(("parts", "row"), "col", None),
        P(("parts", "col"), "row"),
        P(("parts", "col"), "row"),
        P("parts", None),
    )
    return jax.shard_map(shards, mesh=mesh, in_specs=in_specs, out_specs=out_specs, check_vma=False)
```

```python
import functools

import jax
import jax.numpy as jnp
from jax import lax
from jax.experimental import pallas as pl
from jax.experimental.pallas import tpu as pltpu
from jax.sharding import PartitionSpec as P

PROJECTED_SIZE = 32
CZ = 128
WINDOW_AMINOS = 256
CHAINS = 8
LANES = 128
MESH = pl.DeviceIdType.MESH


def standardize_entries(alignment_tensor, standard_multiplier, additive_offset):
    incoming_entries = alignment_tensor.astype(jnp.float32)
    center = incoming_entries - jnp.mean(incoming_entries, axis=-1, keepdims=True)
    spread = jnp.mean(center * center, axis=-1, keepdims=True)
    return (center * lax.rsqrt(spread + 1e-05) * standard_multiplier + additive_offset).astype(
        jnp.bfloat16
    )


def to(source, target, send, recv, row, col):
    return pltpu.make_async_remote_copy(
        src_ref=source,
        dst_ref=target,
        send_sem=send,
        recv_sem=recv,
        device_id={"row": row, "col": col},
        device_id_type=MESH,
    )


def arrived(ref, sem):
    pltpu.make_async_copy(ref, ref, sem).wait()


def greet(n_row, n_col, me):
    peers = n_row * n_col
    barrier = pltpu.get_barrier_semaphore()

    def signal(off, carry):
        peer = (me + off) % peers
        pl.semaphore_signal(
            barrier,
            inc=1,
            device_id={"row": peer // n_col, "col": peer % n_col},
            device_id_type=MESH,
        )
        return carry

    lax.fori_loop(1, peers, signal, 0)
    pl.semaphore_wait(barrier, peers - 1)


def gather_kernel(
    n_row, n_col, ratio,
    left_ref, right_ref,
    left_out, right_out,
    up_send, down_send, left_recv, right_send, right_recv, hop_send, twin_send, own_sem,
):
    row, col = lax.axis_index("row"), lax.axis_index("col")
    share = left_ref.shape[0]
    parts = left_recv.shape[1]
    part = left_ref.shape[1] // parts
    greet(n_row, n_col, row * n_col + col)
    rows_of = lambda index: pl.ds(pl.multiple_of(index * share, share), share)
    block = lambda ref, index: ref.at[rows_of(index)]
    owner = col // ratio
    twin = row + 1 - 2 * (row % 2)
    chips = n_row // 2
    is_owner = row == owner
    same_side = row % 2 == owner % 2

    def right_copy(t):
        return to(
            right_ref.at[t], block(right_out, col), right_send.at[t], right_recv.at[col],
            row, row * ratio + t,
        )

    def left_part(index, h):
        return left_out.at[rows_of(index), h * part : (h + 1) * part]

    def left_copy(index, h, step, own=False):
        sends = up_send if step > 0 else down_send
        source = left_ref.at[:, h * part : (h + 1) * part] if own else left_part(index, h)
        return to(
            source, left_part(index, h), sends.at[index, h], left_recv.at[index, h],
            row, (col + step) % n_col,
        )

    def hop_copy(source, index, hop):
        return to(
            source, block(right_out, index), hop_send.at[index, hop], right_recv.at[index],
            (row + 2 * hop) % n_row, col,
        )

    def twin_copy(source, index):
        return to(
            source, block(right_out, index), twin_send.at[index], right_recv.at[index], twin, col
        )

    has_up, has_down = col + 1 < n_col, col > 0
    for t in range(ratio):
        pl.when(row * ratio + t != col)(right_copy(t).start)
    for h in range(parts):
        pl.when(has_up)(left_copy(col, h, 1, True).start)
        pl.when(has_down)(left_copy(col, h, -1, True).start)
    own_left = pltpu.make_async_copy(left_ref, block(left_out, col), own_sem.at[0])
    own_left.start()
    mine = right_ref.at[col % ratio]
    own_right = pltpu.make_async_copy(mine, block(right_out, col), own_sem.at[1])

    @pl.when(is_owner)
    def _():
        own_right.start()
        for hop in range(1, chips):
            hop_copy(mine, col, hop).start()
        twin_copy(mine, col).start()

    def pass_left(k):
        for h in range(parts):
            for step, there in ((1, col - k), (-1, col + k)):
                here = there >= 0 if step > 0 else there < n_col
                index = there % n_col

                @pl.when(here)
                def _(index=index, h=h):
                    arrived(left_part(index, h), left_recv.at[index, h])

                on = jnp.logical_and(here, has_up if step > 0 else has_down)
                pl.when(on)(left_copy(index, h, step).start)

    def pass_right(k):
        for there in (col - k, col + k) if k else (col,):
            index = there % n_col
            source = block(right_out, index)
            here = jnp.logical_and(there >= 0, there < n_col)

            @pl.when(jnp.logical_and(here, jnp.logical_not(jnp.logical_and(is_owner, k == 0))))
            def _(index=index, source=source):
                arrived(source, right_recv.at[index])

            if k:

                @pl.when(jnp.logical_and(here, is_owner))
                def _(index=index, source=source):
                    for hop in range(1, chips):
                        hop_copy(source, index, hop).start()

            relay = same_side if k else jnp.logical_and(same_side, jnp.logical_not(is_owner))
            pl.when(jnp.logical_and(here, relay))(twin_copy(source, index).start)

    for k in range(1, n_col - 1):
        pass_left(k)
        if k == 1:
            pass_right(0)
        pass_right(k)
    pass_right(n_col - 1)
    pass_left(n_col - 1)

    own_left.wait()
    pl.when(is_owner)(own_right.wait)
    for t in range(ratio):
        pl.when(row * ratio + t != col)(right_copy(t).wait_send)
    for index in range(n_col):
        for h in range(parts):
            pl.when(jnp.logical_and(has_up, index <= col))(left_copy(index, h, 1).wait_send)
            pl.when(jnp.logical_and(has_down, index >= col))(left_copy(index, h, -1).wait_send)

        @pl.when(is_owner)
        def _(index=index):
            for hop in range(1, chips):
                hop_copy(block(right_out, index), index, hop).wait_send()

        pl.when(same_side)(twin_copy(block(right_out, index), index).wait_send)


def pair_kernel(
    tile, cols, seqs,
    labels_ref,
    left_ref, right_ref, table_ref, chain_ref, inverse_ref, grad_ref, weight_ref, weight_t_ref,
    bias_ref,
    pair_ref, left_grad_ref, right_grad_ref, weight_grad_ref,
    kept, kept_t, spread, scaled, outer, acc, left_acc, right_acc, weight_acc, slots,
):
    step = pl.program_id(0)
    size = PROJECTED_SIZE
    inner = LANES // cols
    blocks = size // inner
    width = 2 * LANES if blocks % 2 == 0 else LANES
    f32, bf16 = jnp.float32, jnp.bfloat16
    seq = lax.broadcasted_iota(jnp.int32, (seqs, LANES), 0).astype(f32)

    @pl.when(step == 0)
    def _():
        spread[...] = jnp.zeros_like(spread)
        right_acc[...] = jnp.zeros_like(right_acc)
        weight_acc[...] = jnp.zeros_like(weight_acc)

        def fill(chain, carry):
            keep = jnp.where(seq < table_ref[pl.ds(chain, 1), :], 1.0, 0.0).astype(bf16)
            for b in range(blocks):
                lanes = slice(b * LANES, (b + 1) * LANES)
                piece = right_ref[:, lanes] * keep
                kept[chain, :, lanes] = piece
                kept_t[chain, lanes, :] = piece.T
            return carry

        lax.fori_loop(labels_ref[0], labels_ref[labels_ref.shape[0] - 1] + 2, fill, 0)

    for i in range(tile):
        grad = grad_ref[i * cols : (i + 1) * cols, :]
        for e in range(inner):
            spread[i * LANES + e * cols : i * LANES + (e + 1) * cols, e * CZ : (e + 1) * CZ] = grad
    inverse = [inverse_ref[i : i + 1, :] for i in range(tile)]
    for i in range(0, tile, 2):
        back = lax.dot_general(
            weight_ref[...], spread[i * LANES : (i + 2) * LANES, :], (((1,), (1,)), ((), ())),
            preferred_element_type=f32,
        )
        for k in range(2):
            part = (back[:, k * LANES : (k + 1) * LANES] * inverse[i + k]).astype(bf16)
            for b in range(blocks):
                scaled[(i + k) * size : (i + k + 1) * size, b * LANES : (b + 1) * LANES] = part[
                    b * size : (b + 1) * size
                ]

    low = labels_ref[step * tile]
    high = labels_ref[step * tile + tile - 1]

    def chain_pair(first, chain):
        left = left_ref[...]
        lane = chain_ref[0]
        for k in range(2):
            slots[k * seqs : (k + 1) * seqs, :] = left * jnp.where(
                lane == (chain + k).astype(f32), 1.0, 0.0
            ).astype(bf16)
        both = slots[...]
        both_t = both.T
        keep = [seq < table_ref[pl.ds(chain + k, 1), :] for k in range(2)]
        for start in range(0, blocks * LANES, width):
            lanes = slice(start, start + width)
            right = kept[pl.ds(chain, 2), :, lanes].reshape(2 * seqs, width)
            prod = jnp.dot(both_t, right, preferred_element_type=f32)
            if first:
                acc[:, lanes] = prod
            else:
                acc[:, lanes] += prod
            out = jnp.dot(both, scaled[:, lanes], preferred_element_type=f32)
            for b in range(width // LANES):
                part = slice(b * LANES, (b + 1) * LANES)
                right_acc[:, start + b * LANES : start + (b + 1) * LANES] += jnp.where(
                    keep[0], out[:seqs, part], 0.0
                ) + jnp.where(keep[1], out[seqs:, part], 0.0)
        right_t = jnp.concatenate([kept_t[chain], kept_t[chain + 1]], axis=1)
        out = jnp.dot(scaled[...], right_t, preferred_element_type=f32)
        for i in range(tile):
            label = labels_ref[step * tile + i]
            rows = slice(i * size, (i + 1) * size)
            part = jnp.where(label == chain, out[rows, :seqs], 0.0) + jnp.where(
                label == chain + 1, out[rows, seqs:], 0.0
            )
            if first:
                left_acc[rows, :] = part
            else:
                left_acc[rows, :] += part

    chain_pair(True, low)

    def more(p, carry):
        chain_pair(False, low + 2 * p)
        return carry

    lax.fori_loop(1, (high - low) // 2 + 1, more, 0)
    left_grad_ref[...] = left_acc[...].T.astype(bf16)
    for i in range(tile):
        for b in range(blocks):
            outer[b * size : (b + 1) * size, i * LANES : (i + 1) * LANES] = (
                acc[i * size : (i + 1) * size, b * LANES : (b + 1) * LANES] * inverse[i]
            ).astype(bf16)
    lane = lax.broadcasted_iota(jnp.int32, (CZ, LANES), 1) // cols
    for i in range(0, tile, 2):
        both = jnp.dot(
            weight_t_ref[...], outer[:, i * LANES : (i + 2) * LANES], preferred_element_type=f32
        )
        for k in range(2):
            lanes = slice(k * LANES, (k + 1) * LANES)
            total = both[:CZ, lanes]
            for e in range(1, inner):
                total = jnp.where(lane == e, both[e * CZ : (e + 1) * CZ, lanes], total)
            turned = total.T
            pair = turned[:cols]
            for e in range(1, inner):
                pair = pair + turned[e * cols : (e + 1) * cols]
            pair_ref[(i + k) * cols : (i + k + 1) * cols, :] = (pair + bias_ref[...]).astype(bf16)
    weight_acc[...] += jnp.dot(outer[...], spread[...], preferred_element_type=f32)

    @pl.when(step == pl.num_programs(0) - 1)
    def _():
        right_grad_ref[...] = right_acc[...].astype(bf16)
        rows = blocks * size
        for e in range(inner):
            weight_grad_ref[e * rows : (e + 1) * rows, :] = weight_acc[
                :, e * CZ : (e + 1) * CZ
            ].astype(bf16)


def sum_kernel(
    n_row, n_col, ratio,
    left_ref, right_ref, weight_ref,
    left_out, right_out, weight_out,
    up_in, down_in, right_twin, right_half, right_mid, right_sum, right_in,
    weight_mid, weight_sum, weight_in, weight_part, weight_all,
    up_send, up_recv, down_send, down_recv, twin_send, twin_recv, mid_send, mid_recv,
    right_send, right_recv,
    w1_send, w1_recv, w2_send, w2_recv, w3_send, w3_recv, w4_send, w4_recv,
):
    f32, bf16 = jnp.float32, jnp.bfloat16
    row, col = lax.axis_index("row"), lax.axis_index("col")
    greet(n_row, n_col, row * n_col + col)
    chips = n_row // 2
    chip, side = row // 2, row % 2
    twin = row + 1 - 2 * side
    many = n_col // n_row
    half = n_col // 2
    quarter = weight_ref.shape[0] // n_row
    piece = quarter // n_col
    parts = up_recv.shape[1]
    part = left_ref.shape[2] // parts
    owner, slot = col // ratio, col % ratio
    rows_of = lambda index, extent: pl.ds(pl.multiple_of(index * extent, extent), extent)
    mine = side * chips + chip
    has_up, has_down = col + 1 < n_col, col > 0

    def w1_copy(off):
        peer = (row + off) % n_row
        return to(
            weight_ref.at[rows_of(peer, quarter)], weight_mid.at[row], w1_send.at[off],
            w1_recv.at[row], peer, col,
        )

    twin_copy = to(
        right_ref.at[rows_of(1 - side, half)], right_twin, twin_send, twin_recv, twin, col
    )

    def mid_copy(off):
        peer = (chip + off) % chips
        return to(
            right_half.at[rows_of(peer, many)], right_mid.at[chip], mid_send.at[off],
            mid_recv.at[chip], 2 * peer + side, col,
        )

    def right_copy(b):
        return to(
            right_sum.at[b], right_in.at[slot], right_send.at[b], right_recv.at[slot],
            owner, mine * many + b,
        )

    def left_copy(index, h, step, own=False):
        lanes = slice(h * part, (h + 1) * part)
        buffer, send, recv = (
            (up_in, up_send, up_recv) if step > 0 else (down_in, down_send, down_recv)
        )
        source = (left_ref if own else buffer).at[index, :, lanes]
        return to(
            source, buffer.at[index, :, lanes], send.at[index, h], recv.at[index, h],
            row, (col + step) % n_col,
        )

    def w2_copy(off):
        peer = (col + off) % n_col
        return to(
            weight_sum.at[rows_of(peer, piece)], weight_in.at[col], w2_send.at[off],
            w2_recv.at[col], row, peer,
        )

    def w3_copy(off):
        peer = (col + off) % n_col
        return to(
            weight_part, weight_all.at[rows_of(row * n_col + col, piece)], w3_send.at[off],
            w3_recv.at[col], row, peer,
        )

    def w4_copy(off):
        peer = (row + off) % n_row
        own = weight_all.at[rows_of(row, quarter)]
        return to(own, own, w4_send.at[off], w4_recv.at[row], peer, col)

    def left_own(index, step):
        end = col == 0 if step > 0 else col == n_col - 1
        for h in range(parts):
            pl.when(end)(left_copy(index, h, step, True).start)

    def left_pass(index, step):
        buffer, recv = (up_in, up_recv) if step > 0 else (down_in, down_recv)
        if step > 0:
            on = jnp.logical_and(col > 0, col < index)
        else:
            on = jnp.logical_and(col < n_col - 1, col > index)
        for h in range(parts):
            lanes = slice(h * part, (h + 1) * part)

            @pl.when(on)
            def _(h=h, lanes=lanes):
                arrived(buffer.at[index, :, lanes], recv.at[index, h])
                buffer[index, :, lanes] = (
                    buffer[index, :, lanes].astype(f32) + left_ref[index, :, lanes].astype(f32)
                ).astype(bf16)
                left_copy(index, h, step).start()

    twin_copy.start()
    for off in range(1, n_row):
        w1_copy(off).start()
    for k in range(n_col - 1, 1, -1):
        left_own(k, 1)
        left_own(n_col - 1 - k, -1)

    arrived(right_twin, twin_recv)
    right_half[...] = (
        right_ref[rows_of(side, half)].astype(f32) + right_twin[...].astype(f32)
    ).astype(bf16)
    for off in range(1, chips):
        mid_copy(off).start()

    own = weight_ref[rows_of(row, quarter), :].astype(f32)
    for off in range(1, n_row):
        peer = (row + off) % n_row
        arrived(weight_mid.at[peer], w1_recv.at[peer])
        own = own + weight_mid[peer].astype(f32)
    weight_sum[...] = own.astype(bf16)
    for off in range(1, n_col):
        w2_copy(off).start()
    left_own(1, 1)
    left_own(n_col - 2, -1)
    left_pass(n_col - 1, 1)
    left_pass(0, -1)

    total = right_half[rows_of(chip, many)].astype(f32)
    for off in range(1, chips):
        peer = (chip + off) % chips
        arrived(right_mid.at[peer], mid_recv.at[peer])
        total = total + right_mid[peer].astype(f32)
    right_sum[...] = total.astype(bf16)
    for b in range(many):
        here = jnp.logical_and(owner == row, mine * many + b == col)
        pl.when(jnp.logical_not(here))(right_copy(b).start)
        pl.when(here)(
            pltpu.make_async_copy(right_sum.at[b], right_in.at[slot], right_recv.at[slot]).start
        )

    for k in range(n_col - 2, 1, -1):
        left_pass(k, 1)
        left_pass(n_col - 1 - k, -1)

    own = weight_sum[rows_of(col, piece), :].astype(f32)
    for off in range(1, n_col):
        peer = (col + off) % n_col
        arrived(weight_in.at[peer], w2_recv.at[peer])
        own = own + weight_in[peer].astype(f32)
    weight_part[...] = own.astype(bf16)
    weight_all[rows_of(row * n_col + col, piece), :] = own.astype(bf16)
    for off in range(1, n_col):
        w3_copy(off).start()

    for h in range(parts):
        lanes = slice(h * part, (h + 1) * part)
        left_out[:, lanes] = left_ref[col, :, lanes]

        for on, buffer, recv in ((has_down, up_in, up_recv), (has_up, down_in, down_recv)):
            both = jnp.logical_and(has_up, has_down)

            @pl.when(on)
            def _(buffer=buffer, recv=recv, h=h, lanes=lanes):
                arrived(buffer.at[col, :, lanes], recv.at[col, h])

        @pl.when(both)
        def _(lanes=lanes):
            left_out[:, lanes] = (
                left_ref[col, :, lanes].astype(f32)
                + up_in[col, :, lanes].astype(f32)
                + down_in[col, :, lanes].astype(f32)
            ).astype(bf16)

        for on, buffer in ((jnp.logical_not(has_up), up_in), (jnp.logical_not(has_down), down_in)):

            @pl.when(on)
            def _(buffer=buffer, lanes=lanes):
                left_out[:, lanes] = (
                    left_ref[col, :, lanes].astype(f32) + buffer[col, :, lanes].astype(f32)
                ).astype(bf16)

    for off in range(1, n_col):
        peer = (col + off) % n_col
        arrived(weight_all.at[rows_of(row * n_col + peer, piece)], w3_recv.at[peer])
    for off in range(1, n_row):
        w4_copy(off).start()
    for t in range(ratio):
        arrived(right_in.at[t], right_recv.at[t])
        right_out[t] = right_in[t]
    for off in range(1, n_row):
        peer = (row + off) % n_row
        arrived(weight_all.at[rows_of(peer, quarter)], w4_recv.at[peer])
    weight_out[...] = weight_all[...].astype(f32) * (1.0 / WINDOW_AMINOS)

    twin_copy.wait_send()
    for off in range(1, chips):
        mid_copy(off).wait_send()
    for off in range(1, n_row):
        w1_copy(off).wait_send()
        w4_copy(off).wait_send()
    for off in range(1, n_col):
        w2_copy(off).wait_send()
        w3_copy(off).wait_send()
    for index in range(n_col):
        for h in range(parts):
            pl.when(col < index)(left_copy(index, h, 1).wait_send)
            pl.when(col > index)(left_copy(index, h, -1).wait_send)
    for b in range(many):
        here = jnp.logical_and(owner == row, mine * many + b == col)
        pl.when(jnp.logical_not(here))(right_copy(b).wait_send)


def shards(
    alignment_tensor,
    standardizer_scaling,
    standardizer_offset,
    first_projector,
    second_projector,
    final_projector,
    final_offset,
    amino_strand_label,
    matched_strand_count,
    couple_delta_adjoint,
):
    f32, bf16 = jnp.float32, jnp.bfloat16
    share, rows, feats = alignment_tensor.shape
    cols = couple_delta_adjoint.shape[1]
    size = PROJECTED_SIZE
    n_row, n_col = lax.axis_size("row"), lax.axis_size("col")
    ratio = rows // cols
    seqs = share * n_col
    inner = LANES // cols
    blocks = size // inner
    wide = size * cols
    vmem = pl.BlockSpec(memory_space=pltpu.VMEM)
    dma = pltpu.SemaphoreType.DMA

    entries = standardize_entries(
        alignment_tensor, standardizer_scaling, standardizer_offset
    ).reshape(-1, feats)
    both = jnp.dot(
        entries,
        jnp.concatenate([first_projector, second_projector], axis=1),
        preferred_element_type=f32,
    ).astype(bf16)
    left_own = both[:, :size].reshape(share, rows * size)
    right_own = (
        both[:, size:]
        .reshape(share, ratio, cols, size)
        .transpose(1, 0, 3, 2)
        .reshape(ratio, share, wide)
    )
    left_panel, right_panel = pl.pallas_call(
        functools.partial(gather_kernel, n_row, n_col, ratio),
        in_specs=[vmem] * 2,
        out_specs=[vmem] * 2,
        out_shape=[
            jax.ShapeDtypeStruct((seqs, rows * size), bf16),
            jax.ShapeDtypeStruct((seqs, wide), bf16),
        ],
        scratch_shapes=[
            dma((n_col, 2)), dma((n_col, 2)), dma((n_col, 2)), dma((ratio,)), dma((n_col,)),
            dma((n_col, n_row // 2)), dma((n_col,)), dma((2,)),
        ],
        compiler_params=pltpu.CompilerParams(collective_id=0, has_side_effects=True),
    )(left_own, right_own)

    row_labels = lax.dynamic_slice_in_dim(
        amino_strand_label, lax.axis_index("row") * rows, rows, 0
    )
    col_labels = lax.dynamic_slice_in_dim(
        amino_strand_label, lax.axis_index("col") * cols, cols, 0
    )
    chains = jnp.arange(CHAINS, dtype=jnp.int32)
    row_hot = (row_labels[:, None] == chains[None, :]).astype(f32)
    col_hot = (col_labels[:, None] == chains[None, :]).astype(f32)
    by_chain = jnp.dot(
        matched_strand_count.astype(f32), col_hot.T, precision=lax.Precision.HIGHEST
    )
    depth = jnp.dot(row_hot, by_chain, precision=lax.Precision.HIGHEST)
    table = jnp.pad(jnp.tile(by_chain, (1, inner)), ((0, CHAINS), (0, 0)))
    inverse = jnp.tile(1.0 / depth, (1, inner))
    tile = 8
    steps = rows // tile
    chain_lanes = jnp.repeat(row_labels.astype(f32), size).reshape(steps, 1, tile * size)
    weight = (
        final_projector.reshape(size, blocks, inner, CZ)
        .transpose(1, 0, 2, 3)
        .reshape(blocks * size, inner * CZ)
    )
    flat_grad = couple_delta_adjoint.reshape(-1, CZ)
    whole = lambda shape: pl.BlockSpec(shape, lambda g, labels: (0,) * len(shape))
    pair, left_grad, right_grad, weight_part = pl.pallas_call(
        functools.partial(pair_kernel, tile, cols, seqs),
        grid_spec=pltpu.PrefetchScalarGridSpec(
            num_scalar_prefetch=1,
            grid=(steps,),
            in_specs=[
                pl.BlockSpec((seqs, tile * size), lambda g, labels: (0, g)),
                whole((seqs, wide)),
                whole((2 * CHAINS, LANES)),
                pl.BlockSpec((1, 1, tile * size), lambda g, labels: (g, 0, 0)),
                pl.BlockSpec((tile, LANES), lambda g, labels: (g, 0)),
                pl.BlockSpec((tile * cols, CZ), lambda g, labels: (g, 0)),
                whole((blocks * size, inner * CZ)),
                whole((inner * CZ, blocks * size)),
                whole((1, CZ)),
            ],
            out_specs=[
                pl.BlockSpec((tile * cols, CZ), lambda g, labels: (g, 0)),
                pl.BlockSpec((seqs, tile * size), lambda g, labels: (0, g)),
                whole((seqs, wide)),
                whole((size * size, CZ)),
            ],
            scratch_shapes=[
                pltpu.VMEM((CHAINS + 1, seqs, wide), bf16),
                pltpu.VMEM((CHAINS + 1, wide, seqs), bf16),
                pltpu.VMEM((tile * LANES, inner * CZ), bf16),
                pltpu.VMEM((tile * size, wide), bf16),
                pltpu.VMEM((blocks * size, tile * LANES), bf16),
                pltpu.VMEM((tile * size, wide), f32),
                pltpu.VMEM((tile * size, seqs), f32),
                pltpu.VMEM((seqs, wide), f32),
                pltpu.VMEM((blocks * size, inner * CZ), f32),
                pltpu.VMEM((2 * seqs, tile * size), bf16),
            ],
        ),
        out_shape=[
            jax.ShapeDtypeStruct((rows * cols, CZ), bf16),
            jax.ShapeDtypeStruct((seqs, rows * size), bf16),
            jax.ShapeDtypeStruct((seqs, wide), bf16),
            jax.ShapeDtypeStruct((size * size, CZ), bf16),
        ],
        compiler_params=pltpu.CompilerParams(
            dimension_semantics=("arbitrary",), vmem_limit_bytes=56 * 1024 * 1024
        ),
    )(
        row_labels,
        left_panel,
        right_panel,
        table,
        chain_lanes,
        inverse,
        flat_grad,
        weight,
        weight.T,
        final_offset[None, :],
    )
    pair_update = pair.reshape(rows, cols, CZ)
    many = n_col // n_row
    quarter = size * size // n_row
    piece = quarter // n_col
    adjoint_first_factor, right_sum, weight_total = pl.pallas_call(
        functools.partial(sum_kernel, n_row, n_col, ratio),
        in_specs=[vmem] * 3,
        out_specs=[vmem] * 3,
        out_shape=[
            jax.ShapeDtypeStruct((share, rows * size), bf16),
            jax.ShapeDtypeStruct((ratio, share, wide), bf16),
            jax.ShapeDtypeStruct((size * size, CZ), f32),
        ],
        scratch_shapes=[
            pltpu.VMEM((n_col, share, rows * size), bf16),
            pltpu.VMEM((n_col, share, rows * size), bf16),
            pltpu.VMEM((n_col // 2, share, wide), bf16),
            pltpu.VMEM((n_col // 2, share, wide), bf16),
            pltpu.VMEM((n_row // 2, many, share, wide), bf16),
            pltpu.VMEM((many, share, wide), bf16),
            pltpu.VMEM((ratio, share, wide), bf16),
            pltpu.VMEM((n_row, quarter, CZ), bf16),
            pltpu.VMEM((quarter, CZ), bf16),
            pltpu.VMEM((n_col, piece, CZ), bf16),
            pltpu.VMEM((piece, CZ), bf16),
            pltpu.VMEM((size * size, CZ), bf16),
            dma((n_col, 2)), dma((n_col, 2)), dma((n_col, 2)), dma((n_col, 2)),
            dma, dma,
            dma((n_row // 2,)), dma((n_row // 2,)),
            dma((many,)), dma((ratio,)),
            dma((n_row,)), dma((n_row,)),
            dma((n_col,)), dma((n_col,)),
            dma((n_col,)), dma((n_col,)),
            dma((n_row,)), dma((n_row,)),
        ],
        compiler_params=pltpu.CompilerParams(collective_id=1, has_side_effects=True),
    )(
        left_grad.reshape(n_col, share, rows * size),
        right_grad.reshape(n_col, share, wide),
        weight_part,
    )
    grad_right = (
        right_sum.reshape(ratio, share, size, cols)
        .transpose(1, 0, 3, 2)
        .reshape(share, rows * size)
    )
    grad_w_out = (
        weight_total.reshape(inner, blocks, size, CZ).transpose(2, 1, 0, 3).reshape(size * size, CZ)
    )
    return (pair_update, adjoint_first_factor, grad_right, grad_w_out)


def solution(mesh):
    in_specs = (
        P(("parts", "col"), "row", None),
        P(),
        P(),
        P(),
        P(),
        P(),
        P(),
        P("parts"),
        P("parts", None),
        P(("parts", "row"), "col", None),
    )
    out_specs = (
        P(("parts", "row"), "col", None),
        P(("parts", "col"), "row"),
        P(("parts", "col"), "row"),
        P("parts", None),
    )
    return jax.shard_map(shards, mesh=mesh, in_specs=in_specs, out_specs=out_specs, check_vma=False)
```

```python
import functools

import jax
import jax.numpy as jnp
from jax import lax
from jax.experimental import pallas as pl
from jax.experimental.pallas import tpu as pltpu
from jax.sharding import PartitionSpec as P

PROJECTED_SIZE = 32
CZ = 128
WINDOW_AMINOS = 256
CHAINS = 8
LANES = 128
MESH = pl.DeviceIdType.MESH


def standardize_entries(alignment_tensor, standard_multiplier, additive_offset):
    incoming_entries = alignment_tensor.astype(jnp.float32)
    center = incoming_entries - jnp.mean(incoming_entries, axis=-1, keepdims=True)
    spread = jnp.mean(center * center, axis=-1, keepdims=True)
    return (center * lax.rsqrt(spread + 1e-05) * standard_multiplier + additive_offset).astype(
        jnp.bfloat16
    )


def to(source, target, send, recv, row, col):
    return pltpu.make_async_remote_copy(
        src_ref=source,
        dst_ref=target,
        send_sem=send,
        recv_sem=recv,
        device_id={"row": row, "col": col},
        device_id_type=MESH,
    )


def arrived(ref, sem):
    pltpu.make_async_copy(ref, ref, sem).wait()


def greet(n_row, n_col, me):
    peers = n_row * n_col
    barrier = pltpu.get_barrier_semaphore()

    def signal(off, carry):
        peer = (me + off) % peers
        pl.semaphore_signal(
            barrier,
            inc=1,
            device_id={"row": peer // n_col, "col": peer % n_col},
            device_id_type=MESH,
        )
        return carry

    lax.fori_loop(1, peers, signal, 0)
    return lambda: pl.semaphore_wait(barrier, peers - 1)


def fill_tables(rows, cols, labels_ref, counts_ref, row, col, table_ref, inverse_ref):
    f32 = jnp.float32
    inner = LANES // cols
    lane = lax.broadcasted_iota(jnp.int32, (1, LANES), 1) % cols
    label = jnp.zeros((1, LANES), jnp.int32)
    for j in range(cols):
        label = jnp.where(lane == j, labels_ref[col * cols + j], label)
    table_ref[...] = jnp.zeros_like(table_ref)
    for a in range(CHAINS):
        line = jnp.zeros((1, LANES), jnp.int32)
        for b in range(CHAINS):
            line = jnp.where(label == b, counts_ref[a, b], line)
        table_ref[a : a + 1, :] = line.astype(f32)

    def divide(i, carry):
        inverse_ref[pl.ds(i, 1), :] = 1.0 / table_ref[pl.ds(labels_ref[row * rows + i], 1), :]
        return carry

    lax.fori_loop(0, rows, divide, 0)


def fill_weights(blocks, final_ref, wide_ref, weight_ref, weight_t_ref):
    size = PROJECTED_SIZE
    inner = size // blocks
    wide_ref[...] = final_ref[...].astype(jnp.float32)
    for b in range(blocks):
        for e in range(inner):
            weight_ref[b * size : (b + 1) * size, e * CZ : (e + 1) * CZ] = wide_ref[
                pl.ds(b * inner + e, size, stride=size), :
            ].astype(jnp.bfloat16)
    weight_t_ref[...] = weight_ref[...].T


def project(
    share, rows, align_ref, gain_ref, shift_ref, first_ref, second_ref,
    normed_ref, line_ref, turn_ref, left_own, right_own,
):
    f32, bf16 = jnp.float32, jnp.bfloat16
    size = PROJECTED_SIZE
    feats = align_ref.shape[2]
    gain, shift = gain_ref[...], shift_ref[...]

    def normalise(k, carry):
        x = align_ref[pl.ds(k * 4, 4)].reshape(4 * rows, feats).astype(f32)
        center = x - jnp.mean(x, axis=-1, keepdims=True)
        var = jnp.mean(center * center, axis=-1, keepdims=True)
        normed_ref[pl.ds(pl.multiple_of(k * 4 * rows, 4 * rows), 4 * rows), :] = (
            center * lax.rsqrt(var + 1e-05) * gain + shift
        ).astype(bf16)
        return carry

    lax.fori_loop(0, share // 4, normalise, 0)
    low = share // 2
    second = second_ref[...]
    for p in range(low):
        pair = jnp.concatenate(
            [normed_ref[p * rows : (p + 1) * rows], normed_ref[(p + low) * rows : (p + low + 1) * rows]],
            axis=0,
        )
        turn_ref[p * size : (p + 1) * size, :] = lax.dot_general(
            second, pair, (((1,), (1,)), ((), ())), preferred_element_type=f32
        )
    near = lax.broadcasted_iota(jnp.int32, (low, LANES), 1) < rows
    for b in range(size // 2):
        even = turn_ref[pl.ds(2 * b, low, stride=size), :]
        odd = turn_ref[pl.ds(2 * b + 1, low, stride=size), :]
        lanes = slice(b * LANES, (b + 1) * LANES)
        right_own[0, :low, lanes] = jnp.where(near, even, pltpu.roll(odd, rows, 1)).astype(bf16)
        right_own[0, low:, lanes] = jnp.where(near, pltpu.roll(even, rows, 1), odd).astype(bf16)
    yield
    fold = LANES // size
    first = jnp.concatenate([first_ref[...]] * fold, axis=1)
    line_ref[...] = jnp.dot(normed_ref[...], first, preferred_element_type=f32)
    place = lax.broadcasted_iota(jnp.int32, (share, LANES), 1) // size
    for g in range(rows // fold):
        total = line_ref[pl.ds(g * fold, share, stride=rows), :]
        for k in range(1, fold):
            total = jnp.where(
                place == k, line_ref[pl.ds(g * fold + k, share, stride=rows), :], total
            )
        left_own[:, g * LANES : (g + 1) * LANES] = total.astype(bf16)
    yield


def gather_kernel(
    n_row, n_col, ratio, rows, cols, tile, fused, *refs
):
    f32, bf16 = jnp.float32, jnp.bfloat16
    size = PROJECTED_SIZE
    inner = LANES // cols
    blocks = size // inner
    labels_ref, counts_ref, final_ref, grad_ref = refs[:4]
    count = 9 if fused else 6
    source_refs = refs[4:count]
    left_out, right_out, table_ref, inverse_ref, weight_ref, weight_t_ref, scaled_out = refs[
        count : count + 7
    ]
    grad, spread, scaled, wide_ref = refs[count + 7 : count + 11]
    refs = refs[count + 11 :]
    if fused:
        normed_ref, line_ref, turn_ref, left_ref, right_ref = refs[:5]
        refs = refs[5:]
    else:
        left_ref, right_ref = source_refs
    (
        left_send, left_recv, right_send, right_recv, hop_send, twin_send, own_sem, grad_sem,
        scaled_sem,
    ) = refs
    row, col = lax.axis_index("row"), lax.axis_index("col")
    share = left_ref.shape[0]
    ready = greet(n_row, n_col, row * n_col + col)
    grad_copy = pltpu.make_async_copy(grad_ref, grad, grad_sem)
    grad_copy.start()
    block = lambda ref, index: ref.at[pl.ds(pl.multiple_of(index * share, share), share)]
    owner = col // ratio
    twin = row + 1 - 2 * (row % 2)
    chips = n_row // 2
    is_owner = row == owner
    same_side = row % 2 == owner % 2

    def right_copy(t):
        return to(
            right_ref.at[t], block(right_out, col), right_send.at[t], right_recv.at[col],
            row, row * ratio + t,
        )

    def left_copy(off):
        peer = (col + off) % n_col
        return to(left_ref, block(left_out, col), left_send.at[off], left_recv.at[col], row, peer)

    def hop_copy(source, index, hop):
        return to(
            source, block(right_out, index), hop_send.at[index, hop], right_recv.at[index],
            (row + 2 * hop) % n_row, col,
        )

    def twin_copy(source, index):
        return to(
            source, block(right_out, index), twin_send.at[index], right_recv.at[index], twin, col
        )

    work = project(share, rows, *source_refs, *((normed_ref, line_ref, turn_ref, left_ref, right_ref))) if fused else None
    if fused:
        next(work)
    ready()
    for t in range(ratio):
        pl.when(row * ratio + t != col)(right_copy(t).start)
    mine = right_ref.at[col % ratio]
    own_right = pltpu.make_async_copy(mine, block(right_out, col), own_sem.at[1])

    @pl.when(is_owner)
    def _():
        own_right.start()
        for hop in range(1, chips):
            hop_copy(mine, col, hop).start()
        twin_copy(mine, col).start()

    if fused:
        next(work)
    own_left = pltpu.make_async_copy(left_ref, block(left_out, col), own_sem.at[0])
    own_left.start()
    for off in range(1, n_col):
        left_copy(off).start()

    def pass_right(off):
        peer = (col + off) % n_col
        source = block(right_out, peer)
        if off:
            arrived(source, right_recv.at[peer])

            @pl.when(is_owner)
            def _():
                for hop in range(1, chips):
                    hop_copy(source, peer, hop).start()

            pl.when(same_side)(twin_copy(source, peer).start)
        else:

            @pl.when(jnp.logical_not(is_owner))
            def _():
                arrived(source, right_recv.at[peer])

            pl.when(jnp.logical_and(same_side, jnp.logical_not(is_owner)))(
                twin_copy(source, peer).start
            )

    fill_weights(blocks, final_ref, wide_ref, weight_ref, weight_t_ref)
    fill_tables(rows, cols, labels_ref, counts_ref, row, col, table_ref, inverse_ref)
    spread[...] = jnp.zeros_like(spread)
    grad_copy.wait()
    steps = rows // tile

    def scaled_copy(step, slot):
        extent = tile * size
        return pltpu.make_async_copy(
            scaled.at[slot],
            scaled_out.at[pl.ds(pl.multiple_of(step * extent, extent), extent)],
            scaled_sem.at[slot],
        )

    def scale(step, carry):
        slot = step % 2
        first = pl.multiple_of(step * tile * cols, tile * cols)
        part = grad[pl.ds(first, tile * cols), :]
        for i in range(tile):
            for e in range(inner):
                spread[i * LANES + e * cols : i * LANES + (e + 1) * cols, e * CZ : (e + 1) * CZ] = (
                    part[i * cols : (i + 1) * cols]
                )
        inverse = inverse_ref[pl.ds(pl.multiple_of(step * tile, tile), tile), :]

        @pl.when(step >= 2)
        def _():
            scaled_copy(step - 2, slot).wait()

        for i in range(0, tile, 2):
            back = lax.dot_general(
                weight_ref[...], spread[i * LANES : (i + 2) * LANES, :], (((1,), (1,)), ((), ())),
                preferred_element_type=f32,
            )
            for k in range(2):
                piece = (
                    back[:, k * LANES : (k + 1) * LANES] * inverse[i + k : i + k + 1]
                ).astype(bf16)
                for b in range(blocks):
                    scaled[
                        slot, (i + k) * size : (i + k + 1) * size, b * LANES : (b + 1) * LANES
                    ] = piece[b * size : (b + 1) * size]
        scaled_copy(step, slot).start()
        for off in range(n_col - 1):
            pl.when(step == min(2 * off + 1, steps - 1))(functools.partial(pass_right, off))
        return carry

    lax.fori_loop(0, steps, scale, 0)
    pass_right(n_col - 1)
    for step in range(max(0, steps - 2), steps):
        scaled_copy(step, step % 2).wait()

    own_left.wait()
    pl.when(is_owner)(own_right.wait)
    for off in range(1, n_col):
        peer = (col + off) % n_col
        arrived(block(left_out, peer), left_recv.at[peer])
    for off in range(1, n_col):
        left_copy(off).wait_send()
    for t in range(ratio):
        pl.when(row * ratio + t != col)(right_copy(t).wait_send)

    @pl.when(is_owner)
    def _():
        for off in range(n_col):
            peer = (col + off) % n_col
            for hop in range(1, chips):
                hop_copy(block(right_out, peer), peer, hop).wait_send()

    @pl.when(same_side)
    def _():
        for off in range(n_col):
            peer = (col + off) % n_col
            twin_copy(block(right_out, peer), peer).wait_send()


def pair_kernel(
    tile, cols, seqs,
    labels_ref,
    left_ref, right_ref, table_ref, inverse_ref, grad_ref, scaled, weight_t_ref, bias_ref,
    pair_ref, left_grad_ref, right_grad_ref, weight_grad_ref,
    kept, kept_t, spread, outer, acc, left_acc, right_acc, weight_acc, slots,
):
    step = pl.program_id(0)
    size = PROJECTED_SIZE
    inner = LANES // cols
    blocks = size // inner
    width = 2 * LANES if blocks % 2 == 0 else LANES
    f32, bf16 = jnp.float32, jnp.bfloat16
    seq = lax.broadcasted_iota(jnp.int32, (seqs, LANES), 0).astype(f32)

    @pl.when(step == 0)
    def _():
        spread[...] = jnp.zeros_like(spread)
        right_acc[...] = jnp.zeros_like(right_acc)
        weight_acc[...] = jnp.zeros_like(weight_acc)

        def fill(chain, carry):
            keep = jnp.where(seq < table_ref[pl.ds(chain, 1), :], 1.0, 0.0).astype(bf16)
            for b in range(blocks):
                lanes = slice(b * LANES, (b + 1) * LANES)
                piece = right_ref[:, lanes] * keep
                kept[chain, :, lanes] = piece
                kept_t[chain, lanes, :] = piece.T
            return carry

        extent = pl.num_programs(0) * tile
        first = lax.axis_index("row") * extent
        lax.fori_loop(labels_ref[first], labels_ref[first + extent - 1] + 2, fill, 0)

    for i in range(tile):
        grad = grad_ref[i * cols : (i + 1) * cols, :]
        for e in range(inner):
            spread[i * LANES + e * cols : i * LANES + (e + 1) * cols, e * CZ : (e + 1) * CZ] = grad
    inverse = [inverse_ref[i : i + 1, :] for i in range(tile)]
    offset = lax.axis_index("row") * (pl.num_programs(0) * tile)
    label = [labels_ref[offset + step * tile + i] for i in range(tile)]
    place = lax.broadcasted_iota(jnp.int32, (1, tile * size), 1) // size
    lane = jnp.zeros((1, tile * size), jnp.int32)
    for i in range(tile):
        lane = jnp.where(place == i, label[i], lane)
    low, high = label[0], label[tile - 1]

    def chain_pair(first, chain):
        left = left_ref[...]
        for k in range(2):
            slots[k * seqs : (k + 1) * seqs, :] = left * jnp.where(
                lane == chain + k, 1.0, 0.0
            ).astype(bf16)
        both = slots[...]
        both_t = both.T
        keep = [seq < table_ref[pl.ds(chain + k, 1), :] for k in range(2)]
        for start in range(0, blocks * LANES, width):
            lanes = slice(start, start + width)
            right = kept[pl.ds(chain, 2), :, lanes].reshape(2 * seqs, width)
            prod = jnp.dot(both_t, right, preferred_element_type=f32)
            if first:
                acc[:, lanes] = prod
            else:
                acc[:, lanes] += prod
            out = jnp.dot(both, scaled[:, lanes], preferred_element_type=f32)
            for b in range(width // LANES):
                part = slice(b * LANES, (b + 1) * LANES)
                right_acc[:, start + b * LANES : start + (b + 1) * LANES] += jnp.where(
                    keep[0], out[:seqs, part], 0.0
                ) + jnp.where(keep[1], out[seqs:, part], 0.0)
        right_t = jnp.concatenate([kept_t[chain], kept_t[chain + 1]], axis=1)
        out = jnp.dot(scaled[...], right_t, preferred_element_type=f32)
        for i in range(tile):
            rows = slice(i * size, (i + 1) * size)
            part = jnp.where(label[i] == chain, out[rows, :seqs], 0.0) + jnp.where(
                label[i] == chain + 1, out[rows, seqs:], 0.0
            )
            if first:
                left_acc[rows, :] = part
            else:
                left_acc[rows, :] += part

    chain_pair(True, low)

    def more(p, carry):
        chain_pair(False, low + 2 * p)
        return carry

    lax.fori_loop(1, (high - low) // 2 + 1, more, 0)
    left_grad_ref[...] = left_acc[...].T.astype(bf16)
    for i in range(tile):
        for b in range(blocks):
            outer[b * size : (b + 1) * size, i * LANES : (i + 1) * LANES] = (
                acc[i * size : (i + 1) * size, b * LANES : (b + 1) * LANES] * inverse[i]
            ).astype(bf16)
    group = lax.broadcasted_iota(jnp.int32, (CZ, LANES), 1) // cols
    for i in range(0, tile, 2):
        both = jnp.dot(
            weight_t_ref[...], outer[:, i * LANES : (i + 2) * LANES], preferred_element_type=f32
        )
        for k in range(2):
            lanes = slice(k * LANES, (k + 1) * LANES)
            total = both[:CZ, lanes]
            for e in range(1, inner):
                total = jnp.where(group == e, both[e * CZ : (e + 1) * CZ, lanes], total)
            turned = total.T
            pair = turned[:cols]
            for e in range(1, inner):
                pair = pair + turned[e * cols : (e + 1) * cols]
            pair_ref[(i + k) * cols : (i + k + 1) * cols, :] = (pair + bias_ref[...]).astype(bf16)
    weight_acc[...] += jnp.dot(outer[...], spread[...], preferred_element_type=f32)

    @pl.when(step == pl.num_programs(0) - 1)
    def _():
        right_grad_ref[...] = right_acc[...].astype(bf16)
        rows = blocks * size
        for e in range(inner):
            weight_grad_ref[e * rows : (e + 1) * rows, :] = weight_acc[
                :, e * CZ : (e + 1) * CZ
            ].astype(bf16)


def sum_kernel(
    n_row, n_col, ratio, blocks,
    left_ref, right_ref, weight_ref,
    left_out, right_out, weight_out,
    left_in, right_twin, right_half, right_mid, right_sum, right_in,
    weight_mid, weight_sum, weight_in, weight_part, weight_all,
    up_send, down_send, left_recv, twin_send, twin_recv, mid_send, mid_recv,
    right_send, right_recv,
    w1_send, w1_recv, w2_send, w2_recv, w3_send, w3_recv, w4_send, w4_recv,
):
    f32, bf16 = jnp.float32, jnp.bfloat16
    row, col = lax.axis_index("row"), lax.axis_index("col")
    greet(n_row, n_col, row * n_col + col)()
    chips = n_row // 2
    chip, side = row // 2, row % 2
    twin = row + 1 - 2 * side
    many = n_col // n_row
    half = n_col // 2
    quarter = weight_ref.shape[0] // n_row
    piece = quarter // n_col
    parts = left_recv.shape[1]
    part = left_ref.shape[2] // parts
    owner, slot = col // ratio, col % ratio
    rows_of = lambda index, extent: pl.ds(pl.multiple_of(index * extent, extent), extent)
    mine = side * chips + chip

    def w1_copy(off):
        peer = (row + off) % n_row
        return to(
            weight_ref.at[rows_of(peer, quarter)], weight_mid.at[row], w1_send.at[off],
            w1_recv.at[row], peer, col,
        )

    twin_copy = to(
        right_ref.at[rows_of(1 - side, half)], right_twin, twin_send, twin_recv, twin, col
    )

    def mid_copy(off):
        peer = (chip + off) % chips
        return to(
            right_half.at[rows_of(peer, many)], right_mid.at[chip], mid_send.at[off],
            mid_recv.at[chip], 2 * peer + side, col,
        )

    def right_copy(b):
        return to(
            right_sum.at[b], right_in.at[slot], right_send.at[b], right_recv.at[slot],
            owner, mine * many + b,
        )

    def left_copies(d, h):
        lanes = slice(h * part, (h + 1) * part)
        for step, sends in ((d, up_send), (-d, down_send)):
            there = col + step
            peer = there % n_col
            copy = to(
                left_ref.at[peer, :, lanes], left_in.at[col, :, lanes], sends.at[d, h],
                left_recv.at[col, h], row, peer,
            )
            yield jnp.logical_and(there >= 0, there < n_col), copy

    def left_start(d, h):
        for on, copy in left_copies(d, h):
            pl.when(on)(copy.start)

    def w2_copy(off):
        peer = (col + off) % n_col
        return to(
            weight_sum.at[rows_of(peer, piece)], weight_in.at[col], w2_send.at[off],
            w2_recv.at[col], row, peer,
        )

    def w3_copy(off):
        peer = (col + off) % n_col
        return to(
            weight_part, weight_all.at[rows_of(row * n_col + col, piece)], w3_send.at[off],
            w3_recv.at[col], row, peer,
        )

    def w4_copy(off):
        peer = (row + off) % n_row
        own = weight_all.at[rows_of(row, quarter)]
        return to(own, own, w4_send.at[off], w4_recv.at[row], peer, col)

    for off in range(1, n_row):
        w1_copy(off).start()
    twin_copy.start()
    for h in range(parts):
        left_start(1, h)
    left_start(2, 0)

    arrived(right_twin, twin_recv)
    right_half[...] = (
        right_ref[rows_of(side, half)].astype(f32) + right_twin[...].astype(f32)
    ).astype(bf16)
    for off in range(1, chips):
        mid_copy(off).start()

    own = weight_ref[rows_of(row, quarter), :].astype(f32)
    for off in range(1, n_row):
        peer = (row + off) % n_row
        arrived(weight_mid.at[peer], w1_recv.at[peer])
        own = own + weight_mid[peer].astype(f32)
    weight_sum[...] = own.astype(bf16)
    for off in range(1, n_col):
        w2_copy(off).start()
    for h in range(1, parts):
        left_start(2, h)

    total = right_half[rows_of(chip, many)].astype(f32)
    for off in range(1, chips):
        peer = (chip + off) % chips
        arrived(right_mid.at[peer], mid_recv.at[peer])
        total = total + right_mid[peer].astype(f32)
    right_sum[...] = total.astype(bf16)
    for b in range(many):
        here = jnp.logical_and(owner == row, mine * many + b == col)
        pl.when(jnp.logical_not(here))(right_copy(b).start)
        pl.when(here)(
            pltpu.make_async_copy(right_sum.at[b], right_in.at[slot], right_recv.at[slot]).start
        )

    own = weight_sum[rows_of(col, piece), :].astype(f32)
    for off in range(1, n_col):
        peer = (col + off) % n_col
        arrived(weight_in.at[peer], w2_recv.at[peer])
        own = own + weight_in[peer].astype(f32)
    weight_part[...] = own.astype(bf16)
    weight_all[rows_of(row * n_col + col, piece), :] = own.astype(bf16)
    for off in range(1, n_col):
        w3_copy(off).start()
    for d in range(3, n_col):
        for h in range(parts):
            left_start(d, h)

    for off in range(1, n_col):
        peer = (col + off) % n_col
        arrived(weight_all.at[rows_of(row * n_col + peer, piece)], w3_recv.at[peer])
    for off in range(1, n_row):
        w4_copy(off).start()

    total = left_ref[col].astype(f32)
    for off in range(1, n_col):
        peer = (col + off) % n_col
        for h in range(parts):
            arrived(left_in.at[peer, :, h * part : (h + 1) * part], left_recv.at[peer, h])
        total = total + left_in[peer].astype(f32)
    left_out[...] = total.astype(bf16)
    for t in range(ratio):
        arrived(right_in.at[t], right_recv.at[t])
        right_out[t] = right_in[t]
    for off in range(1, n_row):
        peer = (row + off) % n_row
        arrived(weight_all.at[rows_of(peer, quarter)], w4_recv.at[peer])
    size = PROJECTED_SIZE
    for g in range(size):
        e = (g % blocks) * (size // blocks) + g // blocks
        weight_out[pl.ds(e, size, stride=size), :] = weight_all[
            g * size : (g + 1) * size, :
        ].astype(f32) * (1.0 / WINDOW_AMINOS)

    twin_copy.wait_send()
    for off in range(1, chips):
        mid_copy(off).wait_send()
    for off in range(1, n_row):
        w1_copy(off).wait_send()
        w4_copy(off).wait_send()
    for off in range(1, n_col):
        w2_copy(off).wait_send()
        w3_copy(off).wait_send()
        for h in range(parts):
            for on, copy in left_copies(off, h):
                pl.when(on)(copy.wait_send)
    for b in range(many):
        here = jnp.logical_and(owner == row, mine * many + b == col)
        pl.when(jnp.logical_not(here))(right_copy(b).wait_send)


def shards(
    alignment_tensor,
    standardizer_scaling,
    standardizer_offset,
    first_projector,
    second_projector,
    final_projector,
    final_offset,
    amino_strand_label,
    matched_strand_count,
    couple_delta_adjoint,
):
    f32, bf16 = jnp.float32, jnp.bfloat16
    share, rows, feats = alignment_tensor.shape
    cols = couple_delta_adjoint.shape[1]
    size = PROJECTED_SIZE
    n_row, n_col = lax.axis_size("row"), lax.axis_size("col")
    ratio = rows // cols
    seqs = share * n_col
    inner = LANES // cols
    blocks = size // inner
    wide = size * cols
    vmem = pl.BlockSpec(memory_space=pltpu.VMEM)
    dma = pltpu.SemaphoreType.DMA

    tile = 8
    steps = rows // tile
    fused = ratio == 1 and 2 * rows == LANES and share % 16 == 0
    if fused:
        sources = (
            alignment_tensor, standardizer_scaling[None, :], standardizer_offset[None, :],
            first_projector, second_projector.T,
        )
        extra = [
            pltpu.VMEM((share * rows, feats), bf16),
            pltpu.VMEM((share * rows, LANES), f32),
            pltpu.VMEM((share // 2 * size, LANES), f32),
            pltpu.VMEM((share, rows * size), bf16),
            pltpu.VMEM((ratio, share, wide), bf16),
        ]
    else:
        entries = standardize_entries(
            alignment_tensor, standardizer_scaling, standardizer_offset
        ).reshape(-1, feats)
        both = jnp.dot(
            entries,
            jnp.concatenate([first_projector, second_projector], axis=1),
            preferred_element_type=f32,
        ).astype(bf16)
        left_own = both[:, :size].reshape(share, rows * size)
        right_own = (
            both[:, size:]
            .reshape(share, ratio, cols, size)
            .transpose(1, 0, 3, 2)
            .reshape(ratio, share, wide)
        )
        sources, extra = (left_own, right_own), []
    flat_grad = couple_delta_adjoint.reshape(-1, CZ)
    smem = pl.BlockSpec(memory_space=pltpu.SMEM)
    hbm = pl.BlockSpec(memory_space=pl.ANY)
    left_panel, right_panel, table, inverse, weight, weight_t, scaled = pl.pallas_call(
        functools.partial(gather_kernel, n_row, n_col, ratio, rows, cols, tile, fused),
        in_specs=[smem, smem, vmem, hbm] + [vmem] * len(sources),
        out_specs=[vmem] * 6 + [hbm],
        out_shape=[
            jax.ShapeDtypeStruct((seqs, rows * size), bf16),
            jax.ShapeDtypeStruct((seqs, wide), bf16),
            jax.ShapeDtypeStruct((2 * CHAINS, LANES), f32),
            jax.ShapeDtypeStruct((rows, LANES), f32),
            jax.ShapeDtypeStruct((blocks * size, inner * CZ), bf16),
            jax.ShapeDtypeStruct((inner * CZ, blocks * size), bf16),
            jax.ShapeDtypeStruct((rows * size, wide), bf16),
        ],
        scratch_shapes=[
            pltpu.VMEM((rows * cols, CZ), bf16),
            pltpu.VMEM((tile * LANES, inner * CZ), bf16),
            pltpu.VMEM((2, tile * size, wide), bf16),
            pltpu.VMEM((size * size, CZ), f32),
            *extra,
            dma((n_col,)), dma((n_col,)), dma((ratio,)), dma((n_col,)),
            dma((n_col, n_row // 2)), dma((n_col,)), dma((2,)), dma, dma((2,)),
        ],
        compiler_params=pltpu.CompilerParams(
            collective_id=0, has_side_effects=True, vmem_limit_bytes=56 * 1024 * 1024
        ),
    )(amino_strand_label, matched_strand_count, final_projector, flat_grad, *sources)

    whole = lambda shape: pl.BlockSpec(shape, lambda g, labels: (0,) * len(shape))
    pair, left_grad, right_grad, weight_part = pl.pallas_call(
        functools.partial(pair_kernel, tile, cols, seqs),
        grid_spec=pltpu.PrefetchScalarGridSpec(
            num_scalar_prefetch=1,
            grid=(steps,),
            in_specs=[
                pl.BlockSpec((seqs, tile * size), lambda g, labels: (0, g)),
                whole((seqs, wide)),
                whole((2 * CHAINS, LANES)),
                pl.BlockSpec((tile, LANES), lambda g, labels: (g, 0)),
                pl.BlockSpec((tile * cols, CZ), lambda g, labels: (g, 0)),
                pl.BlockSpec((tile * size, wide), lambda g, labels: (g, 0)),
                whole((inner * CZ, blocks * size)),
                whole((1, CZ)),
            ],
            out_specs=[
                pl.BlockSpec((tile * cols, CZ), lambda g, labels: (g, 0)),
                pl.BlockSpec((seqs, tile * size), lambda g, labels: (0, g)),
                whole((seqs, wide)),
                whole((size * size, CZ)),
            ],
            scratch_shapes=[
                pltpu.VMEM((CHAINS + 1, seqs, wide), bf16),
                pltpu.VMEM((CHAINS + 1, wide, seqs), bf16),
                pltpu.VMEM((tile * LANES, inner * CZ), bf16),
                pltpu.VMEM((blocks * size, tile * LANES), bf16),
                pltpu.VMEM((tile * size, wide), f32),
                pltpu.VMEM((tile * size, seqs), f32),
                pltpu.VMEM((seqs, wide), f32),
                pltpu.VMEM((blocks * size, inner * CZ), f32),
                pltpu.VMEM((2 * seqs, tile * size), bf16),
            ],
        ),
        out_shape=[
            jax.ShapeDtypeStruct((rows * cols, CZ), bf16),
            jax.ShapeDtypeStruct((seqs, rows * size), bf16),
            jax.ShapeDtypeStruct((seqs, wide), bf16),
            jax.ShapeDtypeStruct((size * size, CZ), bf16),
        ],
        compiler_params=pltpu.CompilerParams(
            dimension_semantics=("arbitrary",), vmem_limit_bytes=56 * 1024 * 1024
        ),
    )(
        amino_strand_label,
        left_panel,
        right_panel,
        table,
        inverse,
        flat_grad,
        scaled,
        weight_t,
        final_offset[None, :],
    )
    pair_update = pair.reshape(rows, cols, CZ)
    many = n_col // n_row
    quarter = size * size // n_row
    piece = quarter // n_col
    adjoint_first_factor, right_sum, weight_total = pl.pallas_call(
        functools.partial(sum_kernel, n_row, n_col, ratio, blocks),
        in_specs=[vmem] * 3,
        out_specs=[vmem] * 3,
        out_shape=[
            jax.ShapeDtypeStruct((share, rows * size), bf16),
            jax.ShapeDtypeStruct((ratio, share, wide), bf16),
            jax.ShapeDtypeStruct((size * size, CZ), f32),
        ],
        scratch_shapes=[
            pltpu.VMEM((n_col, share, rows * size), bf16),
            pltpu.VMEM((n_col // 2, share, wide), bf16),
            pltpu.VMEM((n_col // 2, share, wide), bf16),
            pltpu.VMEM((n_row // 2, many, share, wide), bf16),
            pltpu.VMEM((many, share, wide), bf16),
            pltpu.VMEM((ratio, share, wide), bf16),
            pltpu.VMEM((n_row, quarter, CZ), bf16),
            pltpu.VMEM((quarter, CZ), bf16),
            pltpu.VMEM((n_col, piece, CZ), bf16),
            pltpu.VMEM((piece, CZ), bf16),
            pltpu.VMEM((size * size, CZ), bf16),
            dma((n_col, 2)), dma((n_col, 2)), dma((n_col, 2)),
            dma, dma,
            dma((n_row // 2,)), dma((n_row // 2,)),
            dma((many,)), dma((ratio,)),
            dma((n_row,)), dma((n_row,)),
            dma((n_col,)), dma((n_col,)),
            dma((n_col,)), dma((n_col,)),
            dma((n_row,)), dma((n_row,)),
        ],
        compiler_params=pltpu.CompilerParams(collective_id=1, has_side_effects=True),
    )(
        left_grad.reshape(n_col, share, rows * size),
        right_grad.reshape(n_col, share, wide),
        weight_part,
    )
    grad_right = (
        right_sum.reshape(ratio, share, size, cols)
        .transpose(1, 0, 3, 2)
        .reshape(share, rows * size)
    )
    return (pair_update, adjoint_first_factor, grad_right, weight_total)


def solution(mesh):
    in_specs = (
        P(("parts", "col"), "row", None),
        P(),
        P(),
        P(),
        P(),
        P(),
        P(),
        P("parts"),
        P("parts", None),
        P(("parts", "row"), "col", None),
    )
    out_specs = (
        P(("parts", "row"), "col", None),
        P(("parts", "col"), "row"),
        P(("parts", "col"), "row"),
        P("parts", None),
    )
    return jax.shard_map(shards, mesh=mesh, in_specs=in_specs, out_specs=out_specs, check_vma=False)
```

```python
import functools

import jax
import jax.numpy as jnp
from jax import lax
from jax.experimental import pallas as pl
from jax.experimental.pallas import tpu as pltpu
from jax.sharding import PartitionSpec as P

PROJECTED_SIZE = 32
CZ = 128
WINDOW_AMINOS = 256
CHAINS = 8
LANES = 128
MESH = pl.DeviceIdType.MESH


def standardize_entries(alignment_tensor, standard_multiplier, additive_offset):
    incoming_entries = alignment_tensor.astype(jnp.float32)
    center = incoming_entries - jnp.mean(incoming_entries, axis=-1, keepdims=True)
    spread = jnp.mean(center * center, axis=-1, keepdims=True)
    return (center * lax.rsqrt(spread + 1e-05) * standard_multiplier + additive_offset).astype(
        jnp.bfloat16
    )


def to(source, target, send, recv, row, col):
    return pltpu.make_async_remote_copy(
        src_ref=source,
        dst_ref=target,
        send_sem=send,
        recv_sem=recv,
        device_id={"row": row, "col": col},
        device_id_type=MESH,
    )


def arrived(ref, sem):
    pltpu.make_async_copy(ref, ref, sem).wait()


def greet(n_row, n_col, me):
    peers = n_row * n_col
    barrier = pltpu.get_barrier_semaphore()

    def signal(off, carry):
        peer = (me + off) % peers
        pl.semaphore_signal(
            barrier,
            inc=1,
            device_id={"row": peer // n_col, "col": peer % n_col},
            device_id_type=MESH,
        )
        return carry

    lax.fori_loop(1, peers, signal, 0)
    return lambda: pl.semaphore_wait(barrier, peers - 1)


def fill_tables(rows, cols, labels_ref, counts_ref, row, col, table_ref, inverse_ref):
    f32 = jnp.float32
    inner = LANES // cols
    lane = lax.broadcasted_iota(jnp.int32, (1, LANES), 1) % cols
    label = jnp.zeros((1, LANES), jnp.int32)
    for j in range(cols):
        label = jnp.where(lane == j, labels_ref[col * cols + j], label)
    table_ref[...] = jnp.zeros_like(table_ref)
    for a in range(CHAINS):
        line = jnp.zeros((1, LANES), jnp.int32)
        for b in range(CHAINS):
            line = jnp.where(label == b, counts_ref[a, b], line)
        table_ref[a : a + 1, :] = line.astype(f32)

    def divide(i, carry):
        inverse_ref[pl.ds(i, 1), :] = 1.0 / table_ref[pl.ds(labels_ref[row * rows + i], 1), :]
        return carry

    lax.fori_loop(0, rows, divide, 0)


def fill_weights(blocks, final_ref, wide_ref, weight_ref, weight_t_ref):
    size = PROJECTED_SIZE
    inner = size // blocks
    wide_ref[...] = final_ref[...].astype(jnp.float32)
    for b in range(blocks):
        for e in range(inner):
            weight_ref[b * size : (b + 1) * size, e * CZ : (e + 1) * CZ] = wide_ref[
                pl.ds(b * inner + e, size, stride=size), :
            ].astype(jnp.bfloat16)
    weight_t_ref[...] = weight_ref[...].T


def project(
    share, rows, align_ref, gain_ref, shift_ref, first_ref, second_ref,
    normed_ref, line_ref, turn_ref, left_own, right_own,
):
    f32, bf16 = jnp.float32, jnp.bfloat16
    size = PROJECTED_SIZE
    feats = align_ref.shape[2]
    gain, shift = gain_ref[...], shift_ref[...]

    def normalise(k, carry):
        x = align_ref[pl.ds(k * 4, 4)].reshape(4 * rows, feats).astype(f32)
        center = x - jnp.mean(x, axis=-1, keepdims=True)
        var = jnp.mean(center * center, axis=-1, keepdims=True)
        normed_ref[pl.ds(pl.multiple_of(k * 4 * rows, 4 * rows), 4 * rows), :] = (
            center * lax.rsqrt(var + 1e-05) * gain + shift
        ).astype(bf16)
        return carry

    lax.fori_loop(0, share // 4, normalise, 0)
    low = share // 2
    second = second_ref[...]
    for p in range(low):
        pair = jnp.concatenate(
            [normed_ref[p * rows : (p + 1) * rows], normed_ref[(p + low) * rows : (p + low + 1) * rows]],
            axis=0,
        )
        turn_ref[p * size : (p + 1) * size, :] = lax.dot_general(
            second, pair, (((1,), (1,)), ((), ())), preferred_element_type=f32
        )
    near = lax.broadcasted_iota(jnp.int32, (low, LANES), 1) < rows
    for b in range(size // 2):
        even = turn_ref[pl.ds(2 * b, low, stride=size), :]
        odd = turn_ref[pl.ds(2 * b + 1, low, stride=size), :]
        lanes = slice(b * LANES, (b + 1) * LANES)
        right_own[0, :low, lanes] = jnp.where(near, even, pltpu.roll(odd, rows, 1)).astype(bf16)
        right_own[0, low:, lanes] = jnp.where(near, pltpu.roll(even, rows, 1), odd).astype(bf16)
    yield
    fold = LANES // size
    first = jnp.concatenate([first_ref[...]] * fold, axis=0)
    line_ref[...] = lax.dot_general(
        normed_ref[...], first, (((1,), (1,)), ((), ())), preferred_element_type=f32
    )
    place = lax.broadcasted_iota(jnp.int32, (share, LANES), 1) // size
    for g in range(rows // fold):
        total = line_ref[pl.ds(g * fold, share, stride=rows), :]
        for k in range(1, fold):
            total = jnp.where(
                place == k, line_ref[pl.ds(g * fold + k, share, stride=rows), :], total
            )
        left_own[:, g * LANES : (g + 1) * LANES] = total.astype(bf16)
    yield


def gather_kernel(
    n_row, n_col, ratio, rows, cols, tile, fused, *refs
):
    f32, bf16 = jnp.float32, jnp.bfloat16
    size = PROJECTED_SIZE
    inner = LANES // cols
    blocks = size // inner
    labels_ref, counts_ref, final_ref, grad_ref = refs[:4]
    count = 9 if fused else 6
    source_refs = refs[4:count]
    left_out, right_out, table_ref, inverse_ref, weight_ref, weight_t_ref, scaled_out = refs[
        count : count + 7
    ]
    grad, spread, scaled, wide_ref = refs[count + 7 : count + 11]
    refs = refs[count + 11 :]
    if fused:
        normed_ref, line_ref, turn_ref, left_ref, right_ref = refs[:5]
        refs = refs[5:]
    else:
        left_ref, right_ref = source_refs
    (
        left_send, left_recv, right_send, right_recv, hop_send, twin_send, own_sem, grad_sem,
        scaled_sem,
    ) = refs
    row, col = lax.axis_index("row"), lax.axis_index("col")
    share = left_ref.shape[0]
    ready = greet(n_row, n_col, row * n_col + col)
    grad_copy = pltpu.make_async_copy(grad_ref, grad, grad_sem)
    grad_copy.start()
    block = lambda ref, index: ref.at[pl.ds(pl.multiple_of(index * share, share), share)]
    owner = col // ratio
    twin = row + 1 - 2 * (row % 2)
    chips = n_row // 2
    is_owner = row == owner
    same_side = row % 2 == owner % 2

    def right_copy(t):
        return to(
            right_ref.at[t], block(right_out, col), right_send.at[t], right_recv.at[col],
            row, row * ratio + t,
        )

    def left_copy(off):
        peer = (col + off) % n_col
        return to(left_ref, block(left_out, col), left_send.at[off], left_recv.at[col], row, peer)

    def hop_copy(source, index, hop):
        return to(
            source, block(right_out, index), hop_send.at[index, hop], right_recv.at[index],
            (row + 2 * hop) % n_row, col,
        )

    def twin_copy(source, index):
        return to(
            source, block(right_out, index), twin_send.at[index], right_recv.at[index], twin, col
        )

    work = project(share, rows, *source_refs, *((normed_ref, line_ref, turn_ref, left_ref, right_ref))) if fused else None
    if fused:
        next(work)
    ready()
    for t in range(ratio):
        pl.when(row * ratio + t != col)(right_copy(t).start)
    mine = right_ref.at[col % ratio]
    own_right = pltpu.make_async_copy(mine, block(right_out, col), own_sem.at[1])

    @pl.when(is_owner)
    def _():
        own_right.start()
        for hop in range(1, chips):
            hop_copy(mine, col, hop).start()
        twin_copy(mine, col).start()

    if fused:
        next(work)
    own_left = pltpu.make_async_copy(left_ref, block(left_out, col), own_sem.at[0])
    own_left.start()
    for off in range(1, n_col):
        left_copy(off).start()

    def pass_right(off):
        peer = (col + off) % n_col
        source = block(right_out, peer)
        if off:
            arrived(source, right_recv.at[peer])

            @pl.when(is_owner)
            def _():
                for hop in range(1, chips):
                    hop_copy(source, peer, hop).start()

            pl.when(same_side)(twin_copy(source, peer).start)
        else:

            @pl.when(jnp.logical_not(is_owner))
            def _():
                arrived(source, right_recv.at[peer])

            pl.when(jnp.logical_and(same_side, jnp.logical_not(is_owner)))(
                twin_copy(source, peer).start
            )

    fill_weights(blocks, final_ref, wide_ref, weight_ref, weight_t_ref)
    fill_tables(rows, cols, labels_ref, counts_ref, row, col, table_ref, inverse_ref)
    spread[...] = jnp.zeros_like(spread)
    grad_copy.wait()
    steps = rows // tile

    def scaled_copy(step, slot):
        extent = tile * size
        return pltpu.make_async_copy(
            scaled.at[slot],
            scaled_out.at[pl.ds(pl.multiple_of(step * extent, extent), extent)],
            scaled_sem.at[slot],
        )

    def scale(step, carry):
        slot = step % 2
        first = pl.multiple_of(step * tile * cols, tile * cols)
        part = grad[pl.ds(first, tile * cols), :]
        for i in range(tile):
            for e in range(inner):
                spread[i * LANES + e * cols : i * LANES + (e + 1) * cols, e * CZ : (e + 1) * CZ] = (
                    part[i * cols : (i + 1) * cols]
                )
        inverse = inverse_ref[pl.ds(pl.multiple_of(step * tile, tile), tile), :]

        @pl.when(step >= 2)
        def _():
            scaled_copy(step - 2, slot).wait()

        for i in range(0, tile, 2):
            back = lax.dot_general(
                weight_ref[...], spread[i * LANES : (i + 2) * LANES, :], (((1,), (1,)), ((), ())),
                preferred_element_type=f32,
            )
            for k in range(2):
                piece = (
                    back[:, k * LANES : (k + 1) * LANES] * inverse[i + k : i + k + 1]
                ).astype(bf16)
                for b in range(blocks):
                    scaled[
                        slot, (i + k) * size : (i + k + 1) * size, b * LANES : (b + 1) * LANES
                    ] = piece[b * size : (b + 1) * size]
        scaled_copy(step, slot).start()
        for off in range(n_col - 1):
            pl.when(step == min(2 * off + 1, steps - 1))(functools.partial(pass_right, off))
        return carry

    lax.fori_loop(0, steps, scale, 0)
    pass_right(n_col - 1)
    for step in range(max(0, steps - 2), steps):
        scaled_copy(step, step % 2).wait()

    own_left.wait()
    pl.when(is_owner)(own_right.wait)
    for off in range(1, n_col):
        peer = (col + off) % n_col
        arrived(block(left_out, peer), left_recv.at[peer])
    for off in range(1, n_col):
        left_copy(off).wait_send()
    for t in range(ratio):
        pl.when(row * ratio + t != col)(right_copy(t).wait_send)

    @pl.when(is_owner)
    def _():
        for off in range(n_col):
            peer = (col + off) % n_col
            for hop in range(1, chips):
                hop_copy(block(right_out, peer), peer, hop).wait_send()

    @pl.when(same_side)
    def _():
        for off in range(n_col):
            peer = (col + off) % n_col
            twin_copy(block(right_out, peer), peer).wait_send()


def core_kernel(
    n_row, n_col, ratio, rows, cols, tile,
    labels_ref, left_in_ref, right_in_ref, table_ref, inverse_ref, grad_hbm, scaled_hbm,
    weight_t_ref, bias_ref,
    pair_out, left_out, right_out, weight_out,
    grad, scaled, spread, outer, outer_more, left_more, slots, left_tiles, inverses, label_lanes, right_t, keep, keep_t,
    weight_acc, left_ref, right_ref, weight_ref, local_sem,
    left_in, right_twin, right_half, right_mid, right_sum,
    weight_twin, weight_half, weight_mid, weight_sum, weight_in, weight_part,
    up_send, down_send, left_recv, twin_send, twin_recv, mid_send, mid_recv,
    right_send, right_recv, own_sem,
    w1_send, w1_recv, w2_send, w2_recv, w3_send, w3_recv, around_send, hop_send, last_send,
    all_recv,
):
    f32, bf16 = jnp.float32, jnp.bfloat16
    size = PROJECTED_SIZE
    inner = LANES // cols
    blocks = size // inner
    steps = rows // tile
    span = tile * size
    seqs = left_in_ref.shape[0]
    share = seqs // n_col
    width = 2 * LANES if blocks % 2 == 0 else LANES
    chunks = blocks * LANES // width
    extras = outer_more.shape[0] - 1
    row, col = lax.axis_index("row"), lax.axis_index("col")
    ready = greet(n_row, n_col, row * n_col + col)
    chips = n_row // 2
    chip, side = row // 2, row % 2
    twin = row + 1 - 2 * side
    many = n_col // n_row
    half = n_col // 2
    quarter = weight_ref.shape[0] // n_row
    piece = quarter // n_col
    parts = left_recv.shape[1]
    part = left_ref.shape[2] // parts
    owner, slot = col // ratio, col % ratio
    rows_of = lambda index, extent: pl.ds(pl.multiple_of(index * extent, extent), extent)
    mine = side * chips + chip
    add = lambda *terms: functools.reduce(lambda a, b: a + b, [t.astype(f32) for t in terms])

    w1_copy = to(
        weight_ref.at[rows_of(1 - side, chips * quarter)], weight_twin, w1_send, w1_recv, twin, col
    )
    twin_copy = to(
        right_ref.at[rows_of(1 - side, half)], right_twin, twin_send, twin_recv, twin, col
    )

    def w2_copy(off):
        peer = (chip + off) % chips
        return to(
            weight_half.at[rows_of(peer, quarter)], weight_mid.at[chip], w2_send.at[off],
            w2_recv.at[chip], 2 * peer + side, col,
        )

    def mid_copy(off):
        peer = (chip + off) % chips
        return to(
            right_half.at[rows_of(peer, many)], right_mid.at[chip], mid_send.at[off],
            mid_recv.at[chip], 2 * peer + side, col,
        )

    def right_copy(b):
        return to(
            right_sum.at[b], right_out.at[slot], right_send.at[b], right_recv.at[slot],
            owner, mine * many + b,
        )

    def left_copies(d, h):
        lanes = slice(h * part, (h + 1) * part)
        for step, sends in ((d, up_send), (-d, down_send)):
            there = col + step
            peer = there % n_col
            copy = to(
                left_ref.at[peer, :, lanes], left_in.at[col, :, lanes], sends.at[d, h],
                left_recv.at[col, h], row, peer,
            )
            yield jnp.logical_and(there >= 0, there < n_col), copy

    def left_start(d, h):
        for on, copy in left_copies(d, h):
            pl.when(on)(copy.start)

    def w3_copy(off):
        peer = (col + off) % n_col
        return to(
            weight_sum.at[rows_of(peer, piece)], weight_in.at[col], w3_send.at[off],
            w3_recv.at[col], row, peer,
        )

    def cell(group, index):
        return weight_out.at[rows_of(group * n_col + index, piece)]

    def spread_copy(send, group, index, to_row, to_col, source=None):
        there = cell(group, index)
        return to(
            there if source is None else source, there, send, all_recv.at[group, index],
            to_row, to_col,
        )

    def around_copy(off):
        return spread_copy(around_send.at[off], mine, col, row, (col + off) % n_col, weight_part)

    def hop_copy(index, off, source=None):
        peer = (chip + off) % chips
        return spread_copy(hop_send.at[index, off], mine, index, 2 * peer + side, col, source)

    def last_copy(group, index, source=None):
        return spread_copy(last_send.at[group, index], group, index, twin, col, source)

    def group_of(off):
        return side * chips + (chip + off) % chips

    def here(b):
        return jnp.logical_and(owner == row, mine * many + b == col)


    own_piece = pltpu.make_async_copy(weight_part, cell(mine, col), own_sem)

    def after_left_extra():
        arrived(weight_twin, w1_recv)
        weight_half[...] = add(
            weight_ref[rows_of(side, chips * quarter), :], weight_twin[...]
        ).astype(bf16)
        for off in range(1, chips):
            w2_copy(off).start()

    def first_left():
        for d in range(1, n_col):
            left_start(d, 0)

    def after_left():
        total = weight_half[rows_of(chip, quarter), :].astype(f32)
        for off in range(1, chips):
            peer = (chip + off) % chips
            arrived(weight_mid.at[peer], w2_recv.at[peer])
            total = add(total, weight_mid[peer])
        weight_sum[...] = total.astype(bf16)
        for off in range(1, n_col):
            w3_copy(off).start()

    def during_right():
        total = weight_sum[rows_of(col, piece), :].astype(f32)
        for off in range(1, n_col):
            peer = (col + off) % n_col
            arrived(weight_in.at[peer], w3_recv.at[peer])
            total = add(total, weight_in[peer])
        weight_part[...] = total.astype(bf16)
        own_piece.start()
        for off in range(1, n_col):
            around_copy(off).start()
        for off in range(1, chips):
            hop_copy(col, off, weight_part).start()
        last_copy(mine, col, weight_part).start()
        for h in range(1, parts):
            for d in range(1, n_col):
                left_start(d, h)

    def after_right():
        twin_copy.start()

    def pair_first():
        arrived(right_twin, twin_recv)
        right_half[...] = add(right_ref[rows_of(side, half)], right_twin[...]).astype(bf16)
        for off in range(1, chips):
            mid_copy(off).start()

    def pair_second():
        for off in range(1, n_col):
            peer = (col + off) % n_col
            arrived(cell(mine, peer), all_recv.at[mine, peer])
            for hop in range(1, chips):
                hop_copy(peer, hop).start()
            last_copy(mine, peer).start()

    def pair_third():
        total = right_half[rows_of(chip, many)].astype(f32)
        for off in range(1, chips):
            peer = (chip + off) % chips
            arrived(right_mid.at[peer], mid_recv.at[peer])
            total = add(total, right_mid[peer])
        right_sum[...] = total.astype(bf16)
        for b in range(many):
            pl.when(jnp.logical_not(here(b)))(right_copy(b).start)
            own = pltpu.make_async_copy(right_sum.at[b], right_out.at[slot], right_recv.at[slot])
            pl.when(here(b))(own.start)

    def finish():
        for off in range(n_col):
            peer = (col + off) % n_col
            for hop in range(1, chips):
                arrived(cell(group_of(hop), peer), all_recv.at[group_of(hop), peer])
                last_copy(group_of(hop), peer).start()

        total = left_ref[col].astype(f32)
        for off in range(1, n_col):
            peer = (col + off) % n_col
            for h in range(parts):
                arrived(left_in.at[peer, :, h * part : (h + 1) * part], left_recv.at[peer, h])
            total = add(total, left_in[peer])
        left_out[...] = total.astype(bf16)
        for t in range(ratio):
            arrived(right_out.at[t], right_recv.at[t])
        for off in range(n_col):
            peer = (col + off) % n_col
            for other in range(chips):
                group = (1 - side) * chips + other
                arrived(cell(group, peer), all_recv.at[group, peer])

        own_piece.wait()
        w1_copy.wait_send()
        twin_copy.wait_send()
        for off in range(1, chips):
            w2_copy(off).wait_send()
            mid_copy(off).wait_send()
        for off in range(1, n_col):
            w3_copy(off).wait_send()
            around_copy(off).wait_send()
            for h in range(parts):
                for on, copy in left_copies(off, h):
                    pl.when(on)(copy.wait_send)
        for index in range(n_col):
            for off in range(1, chips):
                hop_copy(index, off).wait_send()
            for off in range(chips):
                last_copy(group_of(off), index).wait_send()
        for b in range(many):
            pl.when(jnp.logical_not(here(b)))(right_copy(b).wait_send)
    grad_copies = [
        pltpu.make_async_copy(
            grad_hbm.at[pl.ds(t * tile * cols, tile * cols)], grad.at[t], local_sem.at[0, t]
        )
        for t in range(steps)
    ]
    scaled_copies = [
        pltpu.make_async_copy(
            scaled_hbm.at[pl.ds(t * span, span)], scaled.at[t], local_sem.at[1, t]
        )
        for t in range(steps)
    ]
    for copy in grad_copies + scaled_copies:
        copy.start()

    place_of = lax.broadcasted_iota(jnp.int32, (tile, span), 1) // size
    seq = lax.broadcasted_iota(jnp.int32, (seqs, LANES), 0).astype(f32)
    for chain in range(keep.shape[0]):
        kept = jnp.where(seq < table_ref[chain : chain + 1, :], 1.0, 0.0)
        keep[chain] = kept.astype(bf16)
        keep_t[chain] = kept.T.astype(bf16)
    for b in range(blocks):
        right_t[b * LANES : (b + 1) * LANES, :] = right_in_ref[:, b * LANES : (b + 1) * LANES].T
    for t in range(steps):
        left_tiles[t] = left_in_ref[:, t * span : (t + 1) * span]
        inverses[t] = inverse_ref[t * tile : (t + 1) * tile, :]
        line = jnp.zeros((tile, span), jnp.int32)
        for i in range(tile):
            line = jnp.where(place_of == i, labels_ref[row * rows + t * tile + i], line)
        label_lanes[t] = line
    spread[...] = jnp.zeros_like(spread)
    weight_acc[...] = jnp.zeros_like(weight_acc)
    outer_more[0] = jnp.zeros(outer_more.shape[1:], bf16)
    left_more[0] = jnp.zeros(left_more.shape[1:], f32)

    offset = row * rows
    label_of = lambda t, i: labels_ref[offset + t * tile + i]
    lows = [label_of(t, 0) for t in range(steps)]
    more = [lax.div(label_of(t, tile - 1) - lows[t], jnp.int32(2)) for t in range(steps)]
    ends, end = [], 0
    for t in range(steps):
        end = end + more[t]
        ends.append(end)

    flag = lambda test: test.astype(jnp.int32)

    def extra_of(u):
        t = sum([flag(ends[k] <= u) for k in range(steps)])
        chain = flag(t == steps) * CHAINS
        for k in range(steps):
            chain = chain + flag(t == k) * (lows[k] + 2 * (u - ends[k] + more[k] + 1))
        return t - flag(t == steps), chain

    def slot_of(t):
        return sum([flag(t == k) * flag(more[k] > 0) * ends[k] for k in range(steps)])

    def same_of(u):
        return flag(extra_of(u)[0] == extra_of(u - 1)[0]).astype(f32)

    def build(t, chain, place):
        lane = label_lanes[t][:1]
        left = left_tiles[t]
        for k in range(2):
            slots[place, k * seqs : (k + 1) * seqs, :] = left * jnp.where(
                lane == chain + k, 1.0, 0.0
            ).astype(bf16)
        return slots[place]

    def forward(t, chain, place, store):
        both_t = build(t, chain, place).T
        inverse = inverses[t]
        kept = [jnp.concatenate([keep[chain + k]] * (width // LANES), axis=1) for k in range(2)]
        for c in range(chunks):
            lanes = slice(c * width, (c + 1) * width)
            right = right_in_ref[:, lanes]
            right = jnp.concatenate([right * kept[0], right * kept[1]], axis=0)
            prod = jnp.dot(both_t, right, preferred_element_type=f32)
            for i in range(tile):
                for b in range(width // LANES):
                    first = (c * (width // LANES) + b) * size
                    store(
                        slice(first, first + size), slice(i * LANES, (i + 1) * LANES),
                        (
                            prod[i * size : (i + 1) * size, b * LANES : (b + 1) * LANES]
                            * inverse[i : i + 1]
                        ).astype(bf16),
                    )

    def forward_more(u, carry):
        t, chain = extra_of(u)
        same = jnp.full((size, LANES), same_of(u), f32).astype(bf16)

        def store(where, lanes, value):
            outer_more[u + 1, where, lanes] = value + outer_more[u, where, lanes] * same

        forward(t, chain, steps + u, store)
        return carry

    lax.fori_loop(0, extras, forward_more, 0)
    for copy in grad_copies:
        copy.wait()

    def forward_main(t, carry):
        slot = slot_of(t)

        def store(where, lanes, value):
            outer[t, where, lanes] = value + outer_more[slot, where, lanes]

        forward(t, label_of(t, 0), t, store)
        for i in range(tile):
            part = grad[t, i * cols : (i + 1) * cols, :]
            for e in range(inner):
                spread[i * LANES + e * cols : i * LANES + (e + 1) * cols, e * CZ : (e + 1) * CZ] = (
                    part
                )
        weight_acc[...] += jnp.dot(outer[t], spread[...], preferred_element_type=f32)
        return carry

    lax.fori_loop(0, steps, forward_main, 0)
    extent = blocks * size
    for e in range(inner):
        weight_ref[e * extent : (e + 1) * extent, :] = weight_acc[
            :, e * CZ : (e + 1) * CZ
        ].astype(bf16)
    ready()
    w1_copy.start()
    for copy in scaled_copies:
        copy.wait()

    def left_part(t, chain):
        tall = jnp.zeros((span, 2 * seqs), f32)
        for c in range(chunks):
            lanes = slice(c * width, (c + 1) * width)
            kept = [
                jnp.concatenate([keep_t[chain + k]] * (width // LANES), axis=0) for k in range(2)
            ]
            right = right_t[lanes, :]
            right = jnp.concatenate([right * kept[0], right * kept[1]], axis=1)
            tall = tall + jnp.dot(scaled[t, :, lanes], right, preferred_element_type=f32)
        turned = tall.T
        lane = label_lanes[t][:1]
        return jnp.where(lane == chain, turned[:seqs], 0.0) + jnp.where(
            lane == chain + 1, turned[seqs:], 0.0
        )

    def left_extra(u, carry):
        t, chain = extra_of(u)
        left_more[u + 1] = left_part(t, chain) + left_more[u] * same_of(u)
        return carry

    lax.fori_loop(0, extras, left_extra, 0)
    after_left_extra()

    def left_main(t, carry):
        slot = slot_of(t)
        turned = left_part(t, label_of(t, 0)) + left_more[slot]
        lanes = pl.ds(pl.multiple_of(t * span, span), span)
        for q in range(n_col):
            left_ref[q, :, lanes] = turned[q * share : (q + 1) * share].astype(bf16)
        pl.when(t == steps // parts - 1)(first_left)
        return carry

    lax.fori_loop(0, steps, left_main, 0)
    after_left()
    pairs = [(t, label_of(t, 0), t) for t in range(steps)]
    for u in range(extras):
        pairs.append((*extra_of(jnp.int32(u)), steps + u))

    def right_main(c, carry):
        lanes = pl.ds(pl.multiple_of(c * width, width), width)
        total = [jnp.zeros((seqs, LANES), f32) for _ in range(width // LANES)]
        for t, chain, place in pairs:
            out = jnp.dot(slots[place], scaled[t, :, lanes], preferred_element_type=f32)
            kept = [seq < table_ref[pl.ds(chain + k, 1), :] for k in range(2)]
            for b in range(width // LANES):
                part = slice(b * LANES, (b + 1) * LANES)
                total[b] = total[b] + (
                    jnp.where(kept[0], out[:seqs, part], 0.0)
                    + jnp.where(kept[1], out[seqs:, part], 0.0)
                )
        whole = jnp.concatenate(total, axis=1)
        for q in range(n_col):
            right_ref[q, :, lanes] = whole[q * share : (q + 1) * share].astype(bf16)
        pl.when(c == chunks * 3 // 4)(during_right)
        return carry

    lax.fori_loop(0, chunks, right_main, 0)
    after_right()
    group = lax.broadcasted_iota(jnp.int32, (CZ, LANES), 1) // cols

    def pairs_of(t, carry):
        for i in range(0, tile, 2):
            both = jnp.dot(
                weight_t_ref[...], outer[t, :, i * LANES : (i + 2) * LANES],
                preferred_element_type=f32,
            )
            for k in range(2):
                lanes = slice(k * LANES, (k + 1) * LANES)
                total = both[:CZ, lanes]
                for e in range(1, inner):
                    total = jnp.where(group == e, both[e * CZ : (e + 1) * CZ, lanes], total)
                turned = total.T
                pair = turned[:cols]
                for e in range(1, inner):
                    pair = pair + turned[e * cols : (e + 1) * cols]
                first = pl.multiple_of((t * tile + i + k) * cols, cols)
                pair_out[pl.ds(first, cols), :] = (pair + bias_ref[...]).astype(bf16)
        pl.when(t == min(1, steps - 1))(pair_first)
        pl.when(t == steps // 2)(pair_second)
        pl.when(t == steps - 1)(pair_third)
        return carry

    lax.fori_loop(0, steps, pairs_of, 0)
    finish()


def finish_kernel(fused, blocks, left_ref, right_ref, weight_ref, *refs):
    f32, bf16 = jnp.float32, jnp.bfloat16
    size = PROJECTED_SIZE
    left_out, right_out, weight_out = refs[:3]
    left_out[...] = left_ref[...]
    for g in range(size):
        e = (g % blocks) * (size // blocks) + g // blocks
        weight_out[pl.ds(e, size, stride=size), :] = weight_ref[
            g * size : (g + 1) * size, :
        ].astype(f32) * (1.0 / WINDOW_AMINOS)
    if not fused:
        right_out[...] = right_ref[...]
        return
    turn_ref, line_ref = refs[3:]
    share = right_ref.shape[1]
    low = share // 2
    rows = line_ref.shape[0] // share
    near = lax.broadcasted_iota(jnp.int32, (low, LANES), 1) < rows
    for b in range(size // 2):
        lanes = slice(b * LANES, (b + 1) * LANES)
        above = right_ref[0, :low, lanes].astype(f32)
        below = right_ref[0, low:, lanes].astype(f32)
        turn_ref[pl.ds(2 * b, low, stride=size), :] = jnp.where(
            near, above, pltpu.roll(below, rows, 1)
        )
        turn_ref[pl.ds(2 * b + 1, low, stride=size), :] = jnp.where(
            near, pltpu.roll(above, rows, 1), below
        )
    fold = LANES // size
    for p in range(low):
        turned = jnp.concatenate([turn_ref[p * size : (p + 1) * size, :]] * fold, axis=0).T
        line_ref[p * rows : (p + 1) * rows, :] = turned[:rows]
        line_ref[(p + low) * rows : (p + low + 1) * rows, :] = turned[rows:]
    place = lax.broadcasted_iota(jnp.int32, (share, LANES), 1) // size
    for g in range(rows // fold):
        total = line_ref[pl.ds(g * fold, share, stride=rows), :]
        for k in range(1, fold):
            total = jnp.where(
                place == k, line_ref[pl.ds(g * fold + k, share, stride=rows), :], total
            )
        right_out[:, g * LANES : (g + 1) * LANES] = total.astype(bf16)


def shards(
    alignment_tensor,
    standardizer_scaling,
    standardizer_offset,
    first_projector,
    second_projector,
    final_projector,
    final_offset,
    amino_strand_label,
    matched_strand_count,
    couple_delta_adjoint,
):
    f32, bf16 = jnp.float32, jnp.bfloat16
    share, rows, feats = alignment_tensor.shape
    cols = couple_delta_adjoint.shape[1]
    size = PROJECTED_SIZE
    n_row, n_col = lax.axis_size("row"), lax.axis_size("col")
    ratio = rows // cols
    seqs = share * n_col
    inner = LANES // cols
    blocks = size // inner
    wide = size * cols
    vmem = pl.BlockSpec(memory_space=pltpu.VMEM)
    dma = pltpu.SemaphoreType.DMA

    tile = 8
    steps = rows // tile
    fused = ratio == 1 and 2 * rows == LANES and share % 16 == 0
    if fused:
        sources = (
            alignment_tensor, standardizer_scaling[None, :], standardizer_offset[None, :],
            first_projector.T, second_projector.T,
        )
        extra = [
            pltpu.VMEM((share * rows, feats), bf16),
            pltpu.VMEM((share * rows, LANES), f32),
            pltpu.VMEM((share // 2 * size, LANES), f32),
            pltpu.VMEM((share, rows * size), bf16),
            pltpu.VMEM((ratio, share, wide), bf16),
        ]
    else:
        entries = standardize_entries(
            alignment_tensor, standardizer_scaling, standardizer_offset
        ).reshape(-1, feats)
        both = jnp.dot(
            entries,
            jnp.concatenate([first_projector, second_projector], axis=1),
            preferred_element_type=f32,
        ).astype(bf16)
        left_own = both[:, :size].reshape(share, rows * size)
        right_own = (
            both[:, size:]
            .reshape(share, ratio, cols, size)
            .transpose(1, 0, 3, 2)
            .reshape(ratio, share, wide)
        )
        sources, extra = (left_own, right_own), []
    flat_grad = couple_delta_adjoint.reshape(-1, CZ)
    smem = pl.BlockSpec(memory_space=pltpu.SMEM)
    hbm = pl.BlockSpec(memory_space=pl.ANY)
    left_panel, right_panel, table, inverse, weight, weight_t, scaled = pl.pallas_call(
        functools.partial(gather_kernel, n_row, n_col, ratio, rows, cols, tile, fused),
        in_specs=[smem, smem, vmem, hbm] + [vmem] * len(sources),
        out_specs=[vmem] * 6 + [hbm],
        out_shape=[
            jax.ShapeDtypeStruct((seqs, rows * size), bf16),
            jax.ShapeDtypeStruct((seqs, wide), bf16),
            jax.ShapeDtypeStruct((2 * CHAINS, LANES), f32),
            jax.ShapeDtypeStruct((rows, LANES), f32),
            jax.ShapeDtypeStruct((blocks * size, inner * CZ), bf16),
            jax.ShapeDtypeStruct((inner * CZ, blocks * size), bf16),
            jax.ShapeDtypeStruct((rows * size, wide), bf16),
        ],
        scratch_shapes=[
            pltpu.VMEM((rows * cols, CZ), bf16),
            pltpu.VMEM((tile * LANES, inner * CZ), bf16),
            pltpu.VMEM((2, tile * size, wide), bf16),
            pltpu.VMEM((size * size, CZ), f32),
            *extra,
            dma((n_col,)), dma((n_col,)), dma((ratio,)), dma((n_col,)),
            dma((n_col, n_row // 2)), dma((n_col,)), dma((2,)), dma, dma((2,)),
        ],
        compiler_params=pltpu.CompilerParams(
            collective_id=0, has_side_effects=True, vmem_limit_bytes=56 * 1024 * 1024
        ),
    )(amino_strand_label, matched_strand_count, final_projector, flat_grad, *sources)

    many = n_col // n_row
    quarter = size * size // n_row
    piece = quarter // n_col
    extras = min(CHAINS - 1, rows - 1) // 2
    pair, left_sum, right_sum, weight_total = pl.pallas_call(
        functools.partial(core_kernel, n_row, n_col, ratio, rows, cols, tile),
        in_specs=[smem] + [vmem] * 4 + [hbm] * 2 + [vmem] * 2,
        out_specs=[vmem] * 4,
        out_shape=[
            jax.ShapeDtypeStruct((rows * cols, CZ), bf16),
            jax.ShapeDtypeStruct((share, rows * size), bf16),
            jax.ShapeDtypeStruct((ratio, share, wide), bf16),
            jax.ShapeDtypeStruct((size * size, CZ), bf16),
        ],
        scratch_shapes=[
            pltpu.VMEM((steps, tile * cols, CZ), bf16),
            pltpu.VMEM((steps, tile * size, wide), bf16),
            pltpu.VMEM((tile * LANES, inner * CZ), bf16),
            pltpu.VMEM((steps, blocks * size, tile * LANES), bf16),
            pltpu.VMEM((extras + 1, blocks * size, tile * LANES), bf16),
            pltpu.VMEM((extras + 1, seqs, tile * size), f32),
            pltpu.VMEM((steps + extras, 2 * seqs, tile * size), bf16),
            pltpu.VMEM((steps, seqs, tile * size), bf16),
            pltpu.VMEM((steps, tile, LANES), f32),
            pltpu.VMEM((steps, tile, tile * size), jnp.int32),
            pltpu.VMEM((wide, seqs), bf16),
            pltpu.VMEM((CHAINS + 2, seqs, LANES), bf16),
            pltpu.VMEM((CHAINS + 2, LANES, seqs), bf16),
            pltpu.VMEM((blocks * size, inner * CZ), f32),
            pltpu.VMEM((n_col, share, rows * size), bf16),
            pltpu.VMEM((n_col, share, wide), bf16),
            pltpu.VMEM((size * size, CZ), bf16),
            dma((2, steps)),
            pltpu.VMEM((n_col, share, rows * size), bf16),
            pltpu.VMEM((n_col // 2, share, wide), bf16),
            pltpu.VMEM((n_col // 2, share, wide), bf16),
            pltpu.VMEM((n_row // 2, many, share, wide), bf16),
            pltpu.VMEM((many, share, wide), bf16),
            pltpu.VMEM((n_row // 2 * quarter, CZ), bf16),
            pltpu.VMEM((n_row // 2 * quarter, CZ), bf16),
            pltpu.VMEM((n_row // 2, quarter, CZ), bf16),
            pltpu.VMEM((quarter, CZ), bf16),
            pltpu.VMEM((n_col, piece, CZ), bf16),
            pltpu.VMEM((piece, CZ), bf16),
            dma((n_col, 2)), dma((n_col, 2)), dma((n_col, 2)),
            dma, dma,
            dma((n_row // 2,)), dma((n_row // 2,)),
            dma((many,)), dma((ratio,)), dma,
            dma, dma,
            dma((n_row // 2,)), dma((n_row // 2,)),
            dma((n_col,)), dma((n_col,)), dma((n_col,)),
            dma((n_col, n_row // 2)), dma((n_row, n_col)), dma((n_row, n_col)),
        ],
        compiler_params=pltpu.CompilerParams(
            collective_id=1, has_side_effects=True, vmem_limit_bytes=58 * 1024 * 1024
        ),
    )(
        amino_strand_label,
        left_panel,
        right_panel,
        table,
        inverse,
        flat_grad,
        scaled,
        weight_t,
        final_offset[None, :],
    )
    pair_update = pair.reshape(rows, cols, CZ)
    adjoint_first_factor, grad_right, grad_w_out = pl.pallas_call(
        functools.partial(finish_kernel, fused, blocks),
        in_specs=[vmem] * 3,
        out_specs=[vmem] * 3,
        out_shape=[
            jax.ShapeDtypeStruct((share, rows * size), bf16),
            jax.ShapeDtypeStruct((share, rows * size) if fused else (ratio, share, wide), bf16),
            jax.ShapeDtypeStruct((size * size, CZ), f32),
        ],
        scratch_shapes=[
            pltpu.VMEM((share // 2 * size, LANES), f32),
            pltpu.VMEM((share * rows, LANES), f32),
        ]
        if fused
        else [],
    )(left_sum, right_sum, weight_total)
    if not fused:
        grad_right = (
            grad_right.reshape(ratio, share, size, cols)
            .transpose(1, 0, 3, 2)
            .reshape(share, rows * size)
        )
    return (pair_update, adjoint_first_factor, grad_right, grad_w_out)


def solution(mesh):
    in_specs = (
        P(("parts", "col"), "row", None),
        P(),
        P(),
        P(),
        P(),
        P(),
        P(),
        P("parts"),
        P("parts", None),
        P(("parts", "row"), "col", None),
    )
    out_specs = (
        P(("parts", "row"), "col", None),
        P(("parts", "col"), "row"),
        P(("parts", "col"), "row"),
        P("parts", None),
    )
    return jax.shard_map(shards, mesh=mesh, in_specs=in_specs, out_specs=out_specs, check_vma=False)
```

```python
import functools

import jax
import jax.numpy as jnp
from jax import lax
from jax.experimental import pallas as pl
from jax.experimental.pallas import tpu as pltpu
from jax.sharding import PartitionSpec as P

PROJECTED_SIZE = 32
CZ = 128
WINDOW_AMINOS = 256
CHAINS = 8
LANES = 128
MESH = pl.DeviceIdType.MESH


def standardize_entries(alignment_tensor, standard_multiplier, additive_offset):
    incoming_entries = alignment_tensor.astype(jnp.float32)
    center = incoming_entries - jnp.mean(incoming_entries, axis=-1, keepdims=True)
    spread = jnp.mean(center * center, axis=-1, keepdims=True)
    return (center * lax.rsqrt(spread + 1e-05) * standard_multiplier + additive_offset).astype(
        jnp.bfloat16
    )


def to(source, target, send, recv, row, col):
    return pltpu.make_async_remote_copy(
        src_ref=source,
        dst_ref=target,
        send_sem=send,
        recv_sem=recv,
        device_id={"row": row, "col": col},
        device_id_type=MESH,
    )


def arrived(ref, sem):
    pltpu.make_async_copy(ref, ref, sem).wait()


def greet(n_row, n_col, me):
    peers = n_row * n_col
    barrier = pltpu.get_barrier_semaphore()

    def signal(off, carry):
        peer = (me + off) % peers
        pl.semaphore_signal(
            barrier,
            inc=1,
            device_id={"row": peer // n_col, "col": peer % n_col},
            device_id_type=MESH,
        )
        return carry

    lax.fori_loop(1, peers, signal, 0)
    return lambda: pl.semaphore_wait(barrier, peers - 1)


def fill_tables(
    rows, cols, labels_ref, counts_ref, row, col, table_ref, inverse_ref, over_ref
):
    f32 = jnp.float32
    inner = LANES // cols
    lane = lax.broadcasted_iota(jnp.int32, (1, LANES), 1) % cols
    label = jnp.zeros((1, LANES), jnp.int32)
    for j in range(cols):
        label = jnp.where(lane == j, labels_ref[col * cols + j], label)
    table_ref[...] = jnp.zeros_like(table_ref)
    for a in range(CHAINS):
        line = jnp.zeros((1, LANES), jnp.int32)
        for b in range(CHAINS):
            line = jnp.where(label == b, counts_ref[a, b], line)
        table_ref[a : a + 1, :] = line.astype(f32)

    over_ref[...] = 1.0 / jnp.maximum(table_ref[...], 1.0)
    for i in range(rows):
        inverse_ref[i : i + 1, :] = over_ref[pl.ds(labels_ref[row * rows + i], 1), :]


def fill_weights(blocks, final_ref, wide_ref, weight_ref, weight_t_ref):
    size = PROJECTED_SIZE
    inner = size // blocks
    wide_ref[...] = final_ref[...].astype(jnp.float32)
    for b in range(blocks):
        for e in range(inner):
            weight_ref[b * size : (b + 1) * size, e * CZ : (e + 1) * CZ] = wide_ref[
                pl.ds(b * inner + e, size, stride=size), :
            ].astype(jnp.bfloat16)
    weight_t_ref[...] = weight_ref[...].T


def project(
    share, rows, align_ref, gain_ref, shift_ref, first_ref, second_ref,
    normed_ref, line_ref, turn_ref, left_own, right_own,
):
    f32, bf16 = jnp.float32, jnp.bfloat16
    size = PROJECTED_SIZE
    feats = align_ref.shape[2]
    gain, shift = gain_ref[...], shift_ref[...]

    def normalise(k, carry):
        x = align_ref[pl.ds(k * 4, 4)].reshape(4 * rows, feats).astype(f32)
        center = x - jnp.mean(x, axis=-1, keepdims=True)
        var = jnp.mean(center * center, axis=-1, keepdims=True)
        normed_ref[pl.ds(pl.multiple_of(k * 4 * rows, 4 * rows), 4 * rows), :] = (
            center * lax.rsqrt(var + 1e-05) * gain + shift
        ).astype(bf16)
        return carry

    lax.fori_loop(0, share // 4, normalise, 0)
    low = share // 2
    second = second_ref[...]
    for p in range(low):
        pair = jnp.concatenate(
            [normed_ref[p * rows : (p + 1) * rows], normed_ref[(p + low) * rows : (p + low + 1) * rows]],
            axis=0,
        )
        turn_ref[p * size : (p + 1) * size, :] = lax.dot_general(
            second, pair, (((1,), (1,)), ((), ())), preferred_element_type=f32
        )
    near = lax.broadcasted_iota(jnp.int32, (low, LANES), 1) < rows
    for b in range(size // 2):
        even = turn_ref[pl.ds(2 * b, low, stride=size), :]
        odd = turn_ref[pl.ds(2 * b + 1, low, stride=size), :]
        lanes = slice(b * LANES, (b + 1) * LANES)
        right_own[0, :low, lanes] = jnp.where(near, even, pltpu.roll(odd, rows, 1)).astype(bf16)
        right_own[0, low:, lanes] = jnp.where(near, pltpu.roll(even, rows, 1), odd).astype(bf16)
    yield
    fold = LANES // size
    first = jnp.concatenate([first_ref[...]] * fold, axis=0)
    line_ref[...] = lax.dot_general(
        normed_ref[...], first, (((1,), (1,)), ((), ())), preferred_element_type=f32
    )
    place = lax.broadcasted_iota(jnp.int32, (share, LANES), 1) // size
    for g in range(rows // fold):
        total = line_ref[pl.ds(g * fold, share, stride=rows), :]
        for k in range(1, fold):
            total = jnp.where(
                place == k, line_ref[pl.ds(g * fold + k, share, stride=rows), :], total
            )
        span = left_own.shape[2]
        lanes = slice(g * LANES % span, g * LANES % span + LANES)
        left_own[g * LANES // span, :, lanes] = total.astype(bf16)
    yield


def core_kernel(n_row, n_col, ratio, rows, cols, tile, fused, *refs):
    f32, bf16 = jnp.float32, jnp.bfloat16
    size = PROJECTED_SIZE
    inner = LANES // cols
    blocks = size // inner
    steps = rows // tile
    span = tile * size
    labels_ref, counts_ref, final_ref, bias_ref, grad_hbm = refs[:5]
    count = 10 if fused else 7
    source_refs = refs[5:count]
    pair_out, left_out, right_out, weight_out = refs[count : count + 4]
    refs = refs[count + 4 :]
    if fused:
        normed_ref, line_ref, turn_ref, left_own, right_own = refs[:5]
        refs = refs[5:]
    else:
        left_own, right_own = source_refs
    (
        table_ref, over_ref, inverse_ref, wide_ref, weight_w, weight_t_ref, left_tiles, right_panel,
        g_left_send, g_left_recv, g_right_send, g_right_recv, g_hop_send, g_twin_send, g_own_sem,
        grad, scaled, spread, outer, outer_own, outer_more, left_more, slots, inverses, label_lanes,
        right_t, keep, keep_t, weight_acc, left_ref, right_ref, weight_ref, local_sem,
        left_in, right_twin, right_half, right_mid, right_sum,
        weight_twin, weight_half, weight_mid, weight_sum, weight_in, weight_part,
        up_send, down_send, left_recv, twin_send, twin_recv, mid_send, mid_recv,
        right_send, right_recv, own_sem,
        w1_send, w1_recv, w2_send, w2_recv, w3_send, w3_recv, around_send, hop_send, last_send,
        all_recv,
    ) = refs
    row, col = lax.axis_index("row"), lax.axis_index("col")
    ready = greet(n_row, n_col, row * n_col + col)
    grad_copies = [
        pltpu.make_async_copy(
            grad_hbm.at[pl.ds(t * tile * cols, tile * cols)], grad.at[t], local_sem.at[t]
        )
        for t in range(steps)
    ]
    for copy in grad_copies:
        copy.start()
    seqs, wide = right_panel.shape
    share = seqs // n_col
    width = 2 * LANES if blocks % 2 == 0 else LANES
    chunks = blocks * LANES // width
    extras = outer_more.shape[0] - 1
    chips = n_row // 2
    chip, side = row // 2, row % 2
    twin = row + 1 - 2 * side
    many = n_col // n_row
    half = n_col // 2
    quarter = weight_ref.shape[0] // n_row
    piece = quarter // n_col
    parts = left_recv.shape[1]
    part = left_ref.shape[2] // parts
    owner, slot = col // ratio, col % ratio
    rows_of = lambda index, extent: pl.ds(pl.multiple_of(index * extent, extent), extent)
    mine = side * chips + chip
    add = lambda *terms: functools.reduce(lambda a, b: a + b, [t.astype(f32) for t in terms])

    w1_copy = to(
        weight_ref.at[rows_of(1 - side, chips * quarter)], weight_twin, w1_send, w1_recv, twin, col
    )
    twin_copy = to(
        right_ref.at[rows_of(1 - side, half)], right_twin, twin_send, twin_recv, twin, col
    )

    def w2_copy(off):
        peer = (chip + off) % chips
        return to(
            weight_half.at[rows_of(peer, quarter)], weight_mid.at[chip], w2_send.at[off],
            w2_recv.at[chip], 2 * peer + side, col,
        )

    def mid_copy(off):
        peer = (chip + off) % chips
        return to(
            right_half.at[rows_of(peer, many)], right_mid.at[chip], mid_send.at[off],
            mid_recv.at[chip], 2 * peer + side, col,
        )

    def right_copy(b):
        return to(
            right_sum.at[b], right_out.at[slot], right_send.at[b], right_recv.at[slot],
            owner, mine * many + b,
        )

    def left_copies(d, h):
        lanes = slice(h * part, (h + 1) * part)
        for step, sends in ((d, up_send), (-d, down_send)):
            there = col + step
            peer = there % n_col
            copy = to(
                left_ref.at[peer, :, lanes], left_in.at[col, :, lanes], sends.at[d, h],
                left_recv.at[col, h], row, peer,
            )
            yield jnp.logical_and(there >= 0, there < n_col), copy

    def left_start(d, h):
        for on, copy in left_copies(d, h):
            pl.when(on)(copy.start)

    def w3_copy(off):
        peer = (col + off) % n_col
        return to(
            weight_sum.at[rows_of(peer, piece)], weight_in.at[col], w3_send.at[off],
            w3_recv.at[col], row, peer,
        )

    def cell(group, index):
        return weight_out.at[rows_of(group * n_col + index, piece)]

    def spread_copy(send, group, index, to_row, to_col, source=None):
        there = cell(group, index)
        return to(
            there if source is None else source, there, send, all_recv.at[group, index],
            to_row, to_col,
        )

    def around_copy(off):
        return spread_copy(around_send.at[off], mine, col, row, (col + off) % n_col, weight_part)

    def hop_copy(index, off, source=None):
        peer = (chip + off) % chips
        return spread_copy(hop_send.at[index, off], mine, index, 2 * peer + side, col, source)

    def last_copy(group, index, source=None):
        return spread_copy(last_send.at[group, index], group, index, twin, col, source)

    def group_of(off):
        return side * chips + (chip + off) % chips

    def here(b):
        return jnp.logical_and(owner == row, mine * many + b == col)


    own_piece = pltpu.make_async_copy(weight_part, cell(mine, col), own_sem)

    def after_left_extra():
        arrived(weight_twin, w1_recv)
        weight_half[...] = add(
            weight_ref[rows_of(side, chips * quarter), :], weight_twin[...]
        ).astype(bf16)
        for off in range(1, chips):
            w2_copy(off).start()

    def first_left():
        for d in range(1, n_col):
            left_start(d, 0)

    def after_left():
        total = weight_half[rows_of(chip, quarter), :].astype(f32)
        for off in range(1, chips):
            peer = (chip + off) % chips
            arrived(weight_mid.at[peer], w2_recv.at[peer])
            total = add(total, weight_mid[peer])
        weight_sum[...] = total.astype(bf16)
        for off in range(1, n_col):
            w3_copy(off).start()

    def during_right():
        total = weight_sum[rows_of(col, piece), :].astype(f32)
        for off in range(1, n_col):
            peer = (col + off) % n_col
            arrived(weight_in.at[peer], w3_recv.at[peer])
            total = add(total, weight_in[peer])
        weight_part[...] = total.astype(bf16)
        own_piece.start()
        for off in range(1, n_col):
            around_copy(off).start()
        for off in range(1, chips):
            hop_copy(col, off, weight_part).start()
        last_copy(mine, col, weight_part).start()
        for h in range(1, parts):
            for d in range(1, n_col):
                left_start(d, h)

    def after_right():
        twin_copy.start()

    def pair_first():
        arrived(right_twin, twin_recv)
        right_half[...] = add(right_ref[rows_of(side, half)], right_twin[...]).astype(bf16)
        for off in range(1, chips):
            mid_copy(off).start()

    def pair_second():
        for off in range(1, n_col):
            peer = (col + off) % n_col
            arrived(cell(mine, peer), all_recv.at[mine, peer])
            for hop in range(1, chips):
                hop_copy(peer, hop).start()
            last_copy(mine, peer).start()

    def pair_third():
        total = right_half[rows_of(chip, many)].astype(f32)
        for off in range(1, chips):
            peer = (chip + off) % chips
            arrived(right_mid.at[peer], mid_recv.at[peer])
            total = add(total, right_mid[peer])
        right_sum[...] = total.astype(bf16)
        for b in range(many):
            pl.when(jnp.logical_not(here(b)))(right_copy(b).start)
            own = pltpu.make_async_copy(right_sum.at[b], right_out.at[slot], right_recv.at[slot])
            pl.when(here(b))(own.start)

    def finish():
        for off in range(n_col):
            peer = (col + off) % n_col
            for hop in range(1, chips):
                arrived(cell(group_of(hop), peer), all_recv.at[group_of(hop), peer])
                last_copy(group_of(hop), peer).start()

        total = left_ref[col].astype(f32)
        for off in range(1, n_col):
            peer = (col + off) % n_col
            for h in range(parts):
                arrived(left_in.at[peer, :, h * part : (h + 1) * part], left_recv.at[peer, h])
            total = add(total, left_in[peer])
        left_out[...] = total.astype(bf16)
        for t in range(ratio):
            arrived(right_out.at[t], right_recv.at[t])
        for off in range(n_col):
            peer = (col + off) % n_col
            for other in range(chips):
                group = (1 - side) * chips + other
                arrived(cell(group, peer), all_recv.at[group, peer])

        own_piece.wait()
        w1_copy.wait_send()
        twin_copy.wait_send()
        for off in range(1, chips):
            w2_copy(off).wait_send()
            mid_copy(off).wait_send()
        for off in range(1, n_col):
            w3_copy(off).wait_send()
            around_copy(off).wait_send()
            for h in range(parts):
                for on, copy in left_copies(off, h):
                    pl.when(on)(copy.wait_send)
        for index in range(n_col):
            for off in range(1, chips):
                hop_copy(index, off).wait_send()
            for off in range(chips):
                last_copy(group_of(off), index).wait_send()
        for b in range(many):
            pl.when(jnp.logical_not(here(b)))(right_copy(b).wait_send)
    is_owner = row == owner
    same_side = row % 2 == owner % 2
    group = steps // parts
    seq_rows = lambda index: pl.ds(pl.multiple_of(index * share, share), share)
    block = lambda index: right_panel.at[seq_rows(index)]
    tiles_of = lambda index, h: left_tiles.at[h * group : (h + 1) * group, seq_rows(index)]

    def out_right(t):
        return to(
            right_own.at[t], block(col), g_right_send.at[t], g_right_recv.at[col],
            row, row * ratio + t,
        )

    def out_left(d, h):
        for k, step in enumerate((d, -d)):
            there = col + step
            copy = to(
                left_own.at[h * group : (h + 1) * group], tiles_of(col, h),
                g_left_send.at[k, d, h], g_left_recv.at[col, h], row, there % n_col,
            )
            yield jnp.logical_and(there >= 0, there < n_col), copy

    def pass_hop(source, index, hop):
        return to(
            source, block(index), g_hop_send.at[index, hop], g_right_recv.at[index],
            (row + 2 * hop) % n_row, col,
        )

    def pass_twin(source, index):
        return to(source, block(index), g_twin_send.at[index], g_right_recv.at[index], twin, col)

    if fused:
        work = project(
            share, rows, *source_refs, normed_ref, line_ref, turn_ref, left_own, right_own
        )
        next(work)
    ready()
    for t in range(ratio):
        pl.when(row * ratio + t != col)(out_right(t).start)
    own_block = right_own.at[col % ratio]
    own_right = pltpu.make_async_copy(own_block, block(col), g_own_sem.at[1])

    @pl.when(is_owner)
    def _():
        own_right.start()
        for hop in range(1, chips):
            pass_hop(own_block, col, hop).start()
        pass_twin(own_block, col).start()

    if fused:
        next(work)
    own_left = pltpu.make_async_copy(left_own, left_tiles.at[:, seq_rows(col)], g_own_sem.at[0])
    own_left.start()
    for h in range(parts):
        for d in range(1, n_col):
            for on, copy in out_left(d, h):
                pl.when(on)(copy.start)

    def pass_right(off):
        peer = (col + off) % n_col
        source = block(peer)
        if off:
            arrived(source, g_right_recv.at[peer])

            @pl.when(is_owner)
            def _():
                for hop in range(1, chips):
                    pass_hop(source, peer, hop).start()

            pl.when(same_side)(pass_twin(source, peer).start)
        else:

            @pl.when(jnp.logical_not(is_owner))
            def _():
                arrived(source, g_right_recv.at[peer])

            pl.when(jnp.logical_and(same_side, jnp.logical_not(is_owner)))(
                pass_twin(source, peer).start
            )

    fill_weights(blocks, final_ref, wide_ref, weight_w, weight_t_ref)
    fill_tables(
        rows, cols, labels_ref, counts_ref, row, col, table_ref, inverse_ref, over_ref
    )
    place_of = lax.broadcasted_iota(jnp.int32, (tile, span), 1) // size
    seq = lax.broadcasted_iota(jnp.int32, (seqs, LANES), 0).astype(f32)
    for chain in range(keep.shape[0]):
        kept = jnp.where(seq < table_ref[chain : chain + 1, :], 1.0, 0.0)
        keep[chain] = kept.astype(bf16)
        keep_t[chain] = kept.T.astype(bf16)
    for t in range(steps):
        inverses[t] = inverse_ref[t * tile : (t + 1) * tile, :]
        line = jnp.zeros((tile, span), jnp.int32)
        for i in range(tile):
            line = jnp.where(place_of == i, labels_ref[row * rows + t * tile + i], line)
        label_lanes[t] = line
    spread[...] = jnp.zeros_like(spread)
    weight_acc[...] = jnp.zeros_like(weight_acc)
    outer_more[0] = jnp.zeros(outer_more.shape[1:], bf16)
    left_more[0] = jnp.zeros(left_more.shape[1:], f32)
    for copy in grad_copies:
        copy.wait()

    def fill_spread(t):
        for i in range(tile):
            part = grad[t, i * cols : (i + 1) * cols, :]
            for e in range(inner):
                spread[i * LANES + e * cols : i * LANES + (e + 1) * cols, e * CZ : (e + 1) * CZ] = (
                    part
                )

    def scale(step, carry):
        fill_spread(step)
        inverse = inverses[step]
        for i in range(0, tile, 2):
            back = lax.dot_general(
                weight_w[...], spread[i * LANES : (i + 2) * LANES, :], (((1,), (1,)), ((), ())),
                preferred_element_type=f32,
            )
            for k in range(2):
                value = (
                    back[:, k * LANES : (k + 1) * LANES] * inverse[i + k : i + k + 1]
                ).astype(bf16)
                for b in range(blocks):
                    scaled[
                        step, (i + k) * size : (i + k + 1) * size, b * LANES : (b + 1) * LANES
                    ] = value[b * size : (b + 1) * size]
        for off in range(n_col - 1):
            pl.when(step == min(2 * off + 1, steps - 1))(functools.partial(pass_right, off))
        return carry

    lax.fori_loop(0, steps, scale, 0)
    pass_right(n_col - 1)
    pl.when(is_owner)(own_right.wait)
    own_left.wait()
    for b in range(blocks):
        right_t[b * LANES : (b + 1) * LANES, :] = right_panel[:, b * LANES : (b + 1) * LANES].T

    offset = row * rows
    label_of = lambda t, i: labels_ref[offset + t * tile + i]
    lows = [label_of(t, 0) for t in range(steps)]
    more = [lax.div(label_of(t, tile - 1) - lows[t], jnp.int32(2)) for t in range(steps)]
    ends, end = [], 0
    for t in range(steps):
        end = end + more[t]
        ends.append(end)

    flag = lambda test: test.astype(jnp.int32)

    def extra_of(u):
        t = sum([flag(ends[k] <= u) for k in range(steps)])
        chain = flag(t == steps) * CHAINS
        for k in range(steps):
            chain = chain + flag(t == k) * (lows[k] + 2 * (u - ends[k] + more[k] + 1))
        return t - flag(t == steps), chain

    def slot_of(t):
        return sum([flag(t == k) * flag(more[k] > 0) * ends[k] for k in range(steps)])

    def same_of(u):
        return flag(extra_of(u)[0] == extra_of(u - 1)[0]).astype(f32)

    def build(t, chain, place):
        lane = label_lanes[t][:1]
        left = left_tiles[t]
        for k in range(2):
            slots[place, k * seqs : (k + 1) * seqs, :] = left * jnp.where(
                lane == chain + k, 1.0, 0.0
            ).astype(bf16)
        return slots[place]

    def forward(t, chain, place, store):
        both_t = build(t, chain, place).T
        inverse = inverses[t]
        kept = [jnp.concatenate([keep[chain + k]] * (width // LANES), axis=1) for k in range(2)]
        for c in range(chunks):
            lanes = slice(c * width, (c + 1) * width)
            right = right_panel[:, lanes]
            right = jnp.concatenate([right * kept[0], right * kept[1]], axis=0)
            prod = jnp.dot(both_t, right, preferred_element_type=f32)
            for i in range(tile):
                for b in range(width // LANES):
                    first = (c * (width // LANES) + b) * size
                    store(
                        slice(first, first + size), slice(i * LANES, (i + 1) * LANES),
                        (
                            prod[i * size : (i + 1) * size, b * LANES : (b + 1) * LANES]
                            * inverse[i : i + 1]
                        ).astype(bf16),
                    )

    def forward_main(t, carry):
        def store(where, lanes, value):
            outer[t, where, lanes] = value

        forward(t, label_of(t, 0), t, store)
        fill_spread(t)
        weight_acc[...] += jnp.dot(outer[t], spread[...], preferred_element_type=f32)
        return carry

    for h in range(parts):
        for off in range(1, n_col):
            peer = (col + off) % n_col
            arrived(tiles_of(peer, h), g_left_recv.at[peer, h])
        lax.fori_loop(h * group, (h + 1) * group, forward_main, 0)

    def forward_more(u, carry):
        t, chain = extra_of(u)
        same = jnp.full((size, LANES), same_of(u), f32).astype(bf16)

        def store(where, lanes, value):
            outer_own[where, lanes] = value
            outer_more[u + 1, where, lanes] = value + outer_more[u, where, lanes] * same

        forward(t, chain, steps + u, store)
        fill_spread(t)
        weight_acc[...] += jnp.dot(outer_own[...], spread[...], preferred_element_type=f32)
        return carry

    lax.fori_loop(0, extras, forward_more, 0)
    extent = blocks * size
    for e in range(inner):
        weight_ref[e * extent : (e + 1) * extent, :] = weight_acc[
            :, e * CZ : (e + 1) * CZ
        ].astype(bf16)
    w1_copy.start()

    def left_part(t, chain):
        tall = jnp.zeros((span, 2 * seqs), f32)
        for c in range(chunks):
            lanes = slice(c * width, (c + 1) * width)
            kept = [
                jnp.concatenate([keep_t[chain + k]] * (width // LANES), axis=0) for k in range(2)
            ]
            right = right_t[lanes, :]
            right = jnp.concatenate([right * kept[0], right * kept[1]], axis=1)
            tall = tall + jnp.dot(scaled[t, :, lanes], right, preferred_element_type=f32)
        turned = tall.T
        lane = label_lanes[t][:1]
        return jnp.where(lane == chain, turned[:seqs], 0.0) + jnp.where(
            lane == chain + 1, turned[seqs:], 0.0
        )

    def left_extra(u, carry):
        t, chain = extra_of(u)
        left_more[u + 1] = left_part(t, chain) + left_more[u] * same_of(u)
        return carry

    lax.fori_loop(0, extras, left_extra, 0)
    after_left_extra()

    def left_main(t, carry):
        slot = slot_of(t)
        turned = left_part(t, label_of(t, 0)) + left_more[slot]
        lanes = pl.ds(pl.multiple_of(t * span, span), span)
        for q in range(n_col):
            left_ref[q, :, lanes] = turned[q * share : (q + 1) * share].astype(bf16)
        pl.when(t == steps // parts - 1)(first_left)
        return carry

    lax.fori_loop(0, steps, left_main, 0)
    after_left()
    pairs = [(t, label_of(t, 0), t) for t in range(steps)]
    for u in range(extras):
        pairs.append((*extra_of(jnp.int32(u)), steps + u))

    def right_main(c, carry):
        lanes = pl.ds(pl.multiple_of(c * width, width), width)
        total = [jnp.zeros((seqs, LANES), f32) for _ in range(width // LANES)]
        for t, chain, place in pairs:
            out = jnp.dot(slots[place], scaled[t, :, lanes], preferred_element_type=f32)
            kept = [seq < table_ref[pl.ds(chain + k, 1), :] for k in range(2)]
            for b in range(width // LANES):
                part = slice(b * LANES, (b + 1) * LANES)
                total[b] = total[b] + (
                    jnp.where(kept[0], out[:seqs, part], 0.0)
                    + jnp.where(kept[1], out[seqs:, part], 0.0)
                )
        whole = jnp.concatenate(total, axis=1)
        for q in range(n_col):
            right_ref[q, :, lanes] = whole[q * share : (q + 1) * share].astype(bf16)
        pl.when(c == chunks * 3 // 4)(during_right)
        return carry

    lax.fori_loop(0, chunks, right_main, 0)
    after_right()
    lane_group = lax.broadcasted_iota(jnp.int32, (CZ, LANES), 1) // cols

    def pairs_of(t, carry):
        slot = slot_of(t)
        for i in range(0, tile, 2):
            lanes = slice(i * LANES, (i + 2) * LANES)
            both = jnp.dot(
                weight_t_ref[...], outer[t, :, lanes] + outer_more[slot, :, lanes],
                preferred_element_type=f32,
            )
            for k in range(2):
                lanes = slice(k * LANES, (k + 1) * LANES)
                total = both[:CZ, lanes]
                for e in range(1, inner):
                    total = jnp.where(lane_group == e, both[e * CZ : (e + 1) * CZ, lanes], total)
                turned = total.T
                pair = turned[:cols]
                for e in range(1, inner):
                    pair = pair + turned[e * cols : (e + 1) * cols]
                first = pl.multiple_of((t * tile + i + k) * cols, cols)
                pair_out[pl.ds(first, cols), :] = (pair + bias_ref[...]).astype(bf16)
        pl.when(t == min(1, steps - 1))(pair_first)
        pl.when(t == steps // 2)(pair_second)
        pl.when(t == steps - 1)(pair_third)
        return carry

    lax.fori_loop(0, steps, pairs_of, 0)
    finish()
    for t in range(ratio):
        pl.when(row * ratio + t != col)(out_right(t).wait_send)
    for h in range(parts):
        for d in range(1, n_col):
            for on, copy in out_left(d, h):
                pl.when(on)(copy.wait_send)

    @pl.when(is_owner)
    def _():
        for index in range(n_col):
            for hop in range(1, chips):
                pass_hop(block(index), index, hop).wait_send()

    @pl.when(same_side)
    def _():
        for index in range(n_col):
            pass_twin(block(index), index).wait_send()


def finish_kernel(
    fused, blocks,
    left_in, right_in, weight_in, pair_in,
    left_out, right_out, weight_out, pair_out,
    left, right, weight, pair, right_done, weight_done, in_sem, out_sem, *more,
):
    f32, bf16 = jnp.float32, jnp.bfloat16
    size = PROJECTED_SIZE
    takes = [
        pltpu.make_async_copy(source, target, in_sem.at[k])
        for k, (source, target) in enumerate(
            ((weight_in, weight), (right_in, right), (left_in, left), (pair_in, pair))
        )
    ]
    gives = [
        pltpu.make_async_copy(source, target, out_sem.at[k])
        for k, (source, target) in enumerate(
            (
                (weight_done, weight_out),
                (right_done if fused else right, right_out),
                (left, left_out),
                (pair, pair_out),
            )
        )
    ]
    for copy in takes:
        copy.start()
    takes[0].wait()
    for g in range(size):
        e = (g % blocks) * (size // blocks) + g // blocks
        weight_done[pl.ds(e, size, stride=size), :] = weight[
            g * size : (g + 1) * size, :
        ].astype(f32) * (1.0 / WINDOW_AMINOS)
    gives[0].start()
    takes[1].wait()
    for k in range(2, 4):
        takes[k].wait()
        gives[k].start()
    if fused:
        turn_ref, line_ref = more
        share = right.shape[1]
        low = share // 2
        rows = line_ref.shape[0] // share
        near = lax.broadcasted_iota(jnp.int32, (low, LANES), 1) < rows
        for b in range(size // 2):
            lanes = slice(b * LANES, (b + 1) * LANES)
            above = right[0, :low, lanes].astype(f32)
            below = right[0, low:, lanes].astype(f32)
            turn_ref[pl.ds(2 * b, low, stride=size), :] = jnp.where(
                near, above, pltpu.roll(below, rows, 1)
            )
            turn_ref[pl.ds(2 * b + 1, low, stride=size), :] = jnp.where(
                near, pltpu.roll(above, rows, 1), below
            )
        fold = LANES // size
        for p in range(low):
            turned = jnp.concatenate([turn_ref[p * size : (p + 1) * size, :]] * fold, axis=0).T
            line_ref[p * rows : (p + 1) * rows, :] = turned[:rows]
            line_ref[(p + low) * rows : (p + low + 1) * rows, :] = turned[rows:]
        place = lax.broadcasted_iota(jnp.int32, (share, LANES), 1) // size
        for g in range(rows // fold):
            total = line_ref[pl.ds(g * fold, share, stride=rows), :]
            for k in range(1, fold):
                total = jnp.where(
                    place == k, line_ref[pl.ds(g * fold + k, share, stride=rows), :], total
                )
            right_done[:, g * LANES : (g + 1) * LANES] = total.astype(bf16)
    gives[1].start()
    for copy in gives:
        copy.wait()


def shards(
    alignment_tensor,
    standardizer_scaling,
    standardizer_offset,
    first_projector,
    second_projector,
    final_projector,
    final_offset,
    amino_strand_label,
    matched_strand_count,
    couple_delta_adjoint,
):
    f32, bf16 = jnp.float32, jnp.bfloat16
    share, rows, feats = alignment_tensor.shape
    cols = couple_delta_adjoint.shape[1]
    size = PROJECTED_SIZE
    n_row, n_col = lax.axis_size("row"), lax.axis_size("col")
    ratio = rows // cols
    seqs = share * n_col
    inner = LANES // cols
    blocks = size // inner
    wide = size * cols
    vmem = pl.BlockSpec(memory_space=pltpu.VMEM)
    dma = pltpu.SemaphoreType.DMA

    tile = 8
    steps = rows // tile
    fused = ratio == 1 and 2 * rows == LANES and share % 16 == 0
    span = tile * size
    if fused:
        sources = (
            alignment_tensor, standardizer_scaling[None, :], standardizer_offset[None, :],
            first_projector.T, second_projector.T,
        )
        extra = [
            pltpu.VMEM((share * rows, feats), bf16),
            pltpu.VMEM((share * rows, LANES), f32),
            pltpu.VMEM((share // 2 * size, LANES), f32),
            pltpu.VMEM((steps, share, span), bf16),
            pltpu.VMEM((ratio, share, wide), bf16),
        ]
    else:
        entries = standardize_entries(
            alignment_tensor, standardizer_scaling, standardizer_offset
        ).reshape(-1, feats)
        both = jnp.dot(
            entries,
            jnp.concatenate([first_projector, second_projector], axis=1),
            preferred_element_type=f32,
        ).astype(bf16)
        left_own = both[:, :size].reshape(share, steps, span).transpose(1, 0, 2)
        right_own = (
            both[:, size:]
            .reshape(share, ratio, cols, size)
            .transpose(1, 0, 3, 2)
            .reshape(ratio, share, wide)
        )
        sources, extra = (left_own, right_own), []
    flat_grad = couple_delta_adjoint.reshape(-1, CZ)
    smem = pl.BlockSpec(memory_space=pltpu.SMEM)
    hbm = pl.BlockSpec(memory_space=pl.ANY)
    chips = n_row // 2
    many = n_col // n_row
    quarter = size * size // n_row
    piece = quarter // n_col
    extras = min(CHAINS - 1, rows - 1) // 2
    pair, left_sum, right_sum, weight_total = pl.pallas_call(
        functools.partial(core_kernel, n_row, n_col, ratio, rows, cols, tile, fused),
        in_specs=[smem, smem, vmem, vmem, hbm] + [vmem] * len(sources),
        out_specs=[vmem] * 4,
        out_shape=[
            jax.ShapeDtypeStruct((rows * cols, CZ), bf16),
            jax.ShapeDtypeStruct((share, rows * size), bf16),
            jax.ShapeDtypeStruct((ratio, share, wide), bf16),
            jax.ShapeDtypeStruct((size * size, CZ), bf16),
        ],
        scratch_shapes=[
            *extra,
            pltpu.VMEM((2 * CHAINS, LANES), f32),
            pltpu.VMEM((2 * CHAINS, LANES), f32),
            pltpu.VMEM((rows, LANES), f32),
            pltpu.VMEM((size * size, CZ), f32),
            pltpu.VMEM((blocks * size, inner * CZ), bf16),
            pltpu.VMEM((inner * CZ, blocks * size), bf16),
            pltpu.VMEM((steps, seqs, span), bf16),
            pltpu.VMEM((seqs, wide), bf16),
            dma((2, n_col, 2)), dma((n_col, 2)), dma((ratio,)), dma((n_col,)),
            dma((n_col, chips)), dma((n_col,)), dma((2,)),
            pltpu.VMEM((steps, tile * cols, CZ), bf16),
            pltpu.VMEM((steps, span, wide), bf16),
            pltpu.VMEM((tile * LANES, inner * CZ), bf16),
            pltpu.VMEM((steps, blocks * size, tile * LANES), bf16),
            pltpu.VMEM((blocks * size, tile * LANES), bf16),
            pltpu.VMEM((extras + 1, blocks * size, tile * LANES), bf16),
            pltpu.VMEM((extras + 1, seqs, span), f32),
            pltpu.VMEM((steps + extras, 2 * seqs, span), bf16),
            pltpu.VMEM((steps, tile, LANES), f32),
            pltpu.VMEM((steps, tile, span), jnp.int32),
            pltpu.VMEM((wide, seqs), bf16),
            pltpu.VMEM((CHAINS + 2, seqs, LANES), bf16),
            pltpu.VMEM((CHAINS + 2, LANES, seqs), bf16),
            pltpu.VMEM((blocks * size, inner * CZ), f32),
            pltpu.VMEM((n_col, share, rows * size), bf16),
            pltpu.VMEM((n_col, share, wide), bf16),
            pltpu.VMEM((size * size, CZ), bf16),
            dma((steps,)),
            pltpu.VMEM((n_col, share, rows * size), bf16),
            pltpu.VMEM((n_col // 2, share, wide), bf16),
            pltpu.VMEM((n_col // 2, share, wide), bf16),
            pltpu.VMEM((chips, many, share, wide), bf16),
            pltpu.VMEM((many, share, wide), bf16),
            pltpu.VMEM((chips * quarter, CZ), bf16),
            pltpu.VMEM((chips * quarter, CZ), bf16),
            pltpu.VMEM((chips, quarter, CZ), bf16),
            pltpu.VMEM((quarter, CZ), bf16),
            pltpu.VMEM((n_col, piece, CZ), bf16),
            pltpu.VMEM((piece, CZ), bf16),
            dma((n_col, 2)), dma((n_col, 2)), dma((n_col, 2)),
            dma, dma,
            dma((chips,)), dma((chips,)),
            dma((many,)), dma((ratio,)), dma,
            dma, dma,
            dma((chips,)), dma((chips,)),
            dma((n_col,)), dma((n_col,)), dma((n_col,)),
            dma((n_col, chips)), dma((n_row, n_col)), dma((n_row, n_col)),
        ],
        compiler_params=pltpu.CompilerParams(
            collective_id=0, has_side_effects=True, vmem_limit_bytes=60 * 1024 * 1024
        ),
    )(
        amino_strand_label,
        matched_strand_count,
        final_projector,
        final_offset[None, :],
        flat_grad,
        *sources,
    )
    adjoint_first_factor, grad_right, grad_w_out, pair = pl.pallas_call(
        functools.partial(finish_kernel, fused, blocks),
        in_specs=[hbm] * 4,
        out_specs=[hbm] * 4,
        out_shape=[
            jax.ShapeDtypeStruct((share, rows * size), bf16),
            jax.ShapeDtypeStruct((share, rows * size) if fused else (ratio, share, wide), bf16),
            jax.ShapeDtypeStruct((size * size, CZ), f32),
            jax.ShapeDtypeStruct((rows * cols, CZ), bf16),
        ],
        scratch_shapes=[
            pltpu.VMEM((share, rows * size), bf16),
            pltpu.VMEM((ratio, share, wide), bf16),
            pltpu.VMEM((size * size, CZ), bf16),
            pltpu.VMEM((rows * cols, CZ), bf16),
            pltpu.VMEM((share, rows * size), bf16),
            pltpu.VMEM((size * size, CZ), f32),
            dma((4,)), dma((4,)),
        ]
        + (
            [pltpu.VMEM((share // 2 * size, LANES), f32), pltpu.VMEM((share * rows, LANES), f32)]
            if fused
            else []
        ),
    )(left_sum, right_sum, weight_total, pair)
    pair_update = pair.reshape(rows, cols, CZ)
    if not fused:
        grad_right = (
            grad_right.reshape(ratio, share, size, cols)
            .transpose(1, 0, 3, 2)
            .reshape(share, rows * size)
        )
    return (pair_update, adjoint_first_factor, grad_right, grad_w_out)


def solution(mesh):
    in_specs = (
        P(("parts", "col"), "row", None),
        P(),
        P(),
        P(),
        P(),
        P(),
        P(),
        P("parts"),
        P("parts", None),
        P(("parts", "row"), "col", None),
    )
    out_specs = (
        P(("parts", "row"), "col", None),
        P(("parts", "col"), "row"),
        P(("parts", "col"), "row"),
        P("parts", None),
    )
    return jax.shard_map(shards, mesh=mesh, in_specs=in_specs, out_specs=out_specs, check_vma=False)
```

```python
import functools

import jax
import jax.numpy as jnp
from jax import lax
from jax.experimental import pallas as pl
from jax.experimental.pallas import tpu as pltpu
from jax.sharding import PartitionSpec as P

PROJECTED_SIZE = 32
CZ = 128
WINDOW_AMINOS = 256
CHAINS = 8
LANES = 128
MESH = pl.DeviceIdType.MESH


def standardize_entries(alignment_tensor, standard_multiplier, additive_offset):
    incoming_entries = alignment_tensor.astype(jnp.float32)
    center = incoming_entries - jnp.mean(incoming_entries, axis=-1, keepdims=True)
    spread = jnp.mean(center * center, axis=-1, keepdims=True)
    return (center * lax.rsqrt(spread + 1e-05) * standard_multiplier + additive_offset).astype(
        jnp.bfloat16
    )


def to(source, target, send, recv, row, col):
    return pltpu.make_async_remote_copy(
        src_ref=source,
        dst_ref=target,
        send_sem=send,
        recv_sem=recv,
        device_id={"row": row, "col": col},
        device_id_type=MESH,
    )


def arrived(ref, sem):
    pltpu.make_async_copy(ref, ref, sem).wait()


def greet(n_row, n_col, me):
    peers = n_row * n_col
    barrier = pltpu.get_barrier_semaphore()

    def signal(off, carry):
        peer = (me + off) % peers
        pl.semaphore_signal(
            barrier,
            inc=1,
            device_id={"row": peer // n_col, "col": peer % n_col},
            device_id_type=MESH,
        )
        return carry

    lax.fori_loop(1, peers, signal, 0)
    return lambda: pl.semaphore_wait(barrier, peers - 1)


def fill_tables(
    rows, cols, labels_ref, counts_ref, row, col, table_ref, inverse_ref, over_ref
):
    f32 = jnp.float32
    inner = LANES // cols
    lane = lax.broadcasted_iota(jnp.int32, (1, LANES), 1) % cols
    label = jnp.zeros((1, LANES), jnp.int32)
    for j in range(cols):
        label = jnp.where(lane == j, labels_ref[col * cols + j], label)
    table_ref[...] = jnp.zeros_like(table_ref)
    for a in range(CHAINS):
        line = jnp.zeros((1, LANES), jnp.int32)
        for b in range(CHAINS):
            line = jnp.where(label == b, counts_ref[a, b], line)
        table_ref[a : a + 1, :] = line.astype(f32)

    over_ref[...] = 1.0 / jnp.maximum(table_ref[...], 1.0)
    for i in range(rows):
        inverse_ref[i : i + 1, :] = over_ref[pl.ds(labels_ref[row * rows + i], 1), :]


def fill_weights(blocks, final_ref, wide_ref, weight_ref, weight_t_ref):
    size = PROJECTED_SIZE
    inner = size // blocks
    wide_ref[...] = final_ref[...].astype(jnp.float32)
    for b in range(blocks):
        for e in range(inner):
            weight_ref[b * size : (b + 1) * size, e * CZ : (e + 1) * CZ] = wide_ref[
                pl.ds(b * inner + e, size, stride=size), :
            ].astype(jnp.bfloat16)
    weight_t_ref[...] = weight_ref[...].T


def project(
    share, rows, align_ref, gain_ref, shift_ref, first_ref, second_ref,
    normed_ref, line_ref, turn_ref, left_own, right_own,
):
    f32, bf16 = jnp.float32, jnp.bfloat16
    size = PROJECTED_SIZE
    feats = align_ref.shape[2]
    gain, shift = gain_ref[...], shift_ref[...]

    def normalise(k, carry):
        x = align_ref[pl.ds(k * 4, 4)].reshape(4 * rows, feats).astype(f32)
        center = x - jnp.mean(x, axis=-1, keepdims=True)
        var = jnp.mean(center * center, axis=-1, keepdims=True)
        normed_ref[pl.ds(pl.multiple_of(k * 4 * rows, 4 * rows), 4 * rows), :] = (
            center * lax.rsqrt(var + 1e-05) * gain + shift
        ).astype(bf16)
        return carry

    lax.fori_loop(0, share // 4, normalise, 0)
    low = share // 2
    second = second_ref[...]
    for p in range(low):
        pair = jnp.concatenate(
            [normed_ref[p * rows : (p + 1) * rows], normed_ref[(p + low) * rows : (p + low + 1) * rows]],
            axis=0,
        )
        turn_ref[p * size : (p + 1) * size, :] = lax.dot_general(
            second, pair, (((1,), (1,)), ((), ())), preferred_element_type=f32
        )
    near = lax.broadcasted_iota(jnp.int32, (low, LANES), 1) < rows
    for b in range(size // 2):
        even = turn_ref[pl.ds(2 * b, low, stride=size), :]
        odd = turn_ref[pl.ds(2 * b + 1, low, stride=size), :]
        lanes = slice(b * LANES, (b + 1) * LANES)
        right_own[0, :low, lanes] = jnp.where(near, even, pltpu.roll(odd, rows, 1)).astype(bf16)
        right_own[0, low:, lanes] = jnp.where(near, pltpu.roll(even, rows, 1), odd).astype(bf16)
    yield
    fold = LANES // size
    first = jnp.concatenate([first_ref[...]] * fold, axis=0)
    line_ref[...] = lax.dot_general(
        normed_ref[...], first, (((1,), (1,)), ((), ())), preferred_element_type=f32
    )
    place = lax.broadcasted_iota(jnp.int32, (share, LANES), 1) // size
    for g in range(rows // fold):
        total = line_ref[pl.ds(g * fold, share, stride=rows), :]
        for k in range(1, fold):
            total = jnp.where(
                place == k, line_ref[pl.ds(g * fold + k, share, stride=rows), :], total
            )
        span = left_own.shape[2]
        lanes = slice(g * LANES % span, g * LANES % span + LANES)
        left_own[g * LANES // span, :, lanes] = total.astype(bf16)
    yield


def core_kernel(n_row, n_col, ratio, rows, cols, tile, fused, *refs):
    f32, bf16 = jnp.float32, jnp.bfloat16
    size = PROJECTED_SIZE
    inner = LANES // cols
    blocks = size // inner
    steps = rows // tile
    span = tile * size
    labels_ref, counts_ref, final_ref, bias_ref, grad_hbm = refs[:5]
    count = 10 if fused else 7
    source_refs = refs[5:count]
    pair_out, left_out, right_out, weight_out = refs[count : count + 4]
    refs = refs[count + 4 :]
    if fused:
        normed_ref, line_ref, turn_ref, left_own, right_own = refs[:5]
        refs = refs[5:]
    else:
        left_own, right_own = source_refs
    (
        table_ref, over_ref, inverse_ref, wide_ref, weight_w, weight_t_ref, left_tiles, right_panel,
        g_left_send, g_left_recv, g_right_send, g_right_recv, g_hop_send, g_twin_send, g_own_sem,
        grad, scaled, spread, outer, outer_own, outer_more, left_more, slots, inverses, label_lanes,
        right_t, keep, keep_t, weight_acc, left_ref, right_ref, weight_ref, local_sem,
        left_in, right_twin, right_half, right_mid, right_sum,
        weight_twin, weight_half, weight_mid, weight_sum, weight_in, weight_part,
        up_send, down_send, left_recv, twin_send, twin_recv, mid_send, mid_recv,
        right_send, right_recv, own_sem,
        w1_send, w1_recv, w2_send, w2_recv, w3_send, w3_recv, around_send, hop_send, last_send,
        all_recv,
    ) = refs
    row, col = lax.axis_index("row"), lax.axis_index("col")
    ready = greet(n_row, n_col, row * n_col + col)
    grad_copies = [
        pltpu.make_async_copy(
            grad_hbm.at[pl.ds(t * tile * cols, tile * cols)], grad.at[t], local_sem.at[t]
        )
        for t in range(steps)
    ]
    for copy in grad_copies:
        copy.start()
    seqs, wide = right_panel.shape
    share = seqs // n_col
    width = 2 * LANES if blocks % 2 == 0 else LANES
    chunks = blocks * LANES // width
    extras = outer_more.shape[0] - 1
    chips = n_row // 2
    chip, side = row // 2, row % 2
    twin = row + 1 - 2 * side
    many = n_col // n_row
    half = n_col // 2
    quarter = weight_ref.shape[0] // n_row
    piece = quarter // n_col
    parts = left_recv.shape[1]
    part = left_ref.shape[2] // parts
    owner, slot = col // ratio, col % ratio
    rows_of = lambda index, extent: pl.ds(pl.multiple_of(index * extent, extent), extent)
    mine = side * chips + chip
    add = lambda *terms: functools.reduce(lambda a, b: a + b, [t.astype(f32) for t in terms])

    w1_copy = to(
        weight_ref.at[rows_of(1 - side, chips * quarter)], weight_twin, w1_send, w1_recv, twin, col
    )
    right_parts = twin_recv.shape[0]
    right_part = right_twin.shape[2] // right_parts
    right_lanes = lambda h: slice(h * right_part, (h + 1) * right_part)

    def twin_copy(h):
        return to(
            right_ref.at[rows_of(1 - side, half), :, right_lanes(h)],
            right_twin.at[:, :, right_lanes(h)], twin_send.at[h], twin_recv.at[h], twin, col,
        )

    def w2_copy(off):
        peer = (chip + off) % chips
        return to(
            weight_half.at[rows_of(peer, quarter)], weight_mid.at[chip], w2_send.at[off],
            w2_recv.at[chip], 2 * peer + side, col,
        )

    def mid_copy(off, h):
        peer = (chip + off) % chips
        return to(
            right_half.at[rows_of(peer, many), :, right_lanes(h)],
            right_mid.at[chip, :, :, right_lanes(h)], mid_send.at[off, h],
            mid_recv.at[chip, h], 2 * peer + side, col,
        )

    def right_copy(b, h):
        return to(
            right_sum.at[b, :, right_lanes(h)], right_out.at[slot, :, right_lanes(h)],
            right_send.at[b, h], right_recv.at[slot, h], owner, mine * many + b,
        )

    def left_copies(d, h):
        lanes = slice(h * part, (h + 1) * part)
        for step, sends in ((d, up_send), (-d, down_send)):
            there = col + step
            peer = there % n_col
            copy = to(
                left_ref.at[peer, :, lanes], left_in.at[col, :, lanes], sends.at[d, h],
                left_recv.at[col, h], row, peer,
            )
            yield jnp.logical_and(there >= 0, there < n_col), copy

    def left_start(d, h):
        for on, copy in left_copies(d, h):
            pl.when(on)(copy.start)

    def w3_copy(off):
        peer = (col + off) % n_col
        return to(
            weight_sum.at[rows_of(peer, piece)], weight_in.at[col], w3_send.at[off],
            w3_recv.at[col], row, peer,
        )

    def cell(group, index):
        return weight_out.at[rows_of(group * n_col + index, piece)]

    def spread_copy(send, group, index, to_row, to_col, source=None):
        there = cell(group, index)
        return to(
            there if source is None else source, there, send, all_recv.at[group, index],
            to_row, to_col,
        )

    def around_copy(off):
        return spread_copy(around_send.at[off], mine, col, row, (col + off) % n_col, weight_part)

    def hop_copy(index, off, source=None):
        peer = (chip + off) % chips
        return spread_copy(hop_send.at[index, off], mine, index, 2 * peer + side, col, source)

    def last_copy(group, index, source=None):
        return spread_copy(last_send.at[group, index], group, index, twin, col, source)

    def group_of(off):
        return side * chips + (chip + off) % chips

    def here(b):
        return jnp.logical_and(owner == row, mine * many + b == col)


    own_piece = pltpu.make_async_copy(weight_part, cell(mine, col), own_sem)

    def after_left_extra():
        arrived(weight_twin, w1_recv)
        weight_half[...] = add(
            weight_ref[rows_of(side, chips * quarter), :], weight_twin[...]
        ).astype(bf16)
        for off in range(1, chips):
            w2_copy(off).start()

    def first_left():
        for d in range(1, n_col):
            left_start(d, 0)

    def after_left():
        total = weight_half[rows_of(chip, quarter), :].astype(f32)
        for off in range(1, chips):
            peer = (chip + off) % chips
            arrived(weight_mid.at[peer], w2_recv.at[peer])
            total = add(total, weight_mid[peer])
        weight_sum[...] = total.astype(bf16)
        for off in range(1, n_col):
            w3_copy(off).start()
        for h in range(1, parts):
            for d in range(1, n_col):
                left_start(d, h)

    def during_right():
        total = weight_sum[rows_of(col, piece), :].astype(f32)
        for off in range(1, n_col):
            peer = (col + off) % n_col
            arrived(weight_in.at[peer], w3_recv.at[peer])
            total = add(total, weight_in[peer])
        weight_part[...] = total.astype(bf16)
        own_piece.start()
        for off in range(1, n_col):
            around_copy(off).start()
        for off in range(1, chips):
            hop_copy(col, off, weight_part).start()
        last_copy(mine, col, weight_part).start()

    def right_first(h):
        twin_copy(h).start()

    def right_second(h):
        lanes = right_lanes(h)
        arrived(right_twin.at[:, :, lanes], twin_recv.at[h])
        right_half[:, :, lanes] = add(
            right_ref[rows_of(side, half), :, lanes], right_twin[:, :, lanes]
        ).astype(bf16)
        for off in range(1, chips):
            mid_copy(off, h).start()

    def right_third(h):
        lanes = right_lanes(h)
        total = right_half[rows_of(chip, many), :, lanes].astype(f32)
        for off in range(1, chips):
            peer = (chip + off) % chips
            arrived(right_mid.at[peer, :, :, lanes], mid_recv.at[peer, h])
            total = add(total, right_mid[peer, :, :, lanes])
        right_sum[:, :, lanes] = total.astype(bf16)
        for b in range(many):
            pl.when(jnp.logical_not(here(b)))(right_copy(b, h).start)
            own = pltpu.make_async_copy(
                right_sum.at[b, :, lanes], right_out.at[slot, :, lanes], right_recv.at[slot, h]
            )
            pl.when(here(b))(own.start)

    def pair_second():
        for off in range(1, n_col):
            peer = (col + off) % n_col
            arrived(cell(mine, peer), all_recv.at[mine, peer])
            for hop in range(1, chips):
                hop_copy(peer, hop).start()
            last_copy(mine, peer).start()

    def finish():
        for off in range(n_col):
            peer = (col + off) % n_col
            for hop in range(1, chips):
                arrived(cell(group_of(hop), peer), all_recv.at[group_of(hop), peer])
                last_copy(group_of(hop), peer).start()

        total = left_ref[col].astype(f32)
        for off in range(1, n_col):
            peer = (col + off) % n_col
            for h in range(parts):
                arrived(left_in.at[peer, :, h * part : (h + 1) * part], left_recv.at[peer, h])
            total = add(total, left_in[peer])
        left_out[...] = total.astype(bf16)
        for t in range(ratio):
            for h in range(right_parts):
                arrived(right_out.at[t, :, right_lanes(h)], right_recv.at[t, h])
        for off in range(n_col):
            peer = (col + off) % n_col
            for other in range(chips):
                group = (1 - side) * chips + other
                arrived(cell(group, peer), all_recv.at[group, peer])

        own_piece.wait()
        w1_copy.wait_send()
        for h in range(right_parts):
            twin_copy(h).wait_send()
        for off in range(1, chips):
            w2_copy(off).wait_send()
            for h in range(right_parts):
                mid_copy(off, h).wait_send()
        for off in range(1, n_col):
            w3_copy(off).wait_send()
            around_copy(off).wait_send()
            for h in range(parts):
                for on, copy in left_copies(off, h):
                    pl.when(on)(copy.wait_send)
        for index in range(n_col):
            for off in range(1, chips):
                hop_copy(index, off).wait_send()
            for off in range(chips):
                last_copy(group_of(off), index).wait_send()
        for b in range(many):
            for h in range(right_parts):
                pl.when(jnp.logical_not(here(b)))(right_copy(b, h).wait_send)
    is_owner = row == owner
    same_side = row % 2 == owner % 2
    group = steps // parts
    seq_rows = lambda index: pl.ds(pl.multiple_of(index * share, share), share)
    block = lambda index: right_panel.at[seq_rows(index)]
    tiles_of = lambda index, h: left_tiles.at[h * group : (h + 1) * group, seq_rows(index)]

    def out_right(t):
        return to(
            right_own.at[t], block(col), g_right_send.at[t], g_right_recv.at[col],
            row, row * ratio + t,
        )

    def out_left(d, h):
        for k, step in enumerate((d, -d)):
            there = col + step
            copy = to(
                left_own.at[h * group : (h + 1) * group], tiles_of(col, h),
                g_left_send.at[k, d, h], g_left_recv.at[col, h], row, there % n_col,
            )
            yield jnp.logical_and(there >= 0, there < n_col), copy

    def pass_hop(source, index, hop):
        return to(
            source, block(index), g_hop_send.at[index, hop], g_right_recv.at[index],
            (row + 2 * hop) % n_row, col,
        )

    def pass_twin(source, index):
        return to(source, block(index), g_twin_send.at[index], g_right_recv.at[index], twin, col)

    if fused:
        work = project(
            share, rows, *source_refs, normed_ref, line_ref, turn_ref, left_own, right_own
        )
        next(work)
    ready()
    for t in range(ratio):
        pl.when(row * ratio + t != col)(out_right(t).start)
    own_block = right_own.at[col % ratio]
    own_right = pltpu.make_async_copy(own_block, block(col), g_own_sem.at[1])

    @pl.when(is_owner)
    def _():
        own_right.start()
        for hop in range(1, chips):
            pass_hop(own_block, col, hop).start()
        pass_twin(own_block, col).start()

    if fused:
        next(work)
    own_left = pltpu.make_async_copy(left_own, left_tiles.at[:, seq_rows(col)], g_own_sem.at[0])
    own_left.start()
    for h in range(parts):
        for d in range(1, n_col):
            for on, copy in out_left(d, h):
                pl.when(on)(copy.start)

    def pass_right(off):
        peer = (col + off) % n_col
        source = block(peer)
        if off:
            arrived(source, g_right_recv.at[peer])

            @pl.when(is_owner)
            def _():
                for hop in range(1, chips):
                    pass_hop(source, peer, hop).start()

            pl.when(same_side)(pass_twin(source, peer).start)
        else:

            @pl.when(jnp.logical_not(is_owner))
            def _():
                arrived(source, g_right_recv.at[peer])

            pl.when(jnp.logical_and(same_side, jnp.logical_not(is_owner)))(
                pass_twin(source, peer).start
            )

    fill_weights(blocks, final_ref, wide_ref, weight_w, weight_t_ref)
    fill_tables(
        rows, cols, labels_ref, counts_ref, row, col, table_ref, inverse_ref, over_ref
    )
    place_of = lax.broadcasted_iota(jnp.int32, (tile, span), 1) // size
    seq = lax.broadcasted_iota(jnp.int32, (seqs, LANES), 0).astype(f32)
    for chain in range(keep.shape[0]):
        kept = jnp.where(seq < table_ref[chain : chain + 1, :], 1.0, 0.0)
        keep[chain] = kept.astype(bf16)
        keep_t[chain] = kept.T.astype(bf16)
    for t in range(steps):
        inverses[t] = inverse_ref[t * tile : (t + 1) * tile, :]
        line = jnp.zeros((tile, span), jnp.int32)
        for i in range(tile):
            line = jnp.where(place_of == i, labels_ref[row * rows + t * tile + i], line)
        label_lanes[t] = line
    spread[...] = jnp.zeros_like(spread)
    weight_acc[...] = jnp.zeros_like(weight_acc)
    outer_more[0] = jnp.zeros(outer_more.shape[1:], bf16)
    left_more[0] = jnp.zeros(left_more.shape[1:], f32)
    for copy in grad_copies:
        copy.wait()

    def fill_spread(t):
        for i in range(tile):
            part = grad[t, i * cols : (i + 1) * cols, :]
            for e in range(inner):
                spread[i * LANES + e * cols : i * LANES + (e + 1) * cols, e * CZ : (e + 1) * CZ] = (
                    part
                )

    def scale(step, carry):
        fill_spread(step)
        inverse = inverses[step]
        for i in range(0, tile, 2):
            back = lax.dot_general(
                weight_w[...], spread[i * LANES : (i + 2) * LANES, :], (((1,), (1,)), ((), ())),
                preferred_element_type=f32,
            )
            for k in range(2):
                value = (
                    back[:, k * LANES : (k + 1) * LANES] * inverse[i + k : i + k + 1]
                ).astype(bf16)
                for b in range(blocks):
                    scaled[
                        step, (i + k) * size : (i + k + 1) * size, b * LANES : (b + 1) * LANES
                    ] = value[b * size : (b + 1) * size]
        for off in range(n_col - 1):
            pl.when(step == min(2 * off + 1, steps - 1))(functools.partial(pass_right, off))
        return carry

    lax.fori_loop(0, steps, scale, 0)
    pass_right(n_col - 1)
    pl.when(is_owner)(own_right.wait)
    own_left.wait()
    for b in range(blocks):
        right_t[b * LANES : (b + 1) * LANES, :] = right_panel[:, b * LANES : (b + 1) * LANES].T

    offset = row * rows
    label_of = lambda t, i: labels_ref[offset + t * tile + i]
    lows = [label_of(t, 0) for t in range(steps)]
    more = [lax.div(label_of(t, tile - 1) - lows[t], jnp.int32(2)) for t in range(steps)]
    ends, end = [], 0
    for t in range(steps):
        end = end + more[t]
        ends.append(end)

    flag = lambda test: test.astype(jnp.int32)

    def extra_of(u):
        t = sum([flag(ends[k] <= u) for k in range(steps)])
        chain = flag(t == steps) * CHAINS
        for k in range(steps):
            chain = chain + flag(t == k) * (lows[k] + 2 * (u - ends[k] + more[k] + 1))
        return t - flag(t == steps), chain

    def slot_of(t):
        return sum([flag(t == k) * flag(more[k] > 0) * ends[k] for k in range(steps)])

    def same_of(u):
        return flag(extra_of(u)[0] == extra_of(u - 1)[0]).astype(f32)

    def build(t, chain, place):
        lane = label_lanes[t][:1]
        left = left_tiles[t]
        for k in range(2):
            slots[place, k * seqs : (k + 1) * seqs, :] = left * jnp.where(
                lane == chain + k, 1.0, 0.0
            ).astype(bf16)
        return slots[place]

    def forward(t, chain, place, store):
        both_t = build(t, chain, place).T
        inverse = inverses[t]
        kept = [jnp.concatenate([keep[chain + k]] * (width // LANES), axis=1) for k in range(2)]
        for c in range(chunks):
            lanes = slice(c * width, (c + 1) * width)
            right = right_panel[:, lanes]
            right = jnp.concatenate([right * kept[0], right * kept[1]], axis=0)
            prod = jnp.dot(both_t, right, preferred_element_type=f32)
            for i in range(tile):
                for b in range(width // LANES):
                    first = (c * (width // LANES) + b) * size
                    store(
                        slice(first, first + size), slice(i * LANES, (i + 1) * LANES),
                        (
                            prod[i * size : (i + 1) * size, b * LANES : (b + 1) * LANES]
                            * inverse[i : i + 1]
                        ).astype(bf16),
                    )

    def forward_main(t, carry):
        def store(where, lanes, value):
            outer[t, where, lanes] = value

        forward(t, label_of(t, 0), t, store)
        fill_spread(t)
        weight_acc[...] += jnp.dot(outer[t], spread[...], preferred_element_type=f32)
        return carry

    for h in range(parts):
        for off in range(1, n_col):
            peer = (col + off) % n_col
            arrived(tiles_of(peer, h), g_left_recv.at[peer, h])
        lax.fori_loop(h * group, (h + 1) * group, forward_main, 0)

    def forward_more(u, carry):
        t, chain = extra_of(u)
        same = jnp.full((size, LANES), same_of(u), f32).astype(bf16)

        def store(where, lanes, value):
            outer_own[where, lanes] = value
            outer_more[u + 1, where, lanes] = value + outer_more[u, where, lanes] * same

        forward(t, chain, steps + u, store)
        fill_spread(t)
        weight_acc[...] += jnp.dot(outer_own[...], spread[...], preferred_element_type=f32)
        return carry

    lax.fori_loop(0, extras, forward_more, 0)
    extent = blocks * size
    for e in range(inner):
        weight_ref[e * extent : (e + 1) * extent, :] = weight_acc[
            :, e * CZ : (e + 1) * CZ
        ].astype(bf16)
    w1_copy.start()

    def left_part(t, chain):
        tall = jnp.zeros((span, 2 * seqs), f32)
        for c in range(chunks):
            lanes = slice(c * width, (c + 1) * width)
            kept = [
                jnp.concatenate([keep_t[chain + k]] * (width // LANES), axis=0) for k in range(2)
            ]
            right = right_t[lanes, :]
            right = jnp.concatenate([right * kept[0], right * kept[1]], axis=1)
            tall = tall + jnp.dot(scaled[t, :, lanes], right, preferred_element_type=f32)
        turned = tall.T
        lane = label_lanes[t][:1]
        return jnp.where(lane == chain, turned[:seqs], 0.0) + jnp.where(
            lane == chain + 1, turned[seqs:], 0.0
        )

    def left_extra(u, carry):
        t, chain = extra_of(u)
        left_more[u + 1] = left_part(t, chain) + left_more[u] * same_of(u)
        return carry

    lax.fori_loop(0, extras, left_extra, 0)
    after_left_extra()

    def left_main(t, carry):
        slot = slot_of(t)
        turned = left_part(t, label_of(t, 0)) + left_more[slot]
        lanes = pl.ds(pl.multiple_of(t * span, span), span)
        for q in range(n_col):
            left_ref[q, :, lanes] = turned[q * share : (q + 1) * share].astype(bf16)
        pl.when(t == steps // parts - 1)(first_left)
        return carry

    lax.fori_loop(0, steps, left_main, 0)
    after_left()
    pairs = [(t, label_of(t, 0), t) for t in range(steps)]
    for u in range(extras):
        pairs.append((*extra_of(jnp.int32(u)), steps + u))

    def right_main(c, carry):
        lanes = pl.ds(pl.multiple_of(c * width, width), width)
        total = [jnp.zeros((seqs, LANES), f32) for _ in range(width // LANES)]
        for t, chain, place in pairs:
            out = jnp.dot(slots[place], scaled[t, :, lanes], preferred_element_type=f32)
            kept = [seq < table_ref[pl.ds(chain + k, 1), :] for k in range(2)]
            for b in range(width // LANES):
                part = slice(b * LANES, (b + 1) * LANES)
                total[b] = total[b] + (
                    jnp.where(kept[0], out[:seqs, part], 0.0)
                    + jnp.where(kept[1], out[seqs:, part], 0.0)
                )
        whole = jnp.concatenate(total, axis=1)
        for q in range(n_col):
            right_ref[q, :, lanes] = whole[q * share : (q + 1) * share].astype(bf16)
        pl.when(c == chunks // 2 - 1)(functools.partial(right_first, 0))
        pl.when(c == max(chunks - 2, chunks // 2))(functools.partial(right_second, 0))
        pl.when(c == chunks * 3 // 4)(during_right)
        return carry

    lax.fori_loop(0, chunks, right_main, 0)
    right_first(1)
    lane_group = lax.broadcasted_iota(jnp.int32, (CZ, LANES), 1) // cols

    def pairs_of(t, carry):
        slot = slot_of(t)
        for i in range(0, tile, 2):
            lanes = slice(i * LANES, (i + 2) * LANES)
            both = jnp.dot(
                weight_t_ref[...], outer[t, :, lanes] + outer_more[slot, :, lanes],
                preferred_element_type=f32,
            )
            for k in range(2):
                lanes = slice(k * LANES, (k + 1) * LANES)
                total = both[:CZ, lanes]
                for e in range(1, inner):
                    total = jnp.where(lane_group == e, both[e * CZ : (e + 1) * CZ, lanes], total)
                turned = total.T
                pair = turned[:cols]
                for e in range(1, inner):
                    pair = pair + turned[e * cols : (e + 1) * cols]
                first = pl.multiple_of((t * tile + i + k) * cols, cols)
                pair_out[pl.ds(first, cols), :] = (pair + bias_ref[...]).astype(bf16)
        pl.when(t == min(3, steps - 1))(functools.partial(right_second, 1))
        pl.when(t == steps // 2)(pair_second)
        pl.when(t == steps * 5 // 8)(functools.partial(right_third, 0))
        pl.when(t == steps - 1)(functools.partial(right_third, 1))
        return carry

    lax.fori_loop(0, steps, pairs_of, 0)
    finish()
    for t in range(ratio):
        pl.when(row * ratio + t != col)(out_right(t).wait_send)
    for h in range(parts):
        for d in range(1, n_col):
            for on, copy in out_left(d, h):
                pl.when(on)(copy.wait_send)

    @pl.when(is_owner)
    def _():
        for index in range(n_col):
            for hop in range(1, chips):
                pass_hop(block(index), index, hop).wait_send()

    @pl.when(same_side)
    def _():
        for index in range(n_col):
            pass_twin(block(index), index).wait_send()


def finish_kernel(
    fused, blocks,
    left_in, right_in, weight_in, pair_in,
    left_out, right_out, weight_out, pair_out,
    left, right, weight, pair, right_done, weight_done, in_sem, out_sem, *more,
):
    f32, bf16 = jnp.float32, jnp.bfloat16
    size = PROJECTED_SIZE
    takes = [
        pltpu.make_async_copy(source, target, in_sem.at[k])
        for k, (source, target) in enumerate(
            ((weight_in, weight), (right_in, right), (left_in, left), (pair_in, pair))
        )
    ]
    gives = [
        pltpu.make_async_copy(source, target, out_sem.at[k])
        for k, (source, target) in enumerate(
            (
                (weight_done, weight_out),
                (right_done if fused else right, right_out),
                (left, left_out),
                (pair, pair_out),
            )
        )
    ]
    for copy in takes:
        copy.start()
    takes[0].wait()
    for g in range(size):
        e = (g % blocks) * (size // blocks) + g // blocks
        weight_done[pl.ds(e, size, stride=size), :] = weight[
            g * size : (g + 1) * size, :
        ].astype(f32) * (1.0 / WINDOW_AMINOS)
    gives[0].start()
    takes[1].wait()
    for k in range(2, 4):
        takes[k].wait()
        gives[k].start()
    if fused:
        turn_ref, line_ref = more
        share = right.shape[1]
        low = share // 2
        rows = line_ref.shape[0] // share
        near = lax.broadcasted_iota(jnp.int32, (low, LANES), 1) < rows
        for b in range(size // 2):
            lanes = slice(b * LANES, (b + 1) * LANES)
            above = right[0, :low, lanes].astype(f32)
            below = right[0, low:, lanes].astype(f32)
            turn_ref[pl.ds(2 * b, low, stride=size), :] = jnp.where(
                near, above, pltpu.roll(below, rows, 1)
            )
            turn_ref[pl.ds(2 * b + 1, low, stride=size), :] = jnp.where(
                near, pltpu.roll(above, rows, 1), below
            )
        fold = LANES // size
        for p in range(low):
            turned = jnp.concatenate([turn_ref[p * size : (p + 1) * size, :]] * fold, axis=0).T
            line_ref[p * rows : (p + 1) * rows, :] = turned[:rows]
            line_ref[(p + low) * rows : (p + low + 1) * rows, :] = turned[rows:]
        place = lax.broadcasted_iota(jnp.int32, (share, LANES), 1) // size
        for g in range(rows // fold):
            total = line_ref[pl.ds(g * fold, share, stride=rows), :]
            for k in range(1, fold):
                total = jnp.where(
                    place == k, line_ref[pl.ds(g * fold + k, share, stride=rows), :], total
                )
            right_done[:, g * LANES : (g + 1) * LANES] = total.astype(bf16)
    gives[1].start()
    for copy in gives:
        copy.wait()


def shards(
    alignment_tensor,
    standardizer_scaling,
    standardizer_offset,
    first_projector,
    second_projector,
    final_projector,
    final_offset,
    amino_strand_label,
    matched_strand_count,
    couple_delta_adjoint,
):
    f32, bf16 = jnp.float32, jnp.bfloat16
    share, rows, feats = alignment_tensor.shape
    cols = couple_delta_adjoint.shape[1]
    size = PROJECTED_SIZE
    n_row, n_col = lax.axis_size("row"), lax.axis_size("col")
    ratio = rows // cols
    seqs = share * n_col
    inner = LANES // cols
    blocks = size // inner
    wide = size * cols
    vmem = pl.BlockSpec(memory_space=pltpu.VMEM)
    dma = pltpu.SemaphoreType.DMA

    tile = 8
    steps = rows // tile
    fused = ratio == 1 and 2 * rows == LANES and share % 16 == 0
    span = tile * size
    if fused:
        sources = (
            alignment_tensor, standardizer_scaling[None, :], standardizer_offset[None, :],
            first_projector.T, second_projector.T,
        )
        extra = [
            pltpu.VMEM((share * rows, feats), bf16),
            pltpu.VMEM((share * rows, LANES), f32),
            pltpu.VMEM((share // 2 * size, LANES), f32),
            pltpu.VMEM((steps, share, span), bf16),
            pltpu.VMEM((ratio, share, wide), bf16),
        ]
    else:
        entries = standardize_entries(
            alignment_tensor, standardizer_scaling, standardizer_offset
        ).reshape(-1, feats)
        both = jnp.dot(
            entries,
            jnp.concatenate([first_projector, second_projector], axis=1),
            preferred_element_type=f32,
        ).astype(bf16)
        left_own = both[:, :size].reshape(share, steps, span).transpose(1, 0, 2)
        right_own = (
            both[:, size:]
            .reshape(share, ratio, cols, size)
            .transpose(1, 0, 3, 2)
            .reshape(ratio, share, wide)
        )
        sources, extra = (left_own, right_own), []
    flat_grad = couple_delta_adjoint.reshape(-1, CZ)
    smem = pl.BlockSpec(memory_space=pltpu.SMEM)
    hbm = pl.BlockSpec(memory_space=pl.ANY)
    chips = n_row // 2
    many = n_col // n_row
    quarter = size * size // n_row
    piece = quarter // n_col
    extras = min(CHAINS - 1, rows - 1) // 2
    pair, left_sum, right_sum, weight_total = pl.pallas_call(
        functools.partial(core_kernel, n_row, n_col, ratio, rows, cols, tile, fused),
        in_specs=[smem, smem, vmem, vmem, hbm] + [vmem] * len(sources),
        out_specs=[vmem] * 4,
        out_shape=[
            jax.ShapeDtypeStruct((rows * cols, CZ), bf16),
            jax.ShapeDtypeStruct((share, rows * size), bf16),
            jax.ShapeDtypeStruct((ratio, share, wide), bf16),
            jax.ShapeDtypeStruct((size * size, CZ), bf16),
        ],
        scratch_shapes=[
            *extra,
            pltpu.VMEM((2 * CHAINS, LANES), f32),
            pltpu.VMEM((2 * CHAINS, LANES), f32),
            pltpu.VMEM((rows, LANES), f32),
            pltpu.VMEM((size * size, CZ), f32),
            pltpu.VMEM((blocks * size, inner * CZ), bf16),
            pltpu.VMEM((inner * CZ, blocks * size), bf16),
            pltpu.VMEM((steps, seqs, span), bf16),
            pltpu.VMEM((seqs, wide), bf16),
            dma((2, n_col, 2)), dma((n_col, 2)), dma((ratio,)), dma((n_col,)),
            dma((n_col, chips)), dma((n_col,)), dma((2,)),
            pltpu.VMEM((steps, tile * cols, CZ), bf16),
            pltpu.VMEM((steps, span, wide), bf16),
            pltpu.VMEM((tile * LANES, inner * CZ), bf16),
            pltpu.VMEM((steps, blocks * size, tile * LANES), bf16),
            pltpu.VMEM((blocks * size, tile * LANES), bf16),
            pltpu.VMEM((extras + 1, blocks * size, tile * LANES), bf16),
            pltpu.VMEM((extras + 1, seqs, span), f32),
            pltpu.VMEM((steps + extras, 2 * seqs, span), bf16),
            pltpu.VMEM((steps, tile, LANES), f32),
            pltpu.VMEM((steps, tile, span), jnp.int32),
            pltpu.VMEM((wide, seqs), bf16),
            pltpu.VMEM((CHAINS + 2, seqs, LANES), bf16),
            pltpu.VMEM((CHAINS + 2, LANES, seqs), bf16),
            pltpu.VMEM((blocks * size, inner * CZ), f32),
            pltpu.VMEM((n_col, share, rows * size), bf16),
            pltpu.VMEM((n_col, share, wide), bf16),
            pltpu.VMEM((size * size, CZ), bf16),
            dma((steps,)),
            pltpu.VMEM((n_col, share, rows * size), bf16),
            pltpu.VMEM((n_col // 2, share, wide), bf16),
            pltpu.VMEM((n_col // 2, share, wide), bf16),
            pltpu.VMEM((chips, many, share, wide), bf16),
            pltpu.VMEM((many, share, wide), bf16),
            pltpu.VMEM((chips * quarter, CZ), bf16),
            pltpu.VMEM((chips * quarter, CZ), bf16),
            pltpu.VMEM((chips, quarter, CZ), bf16),
            pltpu.VMEM((quarter, CZ), bf16),
            pltpu.VMEM((n_col, piece, CZ), bf16),
            pltpu.VMEM((piece, CZ), bf16),
            dma((n_col, 2)), dma((n_col, 2)), dma((n_col, 2)),
            dma((2,)), dma((2,)),
            dma((chips, 2)), dma((chips, 2)),
            dma((many, 2)), dma((ratio, 2)), dma,
            dma, dma,
            dma((chips,)), dma((chips,)),
            dma((n_col,)), dma((n_col,)), dma((n_col,)),
            dma((n_col, chips)), dma((n_row, n_col)), dma((n_row, n_col)),
        ],
        compiler_params=pltpu.CompilerParams(
            collective_id=0, has_side_effects=True, vmem_limit_bytes=60 * 1024 * 1024
        ),
    )(
        amino_strand_label,
        matched_strand_count,
        final_projector,
        final_offset[None, :],
        flat_grad,
        *sources,
    )
    adjoint_first_factor, grad_right, grad_w_out, pair = pl.pallas_call(
        functools.partial(finish_kernel, fused, blocks),
        in_specs=[hbm] * 4,
        out_specs=[hbm] * 4,
        out_shape=[
            jax.ShapeDtypeStruct((share, rows * size), bf16),
            jax.ShapeDtypeStruct((share, rows * size) if fused else (ratio, share, wide), bf16),
            jax.ShapeDtypeStruct((size * size, CZ), f32),
            jax.ShapeDtypeStruct((rows * cols, CZ), bf16),
        ],
        scratch_shapes=[
            pltpu.VMEM((share, rows * size), bf16),
            pltpu.VMEM((ratio, share, wide), bf16),
            pltpu.VMEM((size * size, CZ), bf16),
            pltpu.VMEM((rows * cols, CZ), bf16),
            pltpu.VMEM((share, rows * size), bf16),
            pltpu.VMEM((size * size, CZ), f32),
            dma((4,)), dma((4,)),
        ]
        + (
            [pltpu.VMEM((share // 2 * size, LANES), f32), pltpu.VMEM((share * rows, LANES), f32)]
            if fused
            else []
        ),
    )(left_sum, right_sum, weight_total, pair)
    pair_update = pair.reshape(rows, cols, CZ)
    if not fused:
        grad_right = (
            grad_right.reshape(ratio, share, size, cols)
            .transpose(1, 0, 3, 2)
            .reshape(share, rows * size)
        )
    return (pair_update, adjoint_first_factor, grad_right, grad_w_out)


def solution(mesh):
    in_specs = (
        P(("parts", "col"), "row", None),
        P(),
        P(),
        P(),
        P(),
        P(),
        P(),
        P("parts"),
        P("parts", None),
        P(("parts", "row"), "col", None),
    )
    out_specs = (
        P(("parts", "row"), "col", None),
        P(("parts", "col"), "row"),
        P(("parts", "col"), "row"),
        P("parts", None),
    )
    return jax.shard_map(shards, mesh=mesh, in_specs=in_specs, out_specs=out_specs, check_vma=False)
```

```python
import functools

import jax
import jax.numpy as jnp
from jax import lax
from jax.experimental import pallas as pl
from jax.experimental.pallas import tpu as pltpu
from jax.sharding import PartitionSpec as P

PROJECTED_SIZE = 32
CZ = 128
WINDOW_AMINOS = 256
CHAINS = 8
LANES = 128
MESH = pl.DeviceIdType.MESH


def standardize_entries(alignment_tensor, standard_multiplier, additive_offset):
    incoming_entries = alignment_tensor.astype(jnp.float32)
    center = incoming_entries - jnp.mean(incoming_entries, axis=-1, keepdims=True)
    spread = jnp.mean(center * center, axis=-1, keepdims=True)
    return (center * lax.rsqrt(spread + 1e-05) * standard_multiplier + additive_offset).astype(
        jnp.bfloat16
    )


def to(source, target, send, recv, row, col):
    return pltpu.make_async_remote_copy(
        src_ref=source,
        dst_ref=target,
        send_sem=send,
        recv_sem=recv,
        device_id={"row": row, "col": col},
        device_id_type=MESH,
    )


def arrived(ref, sem):
    pltpu.make_async_copy(ref, ref, sem).wait()


def greet(n_row, n_col, me):
    peers = n_row * n_col
    barrier = pltpu.get_barrier_semaphore()

    def signal(off, carry):
        peer = (me + off) % peers
        pl.semaphore_signal(
            barrier,
            inc=1,
            device_id={"row": peer // n_col, "col": peer % n_col},
            device_id_type=MESH,
        )
        return carry

    lax.fori_loop(1, peers, signal, 0)
    return lambda: pl.semaphore_wait(barrier, peers - 1)


def fill_tables(
    rows, cols, labels_ref, counts_ref, row, col, table_ref, inverse_ref, over_ref
):
    f32 = jnp.float32
    inner = LANES // cols
    lane = lax.broadcasted_iota(jnp.int32, (1, LANES), 1) % cols
    label = jnp.zeros((1, LANES), jnp.int32)
    for j in range(cols):
        label = jnp.where(lane == j, labels_ref[col * cols + j], label)
    table_ref[...] = jnp.zeros_like(table_ref)
    for a in range(CHAINS):
        line = jnp.zeros((1, LANES), jnp.int32)
        for b in range(CHAINS):
            line = jnp.where(label == b, counts_ref[a, b], line)
        table_ref[a : a + 1, :] = line.astype(f32)

    over_ref[...] = 1.0 / jnp.maximum(table_ref[...], 1.0)
    for i in range(rows):
        inverse_ref[i : i + 1, :] = over_ref[pl.ds(labels_ref[row * rows + i], 1), :]


def fill_weights(blocks, final_ref, wide_ref, weight_ref, weight_t_ref):
    size = PROJECTED_SIZE
    inner = size // blocks
    wide_ref[...] = final_ref[...].astype(jnp.float32)
    for b in range(blocks):
        for e in range(inner):
            weight_ref[b * size : (b + 1) * size, e * CZ : (e + 1) * CZ] = wide_ref[
                pl.ds(b * inner + e, size, stride=size), :
            ].astype(jnp.bfloat16)
    weight_t_ref[...] = weight_ref[...].T


def project(
    share, rows, align_ref, gain_ref, shift_ref, first_ref, second_ref,
    normed_ref, line_ref, turn_ref, left_own, right_own,
):
    f32, bf16 = jnp.float32, jnp.bfloat16
    size = PROJECTED_SIZE
    feats = align_ref.shape[2]
    gain, shift = gain_ref[...], shift_ref[...]

    def normalise(k, carry):
        x = align_ref[pl.ds(k * 4, 4)].reshape(4 * rows, feats).astype(f32)
        center = x - jnp.mean(x, axis=-1, keepdims=True)
        var = jnp.mean(center * center, axis=-1, keepdims=True)
        normed_ref[pl.ds(pl.multiple_of(k * 4 * rows, 4 * rows), 4 * rows), :] = (
            center * lax.rsqrt(var + 1e-05) * gain + shift
        ).astype(bf16)
        return carry

    lax.fori_loop(0, share // 4, normalise, 0)
    low = share // 2
    second = second_ref[...]
    for p in range(low):
        pair = jnp.concatenate(
            [normed_ref[p * rows : (p + 1) * rows], normed_ref[(p + low) * rows : (p + low + 1) * rows]],
            axis=0,
        )
        turn_ref[p * size : (p + 1) * size, :] = lax.dot_general(
            second, pair, (((1,), (1,)), ((), ())), preferred_element_type=f32
        )
    near = lax.broadcasted_iota(jnp.int32, (low, LANES), 1) < rows
    for b in range(size // 2):
        even = turn_ref[pl.ds(2 * b, low, stride=size), :]
        odd = turn_ref[pl.ds(2 * b + 1, low, stride=size), :]
        lanes = slice(b * LANES, (b + 1) * LANES)
        right_own[0, :low, lanes] = jnp.where(near, even, pltpu.roll(odd, rows, 1)).astype(bf16)
        right_own[0, low:, lanes] = jnp.where(near, pltpu.roll(even, rows, 1), odd).astype(bf16)
    yield
    fold = LANES // size
    first = jnp.concatenate([first_ref[...]] * fold, axis=0)
    line_ref[...] = lax.dot_general(
        normed_ref[...], first, (((1,), (1,)), ((), ())), preferred_element_type=f32
    )
    place = lax.broadcasted_iota(jnp.int32, (share, LANES), 1) // size
    for g in range(rows // fold):
        total = line_ref[pl.ds(g * fold, share, stride=rows), :]
        for k in range(1, fold):
            total = jnp.where(
                place == k, line_ref[pl.ds(g * fold + k, share, stride=rows), :], total
            )
        span = left_own.shape[2]
        lanes = slice(g * LANES % span, g * LANES % span + LANES)
        left_own[g * LANES // span, :, lanes] = total.astype(bf16)
    yield


def core_kernel(n_row, n_col, ratio, rows, cols, tile, fused, *refs):
    f32, bf16 = jnp.float32, jnp.bfloat16
    size = PROJECTED_SIZE
    inner = LANES // cols
    blocks = size // inner
    steps = rows // tile
    span = tile * size
    labels_ref, counts_ref, final_ref, bias_ref, grad_hbm = refs[:5]
    count = 10 if fused else 7
    source_refs = refs[5:count]
    pair_out, left_out, right_out, weight_out = refs[count : count + 4]
    refs = refs[count + 4 :]
    if fused:
        normed_ref, line_ref, turn_ref, left_own, right_own = refs[:5]
        refs = refs[5:]
    else:
        left_own, right_own = source_refs
    (
        table_ref, over_ref, inverse_ref, wide_ref, weight_w, weight_t_ref, left_tiles, right_panel,
        g_left_send, g_left_recv, g_right_send, g_right_recv, g_hop_send, g_twin_send, g_own_sem,
        grad, scaled, spread, outer, outer_own, outer_more, left_more, slots, inverses, label_lanes,
        right_t, keep, keep_t, weight_acc, left_ref, right_ref, weight_ref, local_sem,
        left_in, right_twin, right_half, right_mid, right_sum,
        weight_twin, weight_half, weight_mid, weight_sum, weight_in, weight_part,
        up_send, down_send, left_recv, twin_send, twin_recv, mid_send, mid_recv,
        right_send, right_recv, own_sem,
        w1_send, w1_recv, w2_send, w2_recv, w3_send, w3_recv, around_send, hop_send, last_send,
        all_recv,
    ) = refs
    row, col = lax.axis_index("row"), lax.axis_index("col")
    ready = greet(n_row, n_col, row * n_col + col)
    grad_copies = [
        pltpu.make_async_copy(
            grad_hbm.at[pl.ds(t * tile * cols, tile * cols)], grad.at[t], local_sem.at[t]
        )
        for t in range(steps)
    ]
    for copy in grad_copies:
        copy.start()
    seqs, wide = right_panel.shape
    share = seqs // n_col
    width = 2 * LANES if blocks % 2 == 0 else LANES
    chunks = blocks * LANES // width
    extras = outer_more.shape[0] - 1
    chips = n_row // 2
    chip, side = row // 2, row % 2
    twin = row + 1 - 2 * side
    many = n_col // n_row
    half = n_col // 2
    quarter = weight_ref.shape[0] // n_row
    piece = quarter // n_col
    parts = left_recv.shape[1]
    part = left_ref.shape[2] // parts
    owner, slot = col // ratio, col % ratio
    rows_of = lambda index, extent: pl.ds(pl.multiple_of(index * extent, extent), extent)
    mine = side * chips + chip
    add = lambda *terms: functools.reduce(lambda a, b: a + b, [t.astype(f32) for t in terms])

    w1_copy = to(
        weight_ref.at[rows_of(1 - side, chips * quarter)], weight_twin, w1_send, w1_recv, twin, col
    )
    right_parts = twin_recv.shape[0]
    right_part = right_twin.shape[2] // right_parts
    right_lanes = lambda h: slice(h * right_part, (h + 1) * right_part)

    def twin_copy(h):
        return to(
            right_ref.at[rows_of(1 - side, half), :, right_lanes(h)],
            right_twin.at[:, :, right_lanes(h)], twin_send.at[h], twin_recv.at[h], twin, col,
        )

    def w2_copy(off):
        peer = (chip + off) % chips
        return to(
            weight_half.at[rows_of(peer, quarter)], weight_mid.at[chip], w2_send.at[off],
            w2_recv.at[chip], 2 * peer + side, col,
        )

    def mid_copy(off, h):
        peer = (chip + off) % chips
        return to(
            right_half.at[rows_of(peer, many), :, right_lanes(h)],
            right_mid.at[chip, :, :, right_lanes(h)], mid_send.at[off, h],
            mid_recv.at[chip, h], 2 * peer + side, col,
        )

    def right_copy(b, h):
        return to(
            right_sum.at[b, :, right_lanes(h)], right_out.at[slot, :, right_lanes(h)],
            right_send.at[b, h], right_recv.at[slot, h], owner, mine * many + b,
        )

    def left_copies(d, h):
        lanes = slice(h * part, (h + 1) * part)
        for step, sends in ((d, up_send), (-d, down_send)):
            there = col + step
            peer = there % n_col
            copy = to(
                left_ref.at[peer, :, lanes], left_in.at[col, :, lanes], sends.at[d, h],
                left_recv.at[col, h], row, peer,
            )
            yield jnp.logical_and(there >= 0, there < n_col), copy

    def left_start(d, h):
        for on, copy in left_copies(d, h):
            pl.when(on)(copy.start)

    def w3_copy(off):
        peer = (col + off) % n_col
        return to(
            weight_sum.at[rows_of(peer, piece)], weight_in.at[col], w3_send.at[off],
            w3_recv.at[col], row, peer,
        )

    def cell(group, index):
        return weight_out.at[rows_of(group * n_col + index, piece)]

    def spread_copy(send, group, index, to_row, to_col, source=None):
        there = cell(group, index)
        return to(
            there if source is None else source, there, send, all_recv.at[group, index],
            to_row, to_col,
        )

    def around_copy(off):
        return spread_copy(around_send.at[off], mine, col, row, (col + off) % n_col, weight_part)

    def hop_copy(index, off, source=None):
        peer = (chip + off) % chips
        return spread_copy(hop_send.at[index, off], mine, index, 2 * peer + side, col, source)

    def last_copy(group, index, source=None):
        return spread_copy(last_send.at[group, index], group, index, twin, col, source)

    def group_of(off):
        return side * chips + (chip + off) % chips

    def here(b):
        return jnp.logical_and(owner == row, mine * many + b == col)


    own_piece = pltpu.make_async_copy(weight_part, cell(mine, col), own_sem)

    def after_left_extra():
        arrived(weight_twin, w1_recv)
        weight_half[...] = add(
            weight_ref[rows_of(side, chips * quarter), :], weight_twin[...]
        ).astype(bf16)
        for off in range(1, chips):
            w2_copy(off).start()

    def first_left():
        for d in range(1, n_col):
            left_start(d, 0)

    def after_left():
        total = weight_half[rows_of(chip, quarter), :].astype(f32)
        for off in range(1, chips):
            peer = (chip + off) % chips
            arrived(weight_mid.at[peer], w2_recv.at[peer])
            total = add(total, weight_mid[peer])
        weight_sum[...] = total.astype(bf16)
        for off in range(1, n_col):
            w3_copy(off).start()
        for h in range(1, parts):
            for d in range(1, n_col):
                left_start(d, h)

    def during_right():
        total = weight_sum[rows_of(col, piece), :].astype(f32)
        for off in range(1, n_col):
            peer = (col + off) % n_col
            arrived(weight_in.at[peer], w3_recv.at[peer])
            total = add(total, weight_in[peer])
        weight_part[...] = total.astype(bf16)
        own_piece.start()
        for off in range(1, n_col):
            around_copy(off).start()
        for off in range(1, chips):
            hop_copy(col, off, weight_part).start()
        last_copy(mine, col, weight_part).start()

    def right_first(h):
        twin_copy(h).start()

    def right_second(h):
        lanes = right_lanes(h)
        arrived(right_twin.at[:, :, lanes], twin_recv.at[h])
        right_half[:, :, lanes] = add(
            right_ref[rows_of(side, half), :, lanes], right_twin[:, :, lanes]
        ).astype(bf16)
        for off in range(1, chips):
            mid_copy(off, h).start()

    def right_third(h):
        lanes = right_lanes(h)
        total = right_half[rows_of(chip, many), :, lanes].astype(f32)
        for off in range(1, chips):
            peer = (chip + off) % chips
            arrived(right_mid.at[peer, :, :, lanes], mid_recv.at[peer, h])
            total = add(total, right_mid[peer, :, :, lanes])
        right_sum[:, :, lanes] = total.astype(bf16)
        for b in range(many):
            pl.when(jnp.logical_not(here(b)))(right_copy(b, h).start)
            own = pltpu.make_async_copy(
                right_sum.at[b, :, lanes], right_out.at[slot, :, lanes], right_recv.at[slot, h]
            )
            pl.when(here(b))(own.start)

    def pair_second():
        for off in range(1, n_col):
            peer = (col + off) % n_col
            arrived(cell(mine, peer), all_recv.at[mine, peer])
            for hop in range(1, chips):
                hop_copy(peer, hop).start()
            last_copy(mine, peer).start()

    def finish():
        for off in range(n_col):
            peer = (col + off) % n_col
            for hop in range(1, chips):
                arrived(cell(group_of(hop), peer), all_recv.at[group_of(hop), peer])
                last_copy(group_of(hop), peer).start()

        total = left_ref[col].astype(f32)
        for off in range(1, n_col):
            peer = (col + off) % n_col
            for h in range(parts):
                arrived(left_in.at[peer, :, h * part : (h + 1) * part], left_recv.at[peer, h])
            total = add(total, left_in[peer])
        left_out[...] = total.astype(bf16)
        for t in range(ratio):
            for h in range(right_parts):
                arrived(right_out.at[t, :, right_lanes(h)], right_recv.at[t, h])
        for off in range(n_col):
            peer = (col + off) % n_col
            for other in range(chips):
                group = (1 - side) * chips + other
                arrived(cell(group, peer), all_recv.at[group, peer])

        own_piece.wait()
        w1_copy.wait_send()
        for h in range(right_parts):
            twin_copy(h).wait_send()
        for off in range(1, chips):
            w2_copy(off).wait_send()
            for h in range(right_parts):
                mid_copy(off, h).wait_send()
        for off in range(1, n_col):
            w3_copy(off).wait_send()
            around_copy(off).wait_send()
            for h in range(parts):
                for on, copy in left_copies(off, h):
                    pl.when(on)(copy.wait_send)
        for index in range(n_col):
            for off in range(1, chips):
                hop_copy(index, off).wait_send()
            for off in range(chips):
                last_copy(group_of(off), index).wait_send()
        for b in range(many):
            for h in range(right_parts):
                pl.when(jnp.logical_not(here(b)))(right_copy(b, h).wait_send)
    is_owner = row == owner
    same_side = row % 2 == owner % 2
    group = steps // parts
    seq_rows = lambda index: pl.ds(pl.multiple_of(index * share, share), share)
    block = lambda index: right_panel.at[seq_rows(index)]
    tiles_of = lambda index, h: left_tiles.at[h * group : (h + 1) * group, seq_rows(index)]

    def out_right(t):
        return to(
            right_own.at[t], block(col), g_right_send.at[t], g_right_recv.at[col],
            row, row * ratio + t,
        )

    def out_left(d, h):
        for k, step in enumerate((d, -d)):
            there = col + step
            copy = to(
                left_own.at[h * group : (h + 1) * group], tiles_of(col, h),
                g_left_send.at[k, d, h], g_left_recv.at[col, h], row, there % n_col,
            )
            yield jnp.logical_and(there >= 0, there < n_col), copy

    def pass_hop(source, index, hop):
        return to(
            source, block(index), g_hop_send.at[index, hop], g_right_recv.at[index],
            (row + 2 * hop) % n_row, col,
        )

    def pass_twin(source, index):
        return to(source, block(index), g_twin_send.at[index], g_right_recv.at[index], twin, col)

    if fused:
        work = project(
            share, rows, *source_refs, normed_ref, line_ref, turn_ref, left_own, right_own
        )
        next(work)
    ready()
    for t in range(ratio):
        pl.when(row * ratio + t != col)(out_right(t).start)
    own_block = right_own.at[col % ratio]
    own_right = pltpu.make_async_copy(own_block, block(col), g_own_sem.at[1])

    @pl.when(is_owner)
    def _():
        own_right.start()
        for hop in range(1, chips):
            pass_hop(own_block, col, hop).start()
        pass_twin(own_block, col).start()

    if fused:
        next(work)
    own_left = pltpu.make_async_copy(left_own, left_tiles.at[:, seq_rows(col)], g_own_sem.at[0])
    own_left.start()
    for h in range(parts):
        for d in range(1, n_col):
            for on, copy in out_left(d, h):
                pl.when(on)(copy.start)

    def pass_right(off):
        peer = (col + off) % n_col
        source = block(peer)
        if off:
            arrived(source, g_right_recv.at[peer])

            @pl.when(is_owner)
            def _():
                for hop in range(1, chips):
                    pass_hop(source, peer, hop).start()

            pl.when(same_side)(pass_twin(source, peer).start)
        else:

            @pl.when(jnp.logical_not(is_owner))
            def _():
                arrived(source, g_right_recv.at[peer])

            pl.when(jnp.logical_and(same_side, jnp.logical_not(is_owner)))(
                pass_twin(source, peer).start
            )

    fill_weights(blocks, final_ref, wide_ref, weight_w, weight_t_ref)
    fill_tables(
        rows, cols, labels_ref, counts_ref, row, col, table_ref, inverse_ref, over_ref
    )
    place_of = lax.broadcasted_iota(jnp.int32, (tile, span), 1) // size
    seq = lax.broadcasted_iota(jnp.int32, (seqs, LANES), 0).astype(f32)
    for chain in range(keep.shape[0]):
        kept = jnp.where(seq < table_ref[chain : chain + 1, :], 1.0, 0.0)
        keep[chain] = kept.astype(bf16)
        keep_t[chain] = kept.T.astype(bf16)
    for t in range(steps):
        inverses[t] = inverse_ref[t * tile : (t + 1) * tile, :]
        line = jnp.zeros((tile, span), jnp.int32)
        for i in range(tile):
            line = jnp.where(place_of == i, labels_ref[row * rows + t * tile + i], line)
        label_lanes[t] = line
    spread[...] = jnp.zeros_like(spread)
    weight_acc[...] = jnp.zeros_like(weight_acc)
    outer_more[0] = jnp.zeros(outer_more.shape[1:], bf16)
    left_more[0] = jnp.zeros(left_more.shape[1:], f32)
    for copy in grad_copies:
        copy.wait()

    def fill_spread(t):
        for i in range(tile):
            part = grad[t, i * cols : (i + 1) * cols, :]
            for e in range(inner):
                spread[i * LANES + e * cols : i * LANES + (e + 1) * cols, e * CZ : (e + 1) * CZ] = (
                    part
                )

    def scale(step, carry):
        fill_spread(step)
        inverse = inverses[step]
        for i in range(0, tile, 2):
            back = lax.dot_general(
                weight_w[...], spread[i * LANES : (i + 2) * LANES, :], (((1,), (1,)), ((), ())),
                preferred_element_type=f32,
            )
            for k in range(2):
                value = (
                    back[:, k * LANES : (k + 1) * LANES] * inverse[i + k : i + k + 1]
                ).astype(bf16)
                for b in range(blocks):
                    scaled[
                        step, (i + k) * size : (i + k + 1) * size, b * LANES : (b + 1) * LANES
                    ] = value[b * size : (b + 1) * size]
        for off in range(n_col - 1):
            pl.when(step == min(2 * off + 1, steps - 1))(functools.partial(pass_right, off))
        return carry

    lax.fori_loop(0, steps, scale, 0)
    pass_right(n_col - 1)
    pl.when(is_owner)(own_right.wait)
    own_left.wait()
    for b in range(blocks):
        right_t[b * LANES : (b + 1) * LANES, :] = right_panel[:, b * LANES : (b + 1) * LANES].T

    offset = row * rows
    label_of = lambda t, i: labels_ref[offset + t * tile + i]
    lows = [label_of(t, 0) for t in range(steps)]
    more = [lax.div(label_of(t, tile - 1) - lows[t], jnp.int32(2)) for t in range(steps)]
    ends, end = [], 0
    for t in range(steps):
        end = end + more[t]
        ends.append(end)

    flag = lambda test: test.astype(jnp.int32)

    def extra_of(u):
        t = sum([flag(ends[k] <= u) for k in range(steps)])
        chain = flag(t == steps) * CHAINS
        for k in range(steps):
            chain = chain + flag(t == k) * (lows[k] + 2 * (u - ends[k] + more[k] + 1))
        return t - flag(t == steps), chain

    def slot_of(t):
        return sum([flag(t == k) * flag(more[k] > 0) * ends[k] for k in range(steps)])

    def same_of(u):
        return flag(extra_of(u)[0] == extra_of(u - 1)[0]).astype(f32)

    def build(t, chain, place):
        lane = label_lanes[t][:1]
        left = left_tiles[t]
        for k in range(2):
            slots[place, k * seqs : (k + 1) * seqs, :] = left * jnp.where(
                lane == chain + k, 1.0, 0.0
            ).astype(bf16)
        return slots[place]

    def forward(t, chain, place, store):
        both_t = build(t, chain, place).T
        inverse = inverses[t]
        kept = [jnp.concatenate([keep[chain + k]] * (width // LANES), axis=1) for k in range(2)]
        for c in range(chunks):
            lanes = slice(c * width, (c + 1) * width)
            right = right_panel[:, lanes]
            right = jnp.concatenate([right * kept[0], right * kept[1]], axis=0)
            prod = jnp.dot(both_t, right, preferred_element_type=f32)
            for i in range(tile):
                for b in range(width // LANES):
                    first = (c * (width // LANES) + b) * size
                    store(
                        slice(first, first + size), slice(i * LANES, (i + 1) * LANES),
                        (
                            prod[i * size : (i + 1) * size, b * LANES : (b + 1) * LANES]
                            * inverse[i : i + 1]
                        ).astype(bf16),
                    )

    def forward_main(t, carry):
        def store(where, lanes, value):
            outer[t, where, lanes] = value

        forward(t, label_of(t, 0), t, store)
        fill_spread(t)
        weight_acc[...] += jnp.dot(outer[t], spread[...], preferred_element_type=f32)
        return carry

    for h in range(parts):
        for off in range(1, n_col):
            peer = (col + off) % n_col
            arrived(tiles_of(peer, h), g_left_recv.at[peer, h])
        lax.fori_loop(h * group, (h + 1) * group, forward_main, 0)

    def forward_more(u, carry):
        t, chain = extra_of(u)
        same = jnp.full((size, LANES), same_of(u), f32).astype(bf16)

        def store(where, lanes, value):
            outer_own[where, lanes] = value
            outer_more[u + 1, where, lanes] = value + outer_more[u, where, lanes] * same

        forward(t, chain, steps + u, store)
        fill_spread(t)
        weight_acc[...] += jnp.dot(outer_own[...], spread[...], preferred_element_type=f32)
        return carry

    lax.fori_loop(0, extras, forward_more, 0)
    extent = blocks * size
    for e in range(inner):
        weight_ref[e * extent : (e + 1) * extent, :] = weight_acc[
            :, e * CZ : (e + 1) * CZ
        ].astype(bf16)
    w1_copy.start()

    def left_part(t, chain):
        tall = jnp.zeros((span, 2 * seqs), f32)
        for c in range(chunks):
            lanes = slice(c * width, (c + 1) * width)
            kept = [
                jnp.concatenate([keep_t[chain + k]] * (width // LANES), axis=0) for k in range(2)
            ]
            right = right_t[lanes, :]
            right = jnp.concatenate([right * kept[0], right * kept[1]], axis=1)
            tall = tall + jnp.dot(scaled[t, :, lanes], right, preferred_element_type=f32)
        turned = tall.T
        lane = label_lanes[t][:1]
        return jnp.where(lane == chain, turned[:seqs], 0.0) + jnp.where(
            lane == chain + 1, turned[seqs:], 0.0
        )

    def left_extra(u, carry):
        t, chain = extra_of(u)
        left_more[u + 1] = left_part(t, chain) + left_more[u] * same_of(u)
        return carry

    lax.fori_loop(0, extras, left_extra, 0)

    def left_main(t, carry):
        slot = slot_of(t)
        turned = left_part(t, label_of(t, 0)) + left_more[slot]
        lanes = pl.ds(pl.multiple_of(t * span, span), span)
        for q in range(n_col):
            left_ref[q, :, lanes] = turned[q * share : (q + 1) * share].astype(bf16)
        pl.when(t == min(1, steps - 1))(after_left_extra)
        pl.when(t == steps // parts - 1)(first_left)
        return carry

    lax.fori_loop(0, steps, left_main, 0)
    pairs = [(t, label_of(t, 0), t) for t in range(steps)]
    for u in range(extras):
        pairs.append((*extra_of(jnp.int32(u)), steps + u))

    def right_main(c, carry):
        lanes = pl.ds(pl.multiple_of(c * width, width), width)
        total = [jnp.zeros((seqs, LANES), f32) for _ in range(width // LANES)]
        for t, chain, place in pairs:
            out = jnp.dot(slots[place], scaled[t, :, lanes], preferred_element_type=f32)
            kept = [seq < table_ref[pl.ds(chain + k, 1), :] for k in range(2)]
            for b in range(width // LANES):
                part = slice(b * LANES, (b + 1) * LANES)
                total[b] = total[b] + (
                    jnp.where(kept[0], out[:seqs, part], 0.0)
                    + jnp.where(kept[1], out[seqs:, part], 0.0)
                )
        whole = jnp.concatenate(total, axis=1)
        for q in range(n_col):
            right_ref[q, :, lanes] = whole[q * share : (q + 1) * share].astype(bf16)
        pl.when(c == min(1, chunks - 1))(after_left)
        pl.when(c == chunks // 2 - 1)(functools.partial(right_first, 0))
        pl.when(c == max(chunks - 2, chunks // 2))(functools.partial(right_second, 0))
        return carry

    lax.fori_loop(0, chunks, right_main, 0)
    right_first(1)
    lane_group = lax.broadcasted_iota(jnp.int32, (CZ, LANES), 1) // cols

    def pairs_of(t, carry):
        slot = slot_of(t)
        for i in range(0, tile, 2):
            lanes = slice(i * LANES, (i + 2) * LANES)
            both = jnp.dot(
                weight_t_ref[...], outer[t, :, lanes] + outer_more[slot, :, lanes],
                preferred_element_type=f32,
            )
            for k in range(2):
                lanes = slice(k * LANES, (k + 1) * LANES)
                total = both[:CZ, lanes]
                for e in range(1, inner):
                    total = jnp.where(lane_group == e, both[e * CZ : (e + 1) * CZ, lanes], total)
                turned = total.T
                pair = turned[:cols]
                for e in range(1, inner):
                    pair = pair + turned[e * cols : (e + 1) * cols]
                first = pl.multiple_of((t * tile + i + k) * cols, cols)
                pair_out[pl.ds(first, cols), :] = (pair + bias_ref[...]).astype(bf16)
        pl.when(t == min(1, steps - 1))(during_right)
        pl.when(t == min(3, steps - 1))(functools.partial(right_second, 1))
        pl.when(t == steps * 5 // 8)(functools.partial(right_third, 0))
        pl.when(t == steps - 1)(functools.partial(right_third, 1))
        return carry

    lax.fori_loop(0, steps, pairs_of, 0)
    pair_second()
    finish()
    for t in range(ratio):
        pl.when(row * ratio + t != col)(out_right(t).wait_send)
    for h in range(parts):
        for d in range(1, n_col):
            for on, copy in out_left(d, h):
                pl.when(on)(copy.wait_send)

    @pl.when(is_owner)
    def _():
        for index in range(n_col):
            for hop in range(1, chips):
                pass_hop(block(index), index, hop).wait_send()

    @pl.when(same_side)
    def _():
        for index in range(n_col):
            pass_twin(block(index), index).wait_send()


def finish_kernel(
    fused, blocks,
    left_in, right_in, weight_in, pair_in,
    left_out, right_out, weight_out, pair_out,
    left, right, weight, pair, right_done, weight_done, in_sem, out_sem, *more,
):
    f32, bf16 = jnp.float32, jnp.bfloat16
    size = PROJECTED_SIZE
    takes = [
        pltpu.make_async_copy(source, target, in_sem.at[k])
        for k, (source, target) in enumerate(
            ((weight_in, weight), (right_in, right), (left_in, left), (pair_in, pair))
        )
    ]
    gives = [
        pltpu.make_async_copy(source, target, out_sem.at[k])
        for k, (source, target) in enumerate(
            (
                (weight_done, weight_out),
                (right_done if fused else right, right_out),
                (left, left_out),
                (pair, pair_out),
            )
        )
    ]
    for copy in takes:
        copy.start()
    takes[0].wait()
    for g in range(size):
        e = (g % blocks) * (size // blocks) + g // blocks
        weight_done[pl.ds(e, size, stride=size), :] = weight[
            g * size : (g + 1) * size, :
        ].astype(f32) * (1.0 / WINDOW_AMINOS)
    gives[0].start()
    takes[1].wait()
    for k in range(2, 4):
        takes[k].wait()
        gives[k].start()
    if fused:
        turn_ref, line_ref = more
        share = right.shape[1]
        low = share // 2
        rows = line_ref.shape[0] // share
        near = lax.broadcasted_iota(jnp.int32, (low, LANES), 1) < rows
        for b in range(size // 2):
            lanes = slice(b * LANES, (b + 1) * LANES)
            above = right[0, :low, lanes].astype(f32)
            below = right[0, low:, lanes].astype(f32)
            turn_ref[pl.ds(2 * b, low, stride=size), :] = jnp.where(
                near, above, pltpu.roll(below, rows, 1)
            )
            turn_ref[pl.ds(2 * b + 1, low, stride=size), :] = jnp.where(
                near, pltpu.roll(above, rows, 1), below
            )
        fold = LANES // size
        for p in range(low):
            turned = jnp.concatenate([turn_ref[p * size : (p + 1) * size, :]] * fold, axis=0).T
            line_ref[p * rows : (p + 1) * rows, :] = turned[:rows]
            line_ref[(p + low) * rows : (p + low + 1) * rows, :] = turned[rows:]
        place = lax.broadcasted_iota(jnp.int32, (share, LANES), 1) // size
        for g in range(rows // fold):
            total = line_ref[pl.ds(g * fold, share, stride=rows), :]
            for k in range(1, fold):
                total = jnp.where(
                    place == k, line_ref[pl.ds(g * fold + k, share, stride=rows), :], total
                )
            right_done[:, g * LANES : (g + 1) * LANES] = total.astype(bf16)
    gives[1].start()
    for copy in gives:
        copy.wait()


def shards(
    alignment_tensor,
    standardizer_scaling,
    standardizer_offset,
    first_projector,
    second_projector,
    final_projector,
    final_offset,
    amino_strand_label,
    matched_strand_count,
    couple_delta_adjoint,
):
    f32, bf16 = jnp.float32, jnp.bfloat16
    share, rows, feats = alignment_tensor.shape
    cols = couple_delta_adjoint.shape[1]
    size = PROJECTED_SIZE
    n_row, n_col = lax.axis_size("row"), lax.axis_size("col")
    ratio = rows // cols
    seqs = share * n_col
    inner = LANES // cols
    blocks = size // inner
    wide = size * cols
    vmem = pl.BlockSpec(memory_space=pltpu.VMEM)
    dma = pltpu.SemaphoreType.DMA

    tile = 8
    steps = rows // tile
    fused = ratio == 1 and 2 * rows == LANES and share % 16 == 0
    span = tile * size
    if fused:
        sources = (
            alignment_tensor, standardizer_scaling[None, :], standardizer_offset[None, :],
            first_projector.T, second_projector.T,
        )
        extra = [
            pltpu.VMEM((share * rows, feats), bf16),
            pltpu.VMEM((share * rows, LANES), f32),
            pltpu.VMEM((share // 2 * size, LANES), f32),
            pltpu.VMEM((steps, share, span), bf16),
            pltpu.VMEM((ratio, share, wide), bf16),
        ]
    else:
        entries = standardize_entries(
            alignment_tensor, standardizer_scaling, standardizer_offset
        ).reshape(-1, feats)
        both = jnp.dot(
            entries,
            jnp.concatenate([first_projector, second_projector], axis=1),
            preferred_element_type=f32,
        ).astype(bf16)
        left_own = both[:, :size].reshape(share, steps, span).transpose(1, 0, 2)
        right_own = (
            both[:, size:]
            .reshape(share, ratio, cols, size)
            .transpose(1, 0, 3, 2)
            .reshape(ratio, share, wide)
        )
        sources, extra = (left_own, right_own), []
    flat_grad = couple_delta_adjoint.reshape(-1, CZ)
    smem = pl.BlockSpec(memory_space=pltpu.SMEM)
    hbm = pl.BlockSpec(memory_space=pl.ANY)
    chips = n_row // 2
    many = n_col // n_row
    quarter = size * size // n_row
    piece = quarter // n_col
    extras = min(CHAINS - 1, rows - 1) // 2
    pair, left_sum, right_sum, weight_total = pl.pallas_call(
        functools.partial(core_kernel, n_row, n_col, ratio, rows, cols, tile, fused),
        in_specs=[smem, smem, vmem, vmem, hbm] + [vmem] * len(sources),
        out_specs=[vmem] * 4,
        out_shape=[
            jax.ShapeDtypeStruct((rows * cols, CZ), bf16),
            jax.ShapeDtypeStruct((share, rows * size), bf16),
            jax.ShapeDtypeStruct((ratio, share, wide), bf16),
            jax.ShapeDtypeStruct((size * size, CZ), bf16),
        ],
        scratch_shapes=[
            *extra,
            pltpu.VMEM((2 * CHAINS, LANES), f32),
            pltpu.VMEM((2 * CHAINS, LANES), f32),
            pltpu.VMEM((rows, LANES), f32),
            pltpu.VMEM((size * size, CZ), f32),
            pltpu.VMEM((blocks * size, inner * CZ), bf16),
            pltpu.VMEM((inner * CZ, blocks * size), bf16),
            pltpu.VMEM((steps, seqs, span), bf16),
            pltpu.VMEM((seqs, wide), bf16),
            dma((2, n_col, 2)), dma((n_col, 2)), dma((ratio,)), dma((n_col,)),
            dma((n_col, chips)), dma((n_col,)), dma((2,)),
            pltpu.VMEM((steps, tile * cols, CZ), bf16),
            pltpu.VMEM((steps, span, wide), bf16),
            pltpu.VMEM((tile * LANES, inner * CZ), bf16),
            pltpu.VMEM((steps, blocks * size, tile * LANES), bf16),
            pltpu.VMEM((blocks * size, tile * LANES), bf16),
            pltpu.VMEM((extras + 1, blocks * size, tile * LANES), bf16),
            pltpu.VMEM((extras + 1, seqs, span), f32),
            pltpu.VMEM((steps + extras, 2 * seqs, span), bf16),
            pltpu.VMEM((steps, tile, LANES), f32),
            pltpu.VMEM((steps, tile, span), jnp.int32),
            pltpu.VMEM((wide, seqs), bf16),
            pltpu.VMEM((CHAINS + 2, seqs, LANES), bf16),
            pltpu.VMEM((CHAINS + 2, LANES, seqs), bf16),
            pltpu.VMEM((blocks * size, inner * CZ), f32),
            pltpu.VMEM((n_col, share, rows * size), bf16),
            pltpu.VMEM((n_col, share, wide), bf16),
            pltpu.VMEM((size * size, CZ), bf16),
            dma((steps,)),
            pltpu.VMEM((n_col, share, rows * size), bf16),
            pltpu.VMEM((n_col // 2, share, wide), bf16),
            pltpu.VMEM((n_col // 2, share, wide), bf16),
            pltpu.VMEM((chips, many, share, wide), bf16),
            pltpu.VMEM((many, share, wide), bf16),
            pltpu.VMEM((chips * quarter, CZ), bf16),
            pltpu.VMEM((chips * quarter, CZ), bf16),
            pltpu.VMEM((chips, quarter, CZ), bf16),
            pltpu.VMEM((quarter, CZ), bf16),
            pltpu.VMEM((n_col, piece, CZ), bf16),
            pltpu.VMEM((piece, CZ), bf16),
            dma((n_col, 2)), dma((n_col, 2)), dma((n_col, 2)),
            dma((2,)), dma((2,)),
            dma((chips, 2)), dma((chips, 2)),
            dma((many, 2)), dma((ratio, 2)), dma,
            dma, dma,
            dma((chips,)), dma((chips,)),
            dma((n_col,)), dma((n_col,)), dma((n_col,)),
            dma((n_col, chips)), dma((n_row, n_col)), dma((n_row, n_col)),
        ],
        compiler_params=pltpu.CompilerParams(
            collective_id=0, has_side_effects=True, vmem_limit_bytes=60 * 1024 * 1024
        ),
    )(
        amino_strand_label,
        matched_strand_count,
        final_projector,
        final_offset[None, :],
        flat_grad,
        *sources,
    )
    adjoint_first_factor, grad_right, grad_w_out, pair = pl.pallas_call(
        functools.partial(finish_kernel, fused, blocks),
        in_specs=[hbm] * 4,
        out_specs=[hbm] * 4,
        out_shape=[
            jax.ShapeDtypeStruct((share, rows * size), bf16),
            jax.ShapeDtypeStruct((share, rows * size) if fused else (ratio, share, wide), bf16),
            jax.ShapeDtypeStruct((size * size, CZ), f32),
            jax.ShapeDtypeStruct((rows * cols, CZ), bf16),
        ],
        scratch_shapes=[
            pltpu.VMEM((share, rows * size), bf16),
            pltpu.VMEM((ratio, share, wide), bf16),
            pltpu.VMEM((size * size, CZ), bf16),
            pltpu.VMEM((rows * cols, CZ), bf16),
            pltpu.VMEM((share, rows * size), bf16),
            pltpu.VMEM((size * size, CZ), f32),
            dma((4,)), dma((4,)),
        ]
        + (
            [pltpu.VMEM((share // 2 * size, LANES), f32), pltpu.VMEM((share * rows, LANES), f32)]
            if fused
            else []
        ),
    )(left_sum, right_sum, weight_total, pair)
    pair_update = pair.reshape(rows, cols, CZ)
    if not fused:
        grad_right = (
            grad_right.reshape(ratio, share, size, cols)
            .transpose(1, 0, 3, 2)
            .reshape(share, rows * size)
        )
    return (pair_update, adjoint_first_factor, grad_right, grad_w_out)


def solution(mesh):
    in_specs = (
        P(("parts", "col"), "row", None),
        P(),
        P(),
        P(),
        P(),
        P(),
        P(),
        P("parts"),
        P("parts", None),
        P(("parts", "row"), "col", None),
    )
    out_specs = (
        P(("parts", "row"), "col", None),
        P(("parts", "col"), "row"),
        P(("parts", "col"), "row"),
        P("parts", None),
    )
    return jax.shard_map(shards, mesh=mesh, in_specs=in_specs, out_specs=out_specs, check_vma=False)
```
